32 devices in a mesh: leaf: 8 (over z, x), blk: 4 (over y, core).
Axes of the slice: x: 2, y: 2, z: 4, core: 2. Of those that a mesh axis runs over, the one named last changes fastest.
Arguments:
- desc_panel: bfloat16 [256, 384, 128], P(('leaf', 'blk')), may hold values from -18 to 18
- row_map: int32 [256, 3], P(('leaf', 'blk')), may hold values from 0 to 55, as said below
- anc_order: int32 [8], replicated, may hold values from 0 to 7, as said below
- anc_below: int32 [8, 12], replicated, may hold values from 32 to 55, as said below
- anc_panel: float32 [8, 4, 4, 128, 512], P('leaf', None, 'blk'), may hold values from -6 to 27, as said below
Outputs:
- chol_panel: float32 [8, 4, 4, 128, 512], P('leaf', None, 'blk')
The draws below stay inside these ranges and needn't reach their ends.
Inputs may be any that keep to these rules, and one draw needn't show every extreme that they name: `row_map`: entry 0 of each row is a column block of one ancestor; the other entries are distinct entries of that ancestor's row of anc_below. Over the descendants of one device, entry 0 names the column blocks of any one ancestor at most 2 times, and of some ancestor exactly 2 times. `anc_order`: each leaf index holds a different column range. `anc_below`: each row holds 12 distinct indices. `anc_panel`: the leading 512 rows of each ancestor's panel are symmetric, and the leading block of S stays positive definite.
All inputs are finite; a program needn't handle non-finite values.
Results may differ from the reference program's by a relative error of at most 0.0003.
Values may be sent and summed in bfloat16 or wider, within the bound.
No kernel may reach another device: no remote copies, remote signals or barrier semaphores. Data moves between devices by JAX's collectives and lax.ppermute only.
A program may use at most 192 MiB of HBM per device.

```python
import jax
import jax.numpy as jnp
from jax import lax

BR = 128
WD = 128
CB = 4
W = 512
Q = 12
P_SIZE = 16
EXTRA = 24
RB = 3
NA = 8
DESC_DEV = 8
ND = 256
N_BLK = 4


def tree_structure(key):
    keys = jax.random.split(jax.random.fold_in(key, 41), 5)
    anc_order = jax.random.permutation(keys[0], NA).astype(jnp.int32)
    below_picks = jax.vmap(lambda k: jax.random.permutation(k, EXTRA)[:Q])(jax.random.split(keys[1], NA))
    anc_below = (below_picks + NA * CB).astype(jnp.int32)
    device_count = ND // DESC_DEV
    quarter = NA // 4

    def device_targets(k):
        first_key, second_key = jax.random.split(k)
        order = jax.random.permutation(first_key, NA)
        listed = jnp.concatenate([order[:quarter], order[:quarter], order[quarter:3 * quarter]])
        return listed[jax.random.permutation(second_key, DESC_DEV)]
    targets = jax.vmap(device_targets)(jax.random.split(keys[2], device_count)).reshape(ND).astype(jnp.int32)
    columns = jax.random.randint(keys[3], (ND,), 0, CB).astype(jnp.int32)
    picks = jax.vmap(lambda k: jax.random.permutation(k, Q)[:RB - 1])(jax.random.split(keys[4], ND)).astype(jnp.int32)
    below = jnp.take_along_axis(anc_below[targets], picks, axis=1)
    head = anc_order[targets] * CB + columns
    row_map = jnp.concatenate([head[:, None], below], axis=1).astype(jnp.int32)
    return (anc_order, anc_below, row_map)


def draw_anc_order(key, part):
    return tree_structure(key)[0]


def draw_anc_below(key, part):
    return tree_structure(key)[1]


def draw_row_map(key, part):
    return tree_structure(key)[2]


def draw_desc_panel(key, part):
    key = jax.random.fold_in(key, 31)
    shape = (ND, RB, BR, WD)
    values = jnp.clip(jax.random.normal(key, shape, jnp.float32), -6.0, 6.0)
    device_count = ND // DESC_DEV
    head_scale = (2.0 * CB / (device_count * WD)) ** 0.5
    scales = jnp.where(jnp.arange(RB) < 1, head_scale, 3.0).astype(jnp.float32)
    return (values * scales[None, :, None, None]).reshape(ND, RB * BR, WD).astype(jnp.bfloat16)


def draw_anc_panel(key, part):
    keys = jax.random.split(jax.random.fold_in(key, 23), 2)
    total_rows = P_SIZE * BR
    noise = jnp.clip(jax.random.normal(keys[0], (NA, total_rows, W), jnp.float32), -6.0, 6.0)
    diagonal = jax.random.uniform(keys[1], (NA, W), jnp.float32, 12.0, 24.0)
    upper = noise[:, :W, :] * (1.5 / W ** 0.5)
    symmetric = (upper + jnp.swapaxes(upper, 1, 2)) / 2.0 ** 0.5
    symmetric = symmetric + diagonal[:, :, None] * jnp.eye(W, dtype=jnp.float32)[None, :, :]
    whole = jnp.concatenate([symmetric, noise[:, W:, :]], axis=1)
    return whole.reshape(NA, P_SIZE // N_BLK, N_BLK, BR, W).astype(jnp.float32)


def setup_inputs(seed: int = 0) -> dict:
    seeds = jax.random.split(jax.random.key(seed), 6)
    return {
        "desc_panel": draw_desc_panel(jax.random.fold_in(seeds[5], 71), 0),
        "row_map": draw_row_map(jax.random.fold_in(seeds[5], 71), 0),
        "anc_order": draw_anc_order(jax.random.fold_in(seeds[5], 71), 0),
        "anc_below": draw_anc_below(jax.random.fold_in(seeds[5], 71), 0),
        "anc_panel": draw_anc_panel(jax.random.fold_in(seeds[5], 71), 0),
    }


def structure_positions(block_ids, owner_leaf, anc_order, anc_below):
    column_base = anc_order[owner_leaf] * CB
    relative = block_ids - column_base[:, None]
    in_columns = (relative >= 0) & (relative < CB)
    below_ids = anc_below[owner_leaf]
    matching = block_ids[:, :, None] == below_ids[:, None, :]
    offsets = CB + jnp.arange(Q, dtype=jnp.int32)
    below_place = jnp.sum(jnp.where(matching, offsets[None, None, :], 0), axis=2)
    located = jnp.any(matching, axis=2)
    return jnp.where(in_columns, relative, jnp.where(located, below_place, P_SIZE)).astype(jnp.int32)

def owner_of(ranges, anc_order):
    leaves = jnp.arange(NA, dtype=jnp.int32)
    return jnp.sum(jnp.where(anc_order[None, :] == ranges[:, None], leaves[None, :], 0), axis=1).astype(jnp.int32)

def reference(desc_panel, row_map, anc_order, anc_below, anc_panel):
    device_count = ND // DESC_DEV
    panel_groups = desc_panel.reshape(device_count, DESC_DEV, RB, BR, WD)
    id_groups = row_map.reshape(device_count, DESC_DEV, RB)

    def absorb(running, element):
        panel_block, block_ids = element
        blocks = panel_block.astype(jnp.float32)
        owner_leaf = owner_of(block_ids[:, 0] // CB, anc_order)
        positions = structure_positions(block_ids, owner_leaf, anc_order, anc_below)
        column = (block_ids[:, 0] % CB).astype(jnp.int32)
        product = jnp.einsum('nrxw,nyw->nrxy', blocks, blocks[:, 0], precision=lax.Precision.HIGHEST)
        running = running.at[owner_leaf[:, None], positions, :, column[:, None], :].add(product)
        return (running, None)
    initial = jnp.zeros((NA, P_SIZE + 1, BR, CB, BR), jnp.float32)
    running, _ = lax.scan(absorb, initial, (panel_groups, id_groups))
    update = running[:, :P_SIZE].reshape(NA, P_SIZE * BR, W)
    schur_rows = anc_panel.reshape(NA, P_SIZE * BR, W) - update

    def factor(panel_rows):
        lower_factor = jnp.linalg.cholesky(panel_rows[:W])
        return jax.scipy.linalg.solve_triangular(lower_factor, panel_rows.T, lower=True).T
    return lax.map(factor, schur_rows).reshape(anc_panel.shape)
```

```python
import jax
import jax.numpy as jnp
from jax import lax
from jax.experimental import pallas as pl
from jax.experimental.pallas import tpu as pltpu
from jax.sharding import PartitionSpec as P

SLOTS = 2
CODES = 4
CODE_ROWS = 16
PANEL = 8
SPLIT = 2
DIRECT = 8
HIGHEST = lax.Precision.HIGHEST


def repeat(count, body, unroll_to=16):
    if count <= unroll_to:
        for index in range(count):
            body(index)
    else:
        lax.fori_loop(0, count, lambda index, carry: (body(index), carry)[1], 0)


def spaces(count, space):
    return [pl.BlockSpec(memory_space=space)] * count


def pack_kernel(cb, nb, direct, row_map, anc_order, anc_below, panel, *refs):
    leaves = anc_order.shape[0]
    desc_count, block_count = row_map.shape
    rows = panel.shape[1] // block_count
    outs = refs[: leaves if direct else 1]
    tail_out, inverse, used, chosen, codes, code_buf, head_sem, tail_sem, code_sem = refs[len(outs):]
    me = lax.axis_index("leaf")

    def clear(leaf):
        inverse[anc_order[leaf]] = leaf
        used[leaf] = 0
        for slot in range(SLOTS):
            chosen[leaf * SLOTS + slot] = -1
            codes[(leaf * SLOTS + slot) * CODES] = cb
            for r in range(1, CODES):
                codes[(leaf * SLOTS + slot) * CODES + r] = nb

    repeat(leaves, clear)

    def assign(desc):
        head = row_map[desc, 0]
        leaf = inverse[lax.div(head, cb)]
        taken = used[leaf]
        used[leaf] = taken + 1
        place = leaf * SLOTS + taken
        chosen[place] = desc
        codes[place * CODES] = head - anc_order[leaf] * cb
        for r in range(1, block_count):
            target = row_map[desc, r]
            found = jnp.int32(nb)
            for q in range(anc_below.shape[1]):
                found = jnp.where(anc_below[leaf, q] == target, q, found)
            codes[place * CODES + r] = found

    repeat(desc_count, assign)

    def dest(index):
        return jnp.bitwise_xor(me, index) if direct else index

    def head_ref(index):
        return outs[index] if direct else outs[0].at[index]

    def copies(index, slot):
        leaf = dest(index)
        desc = chosen[leaf * SLOTS + slot]
        tail_rows = (block_count - 1) * rows
        head = pltpu.make_async_copy(
            panel.at[desc, pl.ds(0, rows)],
            head_ref(index).at[pl.ds(slot * rows, rows)],
            head_sem.at[index, slot],
        )
        tail = pltpu.make_async_copy(
            panel.at[desc, pl.ds(rows, tail_rows)],
            tail_out.at[leaf, pl.ds(slot * tail_rows, tail_rows)],
            tail_sem.at[index, slot],
        )
        return desc, head, tail

    def code_copy(index):
        return pltpu.make_async_copy(
            code_buf.at[index],
            head_ref(index).at[pl.ds(SLOTS * rows, CODE_ROWS)],
            code_sem.at[index],
        )

    def start(index):
        for slot in range(SLOTS):
            desc, head, tail = copies(index, slot)

            @pl.when(desc >= 0)
            def _():
                head.start()
                tail.start()

    repeat(leaves, start)

    def write_codes(index):
        leaf = dest(index)
        row = lax.broadcasted_iota(jnp.int32, (CODE_ROWS, 128), 0)
        values = jnp.zeros((CODE_ROWS, 128), jnp.int32)
        for entry in range(SLOTS * CODES):
            values = jnp.where(row == entry, codes[leaf * SLOTS * CODES + entry], values)
        code_buf[index] = values.astype(jnp.float32).astype(jnp.bfloat16)
        code_copy(index).start()

    repeat(leaves, write_codes)

    def finish(index):
        for slot in range(SLOTS):
            desc, head, tail = copies(index, slot)

            @pl.when(desc >= 0)
            def _():
                head.wait()
                tail.wait()

        code_copy(index).wait()

    repeat(leaves, finish)


def pack(desc_panel, row_map, anc_order, anc_below, cb, direct):
    leaves = anc_order.shape[0]
    block_count = row_map.shape[1]
    rows = desc_panel.shape[1] // block_count
    width = desc_panel.shape[2]
    head_rows = SLOTS * rows + CODE_ROWS
    dtype = desc_panel.dtype
    if direct:
        heads = [jax.ShapeDtypeStruct((head_rows, width), dtype)] * leaves
    else:
        heads = [jax.ShapeDtypeStruct((leaves, head_rows, width), dtype)]
    tails = jax.ShapeDtypeStruct((leaves, SLOTS * (block_count - 1) * rows, width), dtype)
    nb = anc_below.shape[1]

    def body(*refs):
        pack_kernel(cb, nb, direct, *refs)

    return pl.pallas_call(
        body,
        name="pack",
        out_shape=heads + [tails],
        in_specs=spaces(3, pltpu.SMEM) + spaces(1, pl.ANY),
        out_specs=spaces(len(heads) + 1, pl.ANY),
        scratch_shapes=[
            pltpu.SMEM((leaves,), jnp.int32),
            pltpu.SMEM((leaves,), jnp.int32),
            pltpu.SMEM((leaves * SLOTS,), jnp.int32),
            pltpu.SMEM((leaves * SLOTS * CODES,), jnp.int32),
            pltpu.VMEM((leaves, CODE_ROWS, width), dtype),
            pltpu.SemaphoreType.DMA((leaves, SLOTS)),
            pltpu.SemaphoreType.DMA((leaves, SLOTS)),
            pltpu.SemaphoreType.DMA((leaves,)),
        ],
    )(row_map, anc_order, anc_below, desc_panel)


def diagonal_kernel(cb, leaves, *refs):
    heads = refs[:-3]
    out, left, right = refs[-3:]
    direct = len(heads) > 1
    rows = out.shape[1]
    group = min(leaves, 8)

    def load(index, start, size):
        if direct:
            return heads[index][pl.ds(start, size)]
        return heads[0][index, pl.ds(start, size)]

    def step(base):
        for offset in range(group):
            for slot in range(SLOTS):
                block = load(base + offset, slot * rows, rows)
                code = load(base + offset, SLOTS * rows, CODE_ROWS)[slot * CODES:slot * CODES + 1]
                lanes = pl.ds((offset * SLOTS + slot) * rows, rows)
                valid = jnp.broadcast_to(code.astype(jnp.float32), (rows, rows))
                block = block.astype(jnp.float32)
                right[:, lanes] = jnp.where(valid < cb, block, 0.0).astype(right.dtype)
                for c in range(cb):
                    left[c * rows:(c + 1) * rows, lanes] = jnp.where(
                        valid == c, block, 0.0
                    ).astype(left.dtype)
        return lax.dot_general(
            left[...], right[...], (((1,), (1,)), ((), ())), preferred_element_type=jnp.float32
        )

    if leaves == group:
        out[...] = step(0).reshape(out.shape)
    else:
        out[...] = jnp.zeros_like(out)

        def accumulate(index, carry):
            out[...] += step(index * group).reshape(out.shape)
            return carry

        lax.fori_loop(0, leaves // group, accumulate, 0)


def diagonal_update(heads, cb, leaves, rows):
    group = min(leaves, 8)

    def body(*refs):
        diagonal_kernel(cb, leaves, *refs)

    return pl.pallas_call(
        body,
        name="diagonal",
        out_shape=jax.ShapeDtypeStruct((cb * rows, rows), jnp.float32),
        in_specs=spaces(len(heads), pltpu.VMEM),
        out_specs=pl.BlockSpec(memory_space=pltpu.VMEM),
        scratch_shapes=[
            pltpu.VMEM((cb * rows, group * SLOTS * rows), heads[0].dtype),
            pltpu.VMEM((rows, group * SLOTS * rows), heads[0].dtype),
        ],
        cost_estimate=pl.CostEstimate(flops=2000000000, bytes_accessed=1000000, transcendentals=0),
    )(*heads)


def below_kernel(cb, blk_count, per, leaves, count, codes, tails, *refs):
    heads = refs[:count]
    outs = refs[count:count + blk_count]
    acc, products, sems = refs[count + blk_count:]
    direct = count > 1
    me_leaf = lax.axis_index("leaf")
    me_blk = lax.axis_index("blk")
    rows = acc.shape[1]
    group = min(leaves, 8)
    tail_rows = tails.shape[1] // SLOTS
    extra = tail_rows // rows
    trash = blk_count * cb * per

    def zero(index, carry):
        acc[pl.ds(index * cb, cb)] = jnp.zeros((cb, rows, rows), jnp.float32)
        return carry

    lax.fori_loop(0, blk_count * per, zero, 0)

    def step(base):
        for offset in range(group):
            index = base + offset
            source = jnp.bitwise_xor(me_leaf, index) if direct else index
            for slot in range(SLOTS):
                if direct:
                    head = heads[index][pl.ds(slot * rows, rows)]
                else:
                    head = heads[0][index, pl.ds(slot * rows, rows)]
                tail = tails[source, pl.ds(slot * tail_rows, tail_rows)]
                products[offset * SLOTS + slot] = lax.dot_general(
                    tail, head, (((1,), (1,)), ((), ())), preferred_element_type=jnp.float32
                )
        for offset in range(group):
            for slot in range(SLOTS):
                base_code = ((base + offset) * SLOTS + slot) * CODES
                column = codes[base_code]
                for r in range(extra):
                    position = codes[base_code + 1 + r]
                    relative = jnp.bitwise_xor(lax.rem(position, blk_count), me_blk)
                    place = (relative * cb + column) * per + lax.div(position, blk_count)
                    place = jnp.where(column < cb, place, trash)
                    acc[place] += products[offset * SLOTS + slot, pl.ds(r * rows, rows)]

    if leaves == group:
        step(0)
    else:
        lax.fori_loop(0, leaves // group, lambda index, carry: (step(index * group), carry)[1], 0)
    transfers = [
        pltpu.make_async_copy(acc.at[pl.ds(x * cb * per, cb * per)], outs[x], sems.at[x])
        for x in range(blk_count)
    ]
    for transfer in reversed(transfers):
        transfer.start()
    for transfer in transfers:
        transfer.wait()


def below_update(heads, tails, codes, cb, blk_count, per, leaves, rows):
    group = min(leaves, 8)
    blocks = blk_count * cb * per

    def body(*refs):
        below_kernel(cb, blk_count, per, leaves, len(heads), *refs)

    return pl.pallas_call(
        body,
        name="below",
        out_shape=[jax.ShapeDtypeStruct((cb * per, rows, rows), jnp.float32)] * blk_count,
        in_specs=spaces(1, pltpu.SMEM) + spaces(1 + len(heads), pltpu.VMEM),
        out_specs=spaces(blk_count, pl.ANY),
        scratch_shapes=[
            pltpu.VMEM((blocks + 1, rows, rows), jnp.float32),
            pltpu.VMEM((group * SLOTS, tails.shape[1] // SLOTS, rows), jnp.float32),
            pltpu.SemaphoreType.DMA((blk_count,)),
        ],
        cost_estimate=pl.CostEstimate(flops=2000000000, bytes_accessed=4000000, transcendentals=0),
    )(codes, tails, *heads)


def factor_block(work, rows):
    lane = lax.broadcasted_iota(jnp.int32, (1, rows), 1)
    sub = lax.broadcasted_iota(jnp.int32, (PANEL, 1), 0)
    segments = 4
    size = rows // segments

    for segment in range(segments):
        top = segment * size

        def panel(index, carry):
            base = pl.multiple_of(top + index * PANEL, PANEL)
            strip = work[pl.ds(base, PANEL), :]
            picks = [(lane == base + k) for k in range(PANEL)]
            corner = [
                jnp.sum(jnp.where(picks[k], strip[:, :rows], 0.0), axis=1, keepdims=True)
                for k in range(PANEL)
            ]
            scales = []
            for k in range(PANEL):
                scale = lax.rsqrt(corner[k][k:k + 1])
                scales.append(scale)
                row = strip[k:k + 1] * scale
                low = jnp.where(sub > k, corner[k] * scale, 0.0)
                strip = jnp.where(sub == k, row, strip - low * row)
                for m in range(k, PANEL):
                    entry = corner[m][k:k + 1] * scale
                    corner[m] = jnp.where(sub == k, entry, corner[m] - low * entry)
            full = work[pl.ds(top, rows - top), :rows]
            work[pl.ds(base, PANEL), :] = strip
            rest = lax.broadcasted_iota(jnp.int32, (rows - top, 1), 0) + top >= base + PANEL
            total = jnp.zeros((rows - top, 2 * rows), jnp.float32)
            for k in reversed(range(PANEL)):
                solved = strip[k:k + 1] * scales[k]
                strip = strip - jnp.where(sub < k, corner[k], 0.0) * solved
                column = jnp.sum(jnp.where(picks[k], full, 0.0), axis=1, keepdims=True)
                total = total + jnp.where(rest, column, 0.0) * solved
            work[pl.ds(top, rows - top), :] -= total
            return carry

        lax.fori_loop(0, size // PANEL, panel, 0)


def eliminate(schur, inverses, work, block, cb, rows):
    eye = lax.broadcasted_iota(jnp.int32, (rows, rows), 0) == lax.broadcasted_iota(
        jnp.int32, (rows, rows), 1
    )
    upper = lax.broadcasted_iota(jnp.int32, (rows, rows), 0) <= lax.broadcasted_iota(
        jnp.int32, (rows, rows), 1
    )
    here = block * rows
    work[:, :rows] = schur[block, :, here:here + rows]
    work[:, rows:] = eye.astype(jnp.float32)
    factor_block(work, rows)
    schur[block, :, here:here + rows] = jnp.where(upper, work[:, :rows], 0.0)
    inverse = work[:, rows:]
    inverses[block] = inverse
    if block + 1 < cb:
        after = here + rows
        strip = lax.dot_general(
            inverse, schur[block, :, after:], (((1,), (0,)), ((), ())),
            precision=HIGHEST, preferred_element_type=jnp.float32,
        )
        schur[block, :, after:] = strip
        for other in range(block + 1, cb):
            offset = (other - block - 1) * rows
            schur[other, :, other * rows:] -= lax.dot_general(
                strip[:, offset:offset + rows], strip[:, offset:], (((0,), (0,)), ((), ())),
                precision=HIGHEST, preferred_element_type=jnp.float32,
            )


def first_factor(own_sum, other_sum, strips, cb, rows):
    blk_count = len(strips)

    def body(own_ref, other_ref, *refs):
        strip_refs = refs[:blk_count]
        schur, inverses, work = refs[blk_count:]
        me = lax.axis_index("blk")
        for x in range(blk_count):
            schur[jnp.bitwise_xor(me, x)] = strip_refs[x][...]
        for c in range(cb):
            part = slice(c * rows, (c + 1) * rows)
            schur[c, :, part] -= own_ref[part] + other_ref[part]
        for block in range(cb // SPLIT):
            eliminate(schur, inverses, work, block, cb, rows)

    return pl.pallas_call(
        body,
        name="factor_first",
        out_shape=[
            jax.ShapeDtypeStruct((cb, rows, cb * rows), jnp.float32),
            jax.ShapeDtypeStruct((cb, rows, rows), jnp.float32),
        ],
        in_specs=spaces(2 + blk_count, pltpu.VMEM),
        out_specs=spaces(2, pltpu.VMEM),
        scratch_shapes=[pltpu.VMEM((rows, 2 * rows), jnp.float32)],
        cost_estimate=pl.CostEstimate(flops=10000000000, bytes_accessed=2000000, transcendentals=0),
    )(own_sum, other_sum, *strips)


def last_factor(schur_in, inverses_in, cb, rows):
    width = cb * rows

    def body(schur_ref, inverses_ref, whole, lower, schur, inverses, work):
        me = lax.axis_index("blk")
        schur[...] = schur_ref[...]
        for block in range(cb // SPLIT):
            inverses[block] = inverses_ref[block]
        for block in range(cb // SPLIT, cb):
            eliminate(schur, inverses, work, block, cb, rows)
        for k in range(cb):
            piece = jnp.where(k <= me, schur[k, :, pl.ds(pl.multiple_of(me * rows, rows), rows)], 0.0)
            lower[:, k * rows:(k + 1) * rows] = piece.T
        whole[...] = jnp.zeros_like(whole)
        for i in range(cb):
            whole[i * rows:(i + 1) * rows, i * rows:(i + 1) * rows] = inverses[i]
            if i:
                done = slice(0, i * rows)
                total = jnp.zeros((rows, i * rows), jnp.float32)
                for k in range(i):
                    total = total + lax.dot_general(
                        schur[k, :, i * rows:(i + 1) * rows],
                        whole[k * rows:(k + 1) * rows, done],
                        (((0,), (0,)), ((), ())),
                        precision=HIGHEST, preferred_element_type=jnp.float32,
                    )
                whole[i * rows:(i + 1) * rows, done] = -lax.dot_general(
                    inverses[i], total, (((1,), (0,)), ((), ())),
                    precision=HIGHEST, preferred_element_type=jnp.float32,
                )

    return pl.pallas_call(
        body,
        name="factor_last",
        out_shape=[
            jax.ShapeDtypeStruct((width, width), jnp.float32),
            jax.ShapeDtypeStruct((rows, width), jnp.float32),
        ],
        in_specs=spaces(2, pltpu.VMEM),
        out_specs=spaces(2, pltpu.VMEM),
        scratch_shapes=[
            pltpu.VMEM((cb, rows, width), jnp.float32),
            pltpu.VMEM((cb, rows, rows), jnp.float32),
            pltpu.VMEM((rows, 2 * rows), jnp.float32),
        ],
        cost_estimate=pl.CostEstimate(flops=12000000000, bytes_accessed=2000000, transcendentals=0),
    )(schur_in, inverses_in)


def solve_rows(panel, kept, from_core, from_far, whole, lower, cb, per, rows):
    width = cb * rows

    def body(panel_ref, kept_ref, core_ref, far_ref, whole_ref, lower_ref, out):
        out[0] = lower_ref[...]
        parts = []
        for c in range(cb):
            block = slice(c * per, (c + 1) * per)
            original = panel_ref[1:, :, c * rows:(c + 1) * rows]
            update = kept_ref[block] + core_ref[block] + far_ref[block]
            parts.append((original - update).reshape(per * rows, rows))
        for j in range(cb):
            left = jnp.concatenate(parts[:j + 1], axis=1)
            value = lax.dot_general(
                left, whole_ref[j * rows:(j + 1) * rows, :(j + 1) * rows], (((1,), (1,)), ((), ())),
                precision=HIGHEST, preferred_element_type=jnp.float32,
            )
            out[1:, :, j * rows:(j + 1) * rows] = value.reshape(per, rows, rows)

    return pl.pallas_call(
        body,
        name="solve",
        out_shape=jax.ShapeDtypeStruct((per + 1, rows, width), jnp.float32),
        in_specs=spaces(6, pltpu.VMEM),
        out_specs=pl.BlockSpec(memory_space=pltpu.VMEM),
        cost_estimate=pl.CostEstimate(flops=2000000000, bytes_accessed=5000000, transcendentals=0),
    )(panel, kept, from_core, from_far, whole, lower)


def shards(desc_panel, row_map, anc_order, anc_below, anc_panel):
    leaves = lax.axis_size("leaf")
    blk_count = lax.axis_size("blk")
    rows = anc_panel.shape[3]
    width = anc_panel.shape[4]
    cb = width // rows
    per = anc_below.shape[1] // blk_count
    assert cb == blk_count == 4 and desc_panel.shape[2] == rows
    direct = leaves <= DIRECT and leaves & (leaves - 1) == 0
    near = [(i, i ^ 1) for i in range(blk_count)]
    far = [(i, i ^ 2) for i in range(blk_count)]

    *heads, tails = pack(desc_panel, row_map, anc_order, anc_below, cb, direct)
    if direct:
        heads = [heads[0]] + [
            lax.ppermute(heads[k], "leaf", [(i, i ^ k) for i in range(leaves)])
            for k in range(1, leaves)
        ]
        codes = jnp.stack([head[SLOTS * rows:SLOTS * rows + SLOTS * CODES, 0] for head in heads])
    else:
        heads = [lax.all_to_all(heads[0], "leaf", split_axis=0, concat_axis=0, tiled=True)]
        codes = heads[0][:, SLOTS * rows:SLOTS * rows + SLOTS * CODES, 0]
    codes = codes.astype(jnp.int32).reshape(-1)
    tails = lax.all_to_all(tails, "leaf", split_axis=0, concat_axis=0, tiled=True)

    panel = anc_panel.reshape(per + 1, rows, width)
    strip = panel[0]
    strip_far = lax.ppermute(strip, "blk", far)
    strips = [strip, lax.ppermute(strip, "blk", near), strip_far, lax.ppermute(strip_far, "blk", near)]

    diagonal = diagonal_update(heads, cb, leaves, rows)
    diagonal = diagonal + lax.ppermute(diagonal, "blk", near)
    diagonal_far = lax.ppermute(diagonal, "blk", far)
    schur, inverses = first_factor(diagonal, diagonal_far, strips, cb, rows)

    kept, for_near, for_far, for_both = below_update(
        heads, tails, codes, cb, blk_count, per, leaves, rows
    )
    onward = for_far + lax.ppermute(for_both, "blk", near)
    from_far = lax.ppermute(onward, "blk", far)
    from_near = lax.ppermute(for_near, "blk", near)
    whole, lower = last_factor(schur, inverses, cb, rows)
    out = solve_rows(panel, kept, from_near, from_far, whole, lower, cb, per, rows)
    return out.reshape(anc_panel.shape)


def solution(mesh):
    in_specs = (
        P(("leaf", "blk"), None, None),
        P(("leaf", "blk"), None),
        P(),
        P(),
        P("leaf", None, "blk", None, None),
    )
    out_specs = P("leaf", None, "blk", None, None)
    return jax.shard_map(shards, mesh=mesh, in_specs=in_specs, out_specs=out_specs, check_vma=False)
```

```python
import jax
import jax.numpy as jnp
from jax import lax
from jax.experimental import pallas as pl
from jax.experimental.pallas import tpu as pltpu
from jax.sharding import PartitionSpec as P


SLOTS = 2
CODES = 4
CODE_ROWS = 16
PANEL = 8
SPLIT = 2
DIRECT = 8
HIGHEST = lax.Precision.HIGHEST


def repeat(count, body, unroll_to=16):
    if count <= unroll_to:
        for index in range(count):
            body(index)
    else:
        lax.fori_loop(0, count, lambda index, carry: (body(index), carry)[1], 0)


def spaces(count, space):
    return [pl.BlockSpec(memory_space=space)] * count


def pack_kernel(cb, nb, direct, row_map, anc_order, anc_below, panel, *refs):
    leaves = anc_order.shape[0]
    block_count, desc_count = row_map.shape
    rows = panel.shape[1] // block_count
    outs = refs[: leaves if direct else 1]
    tail_out, inverse, used, chosen, codes, tail_sem = refs[len(outs):]
    me = lax.axis_index("leaf")

    def clear(leaf):
        inverse[anc_order[leaf]] = leaf
        used[leaf] = 0
        for slot in range(SLOTS):
            chosen[leaf * SLOTS + slot] = -1
            codes[(leaf * SLOTS + slot) * CODES] = cb
            for r in range(1, CODES):
                codes[(leaf * SLOTS + slot) * CODES + r] = nb

    repeat(leaves, clear)

    def assign(desc):
        head = row_map[0, desc]
        leaf = inverse[lax.div(head, cb)]
        taken = used[leaf]
        used[leaf] = taken + 1
        place = leaf * SLOTS + taken
        chosen[place] = desc
        codes[place * CODES] = head - anc_order[leaf] * cb
        for r in range(1, block_count):
            target = row_map[r, desc]
            found = jnp.int32(nb)
            for q in range(anc_below.shape[1]):
                found = jnp.where(anc_below[leaf, q] == target, q, found)
            codes[place * CODES + r] = found

    repeat(desc_count, assign)

    def dest(index):
        return jnp.bitwise_xor(me, index) if direct else index

    def tail_copy(index, slot):
        leaf = dest(index)
        desc = chosen[leaf * SLOTS + slot]
        tail_rows = (block_count - 1) * rows
        return desc, pltpu.make_async_copy(
            panel.at[jnp.maximum(desc, 0), pl.ds(rows, tail_rows)],
            tail_out.at[leaf, pl.ds(slot * tail_rows, tail_rows)],
            tail_sem.at[index, slot],
        )

    def start(index):
        for slot in range(SLOTS):
            desc, copy = tail_copy(index, slot)

            @pl.when(desc >= 0)
            def _():
                copy.start()

    repeat(leaves, start)

    def write_head(index):
        leaf = dest(index)
        row = lax.broadcasted_iota(jnp.int32, (CODE_ROWS, 128), 0)
        values = jnp.zeros((CODE_ROWS, 128), jnp.int32)
        for entry in range(SLOTS * CODES):
            values = jnp.where(row == entry, codes[leaf * SLOTS * CODES + entry], values)
        values = values.astype(jnp.float32).astype(panel.dtype)
        for slot in range(SLOTS):
            desc = jnp.maximum(chosen[leaf * SLOTS + slot], 0)
            block = panel[desc, pl.ds(0, rows)]
            if direct:
                outs[index][pl.ds(slot * rows, rows)] = block
            else:
                outs[0][index, pl.ds(slot * rows, rows)] = block
        if direct:
            outs[index][pl.ds(SLOTS * rows, CODE_ROWS)] = values
        else:
            outs[0][index, pl.ds(SLOTS * rows, CODE_ROWS)] = values

    repeat(leaves, write_head)

    def finish(index):
        for slot in range(SLOTS):
            desc, copy = tail_copy(index, slot)

            @pl.when(desc >= 0)
            def _():
                copy.wait()

    repeat(leaves, finish)


def pack(desc_panel, row_map, anc_order, anc_below, cb, direct):
    leaves = anc_order.shape[0]
    block_count = row_map.shape[1]
    rows = desc_panel.shape[1] // block_count
    width = desc_panel.shape[2]
    head_rows = SLOTS * rows + CODE_ROWS
    dtype = desc_panel.dtype
    if direct:
        heads = [jax.ShapeDtypeStruct((head_rows, width), dtype)] * leaves
    else:
        heads = [jax.ShapeDtypeStruct((leaves, head_rows, width), dtype)]
    tails = jax.ShapeDtypeStruct((leaves, SLOTS * (block_count - 1) * rows, width), dtype)
    nb = anc_below.shape[1]

    def body(*refs):
        pack_kernel(cb, nb, direct, *refs)

    return pl.pallas_call(
        body,
        name="pack",
        out_shape=heads + [tails],
        in_specs=spaces(3, pltpu.SMEM) + spaces(1, pltpu.VMEM),
        out_specs=spaces(len(heads), pltpu.VMEM) + spaces(1, pl.ANY),
        scratch_shapes=[
            pltpu.SMEM((leaves,), jnp.int32),
            pltpu.SMEM((leaves,), jnp.int32),
            pltpu.SMEM((leaves * SLOTS,), jnp.int32),
            pltpu.SMEM((leaves * SLOTS * CODES,), jnp.int32),
            pltpu.SemaphoreType.DMA((leaves, SLOTS)),
        ],
    )(row_map.T, anc_order, anc_below, desc_panel)


def diagonal_kernel(cb, leaves, *refs):
    heads = refs[:-4]
    out, codes, left, right = refs[-4:]
    direct = len(heads) > 1
    rows = out.shape[1]
    group = min(leaves, 8)

    def load(index, start, size):
        if direct:
            return heads[index][pl.ds(start, size)]
        return heads[0][index, pl.ds(start, size)]

    lane = lax.broadcasted_iota(jnp.int32, (1, rows), 1)

    def step(base):
        for offset in range(group):
            marks = load(base + offset, SLOTS * rows, CODE_ROWS).astype(jnp.float32)
            packed = jnp.zeros((1, rows), jnp.float32)
            for entry in range(SLOTS * CODES):
                packed = jnp.where(lane == entry, marks[entry:entry + 1], packed)
            codes[pl.ds(base + offset, 1)] = packed.astype(jnp.int32)
            for slot in range(SLOTS):
                block = load(base + offset, slot * rows, rows)
                lanes = pl.ds((offset * SLOTS + slot) * rows, rows)
                code = jnp.broadcast_to(marks[slot * CODES:slot * CODES + 1], (rows, rows))
                code = code.astype(block.dtype)
                zero = jnp.zeros_like(block)
                right[:, lanes] = jnp.where(code < cb, block, zero)
                for c in range(cb):
                    left[c * rows:(c + 1) * rows, lanes] = jnp.where(code == c, block, zero)
        return lax.dot_general(
            left[...], right[...], (((1,), (1,)), ((), ())), preferred_element_type=jnp.float32
        )

    if leaves == group:
        out[...] = step(0).reshape(out.shape)
    else:
        out[...] = jnp.zeros_like(out)

        def accumulate(index, carry):
            out[...] += step(index * group).reshape(out.shape)
            return carry

        lax.fori_loop(0, leaves // group, accumulate, 0)


def diagonal_update(heads, cb, leaves, rows):
    group = min(leaves, 8)

    def body(*refs):
        diagonal_kernel(cb, leaves, *refs)

    return pl.pallas_call(
        body,
        name="diagonal",
        out_shape=[
            jax.ShapeDtypeStruct((cb * rows, rows), jnp.float32),
            jax.ShapeDtypeStruct((leaves, rows), jnp.int32),
        ],
        in_specs=spaces(len(heads), pltpu.VMEM),
        out_specs=spaces(2, pltpu.VMEM),
        scratch_shapes=[
            pltpu.VMEM((cb * rows, group * SLOTS * rows), heads[0].dtype),
            pltpu.VMEM((rows, group * SLOTS * rows), heads[0].dtype),
        ],
        cost_estimate=pl.CostEstimate(flops=2000000000, bytes_accessed=1000000, transcendentals=0),
    )(*heads)


def below_kernel(cb, blk_count, per, leaves, count, codes, tails, *refs):
    heads = refs[:count]
    outs = refs[count:count + blk_count]
    acc, products, sems = refs[count + blk_count:]
    direct = count > 1
    me_leaf = lax.axis_index("leaf")
    me_blk = lax.axis_index("blk")
    rows = acc.shape[1]
    group = min(leaves, 8)
    tail_rows = tails.shape[1] // SLOTS
    extra = tail_rows // rows
    trash = blk_count * cb * per

    def zero(index, carry):
        acc[pl.ds(index * cb, cb)] = jnp.zeros((cb, rows, rows), jnp.float32)
        return carry

    lax.fori_loop(0, blk_count * per, zero, 0)

    def step(base):
        for offset in range(group):
            index = base + offset
            source = jnp.bitwise_xor(me_leaf, index) if direct else index
            for slot in range(SLOTS):
                if direct:
                    head = heads[index][pl.ds(slot * rows, rows)]
                else:
                    head = heads[0][index, pl.ds(slot * rows, rows)]
                tail = tails[source, pl.ds(slot * tail_rows, tail_rows)]
                products[offset * SLOTS + slot] = lax.dot_general(
                    tail, head, (((1,), (1,)), ((), ())), preferred_element_type=jnp.float32
                )
        for offset in range(group):
            for slot in range(SLOTS):
                column = codes[base + offset, slot * CODES]
                for r in range(extra):
                    position = codes[base + offset, slot * CODES + 1 + r]
                    relative = jnp.bitwise_xor(lax.rem(position, blk_count), me_blk)
                    place = (relative * cb + column) * per + lax.div(position, blk_count)
                    place = jnp.where(column < cb, place, trash)
                    acc[place] += products[offset * SLOTS + slot, pl.ds(r * rows, rows)]

    if leaves == group:
        step(0)
    else:
        lax.fori_loop(0, leaves // group, lambda index, carry: (step(index * group), carry)[1], 0)
    transfers = [
        pltpu.make_async_copy(acc.at[pl.ds(x * cb * per, cb * per)], outs[x], sems.at[x])
        for x in range(blk_count)
    ]
    for transfer in reversed(transfers):
        transfer.start()
    for transfer in transfers:
        transfer.wait()


def below_update(heads, tails, codes, cb, blk_count, per, leaves, rows):
    group = min(leaves, 8)
    blocks = blk_count * cb * per

    def body(*refs):
        below_kernel(cb, blk_count, per, leaves, len(heads), *refs)

    return pl.pallas_call(
        body,
        name="below",
        out_shape=[jax.ShapeDtypeStruct((cb * per, rows, rows), jnp.float32)] * blk_count,
        in_specs=spaces(1, pltpu.SMEM) + spaces(1 + len(heads), pltpu.VMEM),
        out_specs=spaces(blk_count, pl.ANY),
        scratch_shapes=[
            pltpu.VMEM((blocks + 1, rows, rows), jnp.float32),
            pltpu.VMEM((group * SLOTS, tails.shape[1] // SLOTS, rows), jnp.float32),
            pltpu.SemaphoreType.DMA((blk_count,)),
        ],
        cost_estimate=pl.CostEstimate(flops=2000000000, bytes_accessed=4000000, transcendentals=0),
    )(codes, tails, *heads)


def factor_block(work, rows):
    lane = lax.broadcasted_iota(jnp.int32, (1, rows), 1)
    sub = lax.broadcasted_iota(jnp.int32, (PANEL, 1), 0)
    segments = 4
    size = rows // segments

    for segment in range(segments):
        top = segment * size

        def panel(index, carry):
            base = pl.multiple_of(top + index * PANEL, PANEL)
            strip = work[pl.ds(base, PANEL), :]
            picks = [(lane == base + k) for k in range(PANEL)]
            corner = [
                jnp.sum(jnp.where(picks[k], strip[:, :rows], 0.0), axis=1, keepdims=True)
                for k in range(PANEL)
            ]
            scales = []
            for k in range(PANEL):
                scale = lax.rsqrt(corner[k][k:k + 1])
                scales.append(scale)
                row = strip[k:k + 1] * scale
                low = jnp.where(sub > k, corner[k] * scale, 0.0)
                strip = jnp.where(sub == k, row, strip - low * row)
                for m in range(k, PANEL):
                    entry = corner[m][k:k + 1] * scale
                    corner[m] = jnp.where(sub == k, entry, corner[m] - low * entry)
            full = work[pl.ds(top, rows - top), :rows]
            work[pl.ds(base, PANEL), :] = strip
            rest = lax.broadcasted_iota(jnp.int32, (rows - top, 1), 0) + top >= base + PANEL
            total = jnp.zeros((rows - top, 2 * rows), jnp.float32)
            for k in reversed(range(PANEL)):
                solved = strip[k:k + 1] * scales[k]
                strip = strip - jnp.where(sub < k, corner[k], 0.0) * solved
                column = jnp.sum(jnp.where(picks[k], full, 0.0), axis=1, keepdims=True)
                total = total + jnp.where(rest, column, 0.0) * solved
            work[pl.ds(top, rows - top), :] -= total
            return carry

        lax.fori_loop(0, size // PANEL, panel, 0)


def eliminate(schur, inverses, work, block, cb, rows):
    eye = lax.broadcasted_iota(jnp.int32, (rows, rows), 0) == lax.broadcasted_iota(
        jnp.int32, (rows, rows), 1
    )
    upper = lax.broadcasted_iota(jnp.int32, (rows, rows), 0) <= lax.broadcasted_iota(
        jnp.int32, (rows, rows), 1
    )
    here = block * rows
    work[:, :rows] = schur[block, :, here:here + rows]
    work[:, rows:] = eye.astype(jnp.float32)
    factor_block(work, rows)
    schur[block, :, here:here + rows] = jnp.where(upper, work[:, :rows], 0.0)
    inverse = work[:, rows:]
    inverses[block] = inverse
    if block + 1 < cb:
        after = here + rows
        strip = lax.dot_general(
            inverse, schur[block, :, after:], (((1,), (0,)), ((), ())),
            precision=HIGHEST, preferred_element_type=jnp.float32,
        )
        schur[block, :, after:] = strip
        for other in range(block + 1, cb):
            offset = (other - block - 1) * rows
            schur[other, :, other * rows:] -= lax.dot_general(
                strip[:, offset:offset + rows], strip[:, offset:], (((0,), (0,)), ((), ())),
                precision=HIGHEST, preferred_element_type=jnp.float32,
            )


def first_factor(own_sum, other_sum, strips, cb, rows):
    blk_count = len(strips)

    def body(own_ref, other_ref, *refs):
        strip_refs = refs[:blk_count]
        schur, inverses, work = refs[blk_count:]
        me = lax.axis_index("blk")
        for x in range(blk_count):
            schur[jnp.bitwise_xor(me, x)] = strip_refs[x][...]
        for c in range(cb):
            part = slice(c * rows, (c + 1) * rows)
            schur[c, :, part] -= own_ref[part] + other_ref[part]
        for block in range(cb // SPLIT):
            eliminate(schur, inverses, work, block, cb, rows)

    return pl.pallas_call(
        body,
        name="factor_first",
        out_shape=[
            jax.ShapeDtypeStruct((cb, rows, cb * rows), jnp.float32),
            jax.ShapeDtypeStruct((cb, rows, rows), jnp.float32),
        ],
        in_specs=spaces(2 + blk_count, pltpu.VMEM),
        out_specs=spaces(2, pltpu.VMEM),
        scratch_shapes=[pltpu.VMEM((rows, 2 * rows), jnp.float32)],
        cost_estimate=pl.CostEstimate(flops=10000000000, bytes_accessed=2000000, transcendentals=0),
    )(own_sum, other_sum, *strips)


def last_factor(schur_in, inverses_in, cb, rows):
    width = cb * rows

    def body(schur_ref, inverses_ref, whole, lower, schur, inverses, work):
        me = lax.axis_index("blk")
        schur[...] = schur_ref[...]
        for block in range(cb // SPLIT):
            inverses[block] = inverses_ref[block]
        for block in range(cb // SPLIT, cb):
            eliminate(schur, inverses, work, block, cb, rows)
        for k in range(cb):
            piece = jnp.where(k <= me, schur[k, :, pl.ds(pl.multiple_of(me * rows, rows), rows)], 0.0)
            lower[:, k * rows:(k + 1) * rows] = piece.T
        whole[...] = jnp.zeros_like(whole)
        for i in range(cb):
            whole[i * rows:(i + 1) * rows, i * rows:(i + 1) * rows] = inverses[i]
            if i:
                done = slice(0, i * rows)
                total = jnp.zeros((rows, i * rows), jnp.float32)
                for k in range(i):
                    total = total + lax.dot_general(
                        schur[k, :, i * rows:(i + 1) * rows],
                        whole[k * rows:(k + 1) * rows, done],
                        (((0,), (0,)), ((), ())),
                        precision=HIGHEST, preferred_element_type=jnp.float32,
                    )
                whole[i * rows:(i + 1) * rows, done] = -lax.dot_general(
                    inverses[i], total, (((1,), (0,)), ((), ())),
                    precision=HIGHEST, preferred_element_type=jnp.float32,
                )

    return pl.pallas_call(
        body,
        name="factor_last",
        out_shape=[
            jax.ShapeDtypeStruct((width, width), jnp.float32),
            jax.ShapeDtypeStruct((rows, width), jnp.float32),
        ],
        in_specs=spaces(2, pltpu.VMEM),
        out_specs=spaces(2, pltpu.VMEM),
        scratch_shapes=[
            pltpu.VMEM((cb, rows, width), jnp.float32),
            pltpu.VMEM((cb, rows, rows), jnp.float32),
            pltpu.VMEM((rows, 2 * rows), jnp.float32),
        ],
        cost_estimate=pl.CostEstimate(flops=12000000000, bytes_accessed=2000000, transcendentals=0),
    )(schur_in, inverses_in)


def solve_rows(panel, kept, from_core, from_far, whole, lower, cb, per, rows):
    width = cb * rows

    def body(panel_ref, kept_ref, core_ref, far_ref, whole_ref, lower_ref, out):
        out[0] = lower_ref[...]
        parts = []
        for c in range(cb):
            block = slice(c * per, (c + 1) * per)
            original = panel_ref[1:, :, c * rows:(c + 1) * rows]
            update = kept_ref[block] + core_ref[block] + far_ref[block]
            parts.append((original - update).reshape(per * rows, rows))
        step = 2
        for j in range(0, cb, step):
            left = jnp.concatenate(parts[:j + step], axis=1)
            span = slice(j * rows, (j + step) * rows)
            value = lax.dot_general(
                left, whole_ref[span, :(j + step) * rows], (((1,), (1,)), ((), ())),
                precision=HIGHEST, preferred_element_type=jnp.float32,
            )
            out[1:, :, span] = value.reshape(per, rows, step * rows)

    return pl.pallas_call(
        body,
        name="solve",
        out_shape=jax.ShapeDtypeStruct((per + 1, rows, width), jnp.float32),
        in_specs=spaces(6, pltpu.VMEM),
        out_specs=pl.BlockSpec(memory_space=pltpu.VMEM),
        cost_estimate=pl.CostEstimate(flops=2000000000, bytes_accessed=5000000, transcendentals=0),
    )(panel, kept, from_core, from_far, whole, lower)


def shards(desc_panel, row_map, anc_order, anc_below, anc_panel):
    leaves = lax.axis_size("leaf")
    blk_count = lax.axis_size("blk")
    rows = anc_panel.shape[3]
    width = anc_panel.shape[4]
    cb = width // rows
    per = anc_below.shape[1] // blk_count
    assert cb == blk_count == 4 and desc_panel.shape[2] == rows
    direct = leaves <= DIRECT and leaves & (leaves - 1) == 0
    near = [(i, i ^ 1) for i in range(blk_count)]
    far = [(i, i ^ 2) for i in range(blk_count)]

    *heads, tails = pack(desc_panel, row_map, anc_order, anc_below, cb, direct)
    if direct:
        heads = [heads[0]] + [
            lax.ppermute(heads[k], "leaf", [(i, i ^ k) for i in range(leaves)])
            for k in range(1, leaves)
        ]
    else:
        heads = [lax.all_to_all(heads[0], "leaf", split_axis=0, concat_axis=0, tiled=True)]
    tails = lax.all_to_all(tails, "leaf", split_axis=0, concat_axis=0, tiled=True)

    panel = anc_panel.reshape(per + 1, rows, width)
    strip = panel[0]
    strip_far = lax.ppermute(strip, "blk", far)
    strip_near = lax.ppermute(strip, "blk", near)
    strip_both = lax.ppermute(strip_far, "blk", near)
    strips = [strip, strip_near, strip_far, strip_both]

    diagonal, codes = diagonal_update(heads, cb, leaves, rows)
    diagonal_near = lax.ppermute(diagonal, "blk", near)
    diagonal = diagonal + diagonal_near
    diagonal_far = lax.ppermute(diagonal, "blk", far)
    schur, inverses = first_factor(diagonal, diagonal_far, strips, cb, rows)

    kept, for_near, for_far, for_both = below_update(
        heads, tails, codes, cb, blk_count, per, leaves, rows
    )
    for_both = lax.ppermute(for_both, "blk", near)
    from_near = lax.ppermute(for_near, "blk", near)
    onward = for_far + for_both
    from_far = lax.ppermute(onward, "blk", far)
    whole, lower = last_factor(schur, inverses, cb, rows)
    out = solve_rows(panel, kept, from_near, from_far, whole, lower, cb, per, rows)
    return out.reshape(anc_panel.shape)


def solution(mesh):
    in_specs = (
        P(("leaf", "blk"), None, None),
        P(("leaf", "blk"), None),
        P(),
        P(),
        P("leaf", None, "blk", None, None),
    )
    out_specs = P("leaf", None, "blk", None, None)

    return jax.shard_map(shards, mesh=mesh, in_specs=in_specs, out_specs=out_specs, check_vma=False)
```

```python
import jax
import jax.numpy as jnp
from jax import lax
from jax.experimental import pallas as pl
from jax.experimental.pallas import tpu as pltpu
from jax.sharding import PartitionSpec as P


SLOTS = 2
CODES = 4
CODE_ROWS = 16
PANEL = 8
SPLIT = 2
HALVES = 2
DIRECT = 8
HIGHEST = lax.Precision.HIGHEST


def repeat(count, body, unroll_to=16):
    if count <= unroll_to:
        for index in range(count):
            body(index)
    else:
        lax.fori_loop(0, count, lambda index, carry: (body(index), carry)[1], 0)


def spaces(count, space):
    return [pl.BlockSpec(memory_space=space)] * count


def pack_kernel(cb, nb, direct, row_map, anc_order, anc_below, panel, *refs):
    leaves = anc_order.shape[0]
    block_count, desc_count = row_map.shape
    rows = panel.shape[1] // block_count
    outs = refs[: leaves if direct else 1]
    tail_out, inverse, used, chosen, codes, tail_sem = refs[len(outs):]
    me = lax.axis_index("leaf")

    def clear(leaf):
        inverse[anc_order[leaf]] = leaf
        used[leaf] = 0
        for slot in range(SLOTS):
            chosen[leaf * SLOTS + slot] = -1
            codes[(leaf * SLOTS + slot) * CODES] = cb
            for r in range(1, CODES):
                codes[(leaf * SLOTS + slot) * CODES + r] = nb

    repeat(leaves, clear)

    def assign(desc):
        head = row_map[0, desc]
        leaf = inverse[lax.div(head, cb)]
        taken = used[leaf]
        used[leaf] = taken + 1
        place = leaf * SLOTS + taken
        chosen[place] = desc
        codes[place * CODES] = head - anc_order[leaf] * cb
        for r in range(1, block_count):
            target = row_map[r, desc]
            found = jnp.int32(nb)
            for q in range(anc_below.shape[1]):
                found = jnp.where(anc_below[leaf, q] == target, q, found)
            codes[place * CODES + r] = found

    repeat(desc_count, assign)

    def dest(index):
        return jnp.bitwise_xor(me, index) if direct else index

    def tail_copy(index, slot):
        leaf = dest(index)
        desc = chosen[leaf * SLOTS + slot]
        tail_rows = (block_count - 1) * rows
        return desc, pltpu.make_async_copy(
            panel.at[jnp.maximum(desc, 0), pl.ds(rows, tail_rows)],
            tail_out.at[leaf, pl.ds(slot * tail_rows, tail_rows)],
            tail_sem.at[index, slot],
        )

    def start(index):
        for slot in range(SLOTS):
            desc, copy = tail_copy(index, slot)

            @pl.when(desc >= 0)
            def _():
                copy.start()

    repeat(leaves, start)

    def write_head(index):
        leaf = dest(index)
        row = lax.broadcasted_iota(jnp.int32, (CODE_ROWS, 128), 0)
        values = jnp.zeros((CODE_ROWS, 128), jnp.int32)
        for entry in range(SLOTS * CODES):
            values = jnp.where(row == entry, codes[leaf * SLOTS * CODES + entry], values)
        values = values.astype(jnp.float32).astype(panel.dtype)
        for slot in range(SLOTS):
            desc = jnp.maximum(chosen[leaf * SLOTS + slot], 0)
            block = panel[desc, pl.ds(0, rows)]
            if direct:
                outs[index][pl.ds(slot * rows, rows)] = block
            else:
                outs[0][index, pl.ds(slot * rows, rows)] = block
        if direct:
            outs[index][pl.ds(SLOTS * rows, CODE_ROWS)] = values
        else:
            outs[0][index, pl.ds(SLOTS * rows, CODE_ROWS)] = values

    repeat(leaves, write_head)

    def finish(index):
        for slot in range(SLOTS):
            desc, copy = tail_copy(index, slot)

            @pl.when(desc >= 0)
            def _():
                copy.wait()

    repeat(leaves, finish)


def pack(desc_panel, row_map, anc_order, anc_below, cb, direct):
    leaves = anc_order.shape[0]
    block_count = row_map.shape[1]
    rows = desc_panel.shape[1] // block_count
    width = desc_panel.shape[2]
    head_rows = SLOTS * rows + CODE_ROWS
    dtype = desc_panel.dtype
    if direct:
        heads = [jax.ShapeDtypeStruct((head_rows, width), dtype)] * leaves
    else:
        heads = [jax.ShapeDtypeStruct((leaves, head_rows, width), dtype)]
    tails = jax.ShapeDtypeStruct((leaves, SLOTS * (block_count - 1) * rows, width), dtype)
    nb = anc_below.shape[1]

    def body(*refs):
        pack_kernel(cb, nb, direct, *refs)

    return pl.pallas_call(
        body,
        name="pack",
        out_shape=heads + [tails],
        in_specs=spaces(3, pltpu.SMEM) + spaces(1, pltpu.VMEM),
        out_specs=spaces(len(heads), pltpu.VMEM) + spaces(1, pl.ANY),
        scratch_shapes=[
            pltpu.SMEM((leaves,), jnp.int32),
            pltpu.SMEM((leaves,), jnp.int32),
            pltpu.SMEM((leaves * SLOTS,), jnp.int32),
            pltpu.SMEM((leaves * SLOTS * CODES,), jnp.int32),
            pltpu.SemaphoreType.DMA((leaves, SLOTS)),
        ],
    )(row_map.T, anc_order, anc_below, desc_panel)


def diagonal_kernel(cb, leaves, *refs):
    heads = refs[:-4]
    out, codes, left, right = refs[-4:]
    direct = len(heads) > 1
    rows = out.shape[1]
    group = min(leaves, 8)

    def load(index, start, size):
        if direct:
            return heads[index][pl.ds(start, size)]
        return heads[0][index, pl.ds(start, size)]

    lane = lax.broadcasted_iota(jnp.int32, (1, rows), 1)

    def step(base):
        for offset in range(group):
            marks = load(base + offset, SLOTS * rows, CODE_ROWS).astype(jnp.float32)
            packed = jnp.zeros((1, rows), jnp.float32)
            for entry in range(SLOTS * CODES):
                packed = jnp.where(lane == entry, marks[entry:entry + 1], packed)
            codes[pl.ds(base + offset, 1)] = packed.astype(jnp.int32)
            for slot in range(SLOTS):
                block = load(base + offset, slot * rows, rows)
                lanes = pl.ds((offset * SLOTS + slot) * rows, rows)
                code = jnp.broadcast_to(marks[slot * CODES:slot * CODES + 1], (rows, rows))
                code = code.astype(block.dtype)
                zero = jnp.zeros_like(block)
                right[:, lanes] = jnp.where(code < cb, block, zero)
                for c in range(cb):
                    left[c * rows:(c + 1) * rows, lanes] = jnp.where(code == c, block, zero)
        return lax.dot_general(
            left[...], right[...], (((1,), (1,)), ((), ())), preferred_element_type=jnp.float32
        )

    if leaves == group:
        out[...] = step(0).reshape(out.shape)
    else:
        out[...] = jnp.zeros_like(out)

        def accumulate(index, carry):
            out[...] += step(index * group).reshape(out.shape)
            return carry

        lax.fori_loop(0, leaves // group, accumulate, 0)


def diagonal_update(heads, cb, leaves, rows):
    group = min(leaves, 8)

    def body(*refs):
        diagonal_kernel(cb, leaves, *refs)

    return pl.pallas_call(
        body,
        name="diagonal",
        out_shape=[
            jax.ShapeDtypeStruct((cb * rows, rows), jnp.float32),
            jax.ShapeDtypeStruct((leaves, rows), jnp.int32),
        ],
        in_specs=spaces(len(heads), pltpu.VMEM),
        out_specs=spaces(2, pltpu.VMEM),
        scratch_shapes=[
            pltpu.VMEM((cb * rows, group * SLOTS * rows), heads[0].dtype),
            pltpu.VMEM((rows, group * SLOTS * rows), heads[0].dtype),
        ],
        cost_estimate=pl.CostEstimate(flops=2000000000, bytes_accessed=1000000, transcendentals=0),
    )(*heads)


def below_kernel(cb, blk_count, per, leaves, count, codes, tails_hbm, *refs):
    heads = refs[:count]
    outs = refs[count:count + blk_count * HALVES]
    acc, products, tails, sems = refs[count + blk_count * HALVES:]
    direct = count > 1
    me_leaf = lax.axis_index("leaf")
    me_blk = lax.axis_index("blk")
    rows = acc.shape[1]
    group = min(leaves, 8)
    tail_rows = tails.shape[1] // SLOTS
    extra = tail_rows // rows
    blocks = blk_count * cb * per

    def source(index):
        return jnp.bitwise_xor(me_leaf, index) if direct else index

    def fetch(index, slot):
        return pltpu.make_async_copy(tails_hbm.at[source(index)], tails.at[slot], sems.at[slot])

    def step(base):
        for offset in range(group):
            fetch(base + offset, offset).start()

        @pl.when(base == 0)
        def _():
            for first in range(0, blocks, cb):
                acc[pl.ds(first, cb)] = jnp.zeros((cb, rows, rows), jnp.float32)

        for offset in range(group):
            index = base + offset
            fetch(index, offset).wait()
            for slot in range(SLOTS):
                if direct:
                    head = heads[index][pl.ds(slot * rows, rows)]
                else:
                    head = heads[0][index, pl.ds(slot * rows, rows)]
                tail = tails[offset, pl.ds(slot * tail_rows, tail_rows)]
                products[offset * SLOTS + slot] = lax.dot_general(
                    tail, head, (((1,), (1,)), ((), ())), preferred_element_type=jnp.float32
                )
        for offset in range(group):
            for slot in range(SLOTS):
                column = codes[base + offset, slot * CODES]
                for r in range(extra):
                    position = codes[base + offset, slot * CODES + 1 + r]
                    relative = jnp.bitwise_xor(lax.rem(position, blk_count), me_blk)
                    place = (relative * cb + column) * per + lax.div(position, blk_count)
                    place = jnp.where(column < cb, place, blocks)
                    acc[place] += products[offset * SLOTS + slot, pl.ds(r * rows, rows)]

    if leaves == group:
        step(0)
    else:
        lax.fori_loop(0, leaves // group, lambda index, carry: (step(index * group), carry)[1], 0)
    size = cb * per // HALVES
    for part, out in enumerate(outs):
        out[...] = acc[pl.ds(part * size, size)]


def below_update(heads, tails, codes, cb, blk_count, per, leaves, rows):
    group = min(leaves, 8)
    blocks = blk_count * cb * per
    outs = blk_count * HALVES

    def body(*refs):
        below_kernel(cb, blk_count, per, leaves, len(heads), *refs)

    return pl.pallas_call(
        body,
        name="below",
        out_shape=[jax.ShapeDtypeStruct((cb * per // HALVES, rows, rows), jnp.float32)] * outs,
        in_specs=spaces(1, pltpu.SMEM) + spaces(1, pl.ANY) + spaces(len(heads), pltpu.VMEM),
        out_specs=spaces(outs, pltpu.VMEM),
        scratch_shapes=[
            pltpu.VMEM((blocks + 1, rows, rows), jnp.float32),
            pltpu.VMEM((group * SLOTS, tails.shape[1] // SLOTS, rows), jnp.float32),
            pltpu.VMEM((group,) + tails.shape[1:], tails.dtype),
            pltpu.SemaphoreType.DMA((group,)),
        ],
        cost_estimate=pl.CostEstimate(flops=2000000000, bytes_accessed=4000000, transcendentals=0),
    )(codes, tails, *heads)


def factor_block(work, rows):
    lane = lax.broadcasted_iota(jnp.int32, (1, rows), 1)
    sub = lax.broadcasted_iota(jnp.int32, (PANEL, 1), 0)
    segments = 4
    size = rows // segments

    for segment in range(segments):
        top = segment * size

        def panel(index, carry):
            base = pl.multiple_of(top + index * PANEL, PANEL)
            strip = work[pl.ds(base, PANEL), :]
            picks = [(lane == base + k) for k in range(PANEL)]
            corner = [
                jnp.sum(jnp.where(picks[k], strip[:, :rows], 0.0), axis=1, keepdims=True)
                for k in range(PANEL)
            ]
            scales = []
            for k in range(PANEL):
                scale = lax.rsqrt(corner[k][k:k + 1])
                scales.append(scale)
                row = strip[k:k + 1] * scale
                low = jnp.where(sub > k, corner[k] * scale, 0.0)
                strip = jnp.where(sub == k, row, strip - low * row)
                for m in range(k, PANEL):
                    entry = corner[m][k:k + 1] * scale
                    corner[m] = jnp.where(sub == k, entry, corner[m] - low * entry)
            full = work[pl.ds(top, rows - top), :rows]
            work[pl.ds(base, PANEL), :] = strip
            rest = lax.broadcasted_iota(jnp.int32, (rows - top, 1), 0) + top >= base + PANEL
            total = jnp.zeros((rows - top, 2 * rows), jnp.float32)
            for k in reversed(range(PANEL)):
                solved = strip[k:k + 1] * scales[k]
                strip = strip - jnp.where(sub < k, corner[k], 0.0) * solved
                column = jnp.sum(jnp.where(picks[k], full, 0.0), axis=1, keepdims=True)
                total = total + jnp.where(rest, column, 0.0) * solved
            work[pl.ds(top, rows - top), :] -= total
            return carry

        lax.fori_loop(0, size // PANEL, panel, 0)


def eliminate(schur, inverses, work, block, cb, rows):
    eye = lax.broadcasted_iota(jnp.int32, (rows, rows), 0) == lax.broadcasted_iota(
        jnp.int32, (rows, rows), 1
    )
    upper = lax.broadcasted_iota(jnp.int32, (rows, rows), 0) <= lax.broadcasted_iota(
        jnp.int32, (rows, rows), 1
    )
    here = block * rows
    work[:, :rows] = schur[block, :, here:here + rows]
    work[:, rows:] = eye.astype(jnp.float32)
    factor_block(work, rows)
    schur[block, :, here:here + rows] = jnp.where(upper, work[:, :rows], 0.0)
    inverse = work[:, rows:]
    inverses[block] = inverse
    if block + 1 < cb:
        after = here + rows
        strip = lax.dot_general(
            inverse, schur[block, :, after:], (((1,), (0,)), ((), ())),
            precision=HIGHEST, preferred_element_type=jnp.float32,
        )
        schur[block, :, after:] = strip
        for other in range(block + 1, cb):
            offset = (other - block - 1) * rows
            schur[other, :, other * rows:] -= lax.dot_general(
                strip[:, offset:offset + rows], strip[:, offset:], (((0,), (0,)), ((), ())),
                precision=HIGHEST, preferred_element_type=jnp.float32,
            )


def first_factor(own_sum, other_sum, strips, cb, rows):
    blk_count = len(strips)

    def body(own_ref, other_ref, *refs):
        strip_refs = refs[:blk_count]
        schur, inverses, work = refs[blk_count:]
        me = lax.axis_index("blk")
        for x in range(blk_count):
            schur[jnp.bitwise_xor(me, x)] = strip_refs[x][...]
        for c in range(cb):
            part = slice(c * rows, (c + 1) * rows)
            schur[c, :, part] -= own_ref[part] + other_ref[part]
        for block in range(cb // SPLIT):
            eliminate(schur, inverses, work, block, cb, rows)

    return pl.pallas_call(
        body,
        name="factor_first",
        out_shape=[
            jax.ShapeDtypeStruct((cb, rows, cb * rows), jnp.float32),
            jax.ShapeDtypeStruct((cb, rows, rows), jnp.float32),
        ],
        in_specs=spaces(2 + blk_count, pltpu.VMEM),
        out_specs=spaces(2, pltpu.VMEM),
        scratch_shapes=[pltpu.VMEM((rows, 2 * rows), jnp.float32)],
        cost_estimate=pl.CostEstimate(flops=10000000000, bytes_accessed=2000000, transcendentals=0),
    )(own_sum, other_sum, *strips)


def last_factor(schur_in, inverses_in, cb, rows):
    width = cb * rows

    def body(schur_ref, inverses_ref, whole, lower, schur, inverses, work):
        me = lax.axis_index("blk")
        schur[...] = schur_ref[...]
        for block in range(cb // SPLIT):
            inverses[block] = inverses_ref[block]
        for block in range(cb // SPLIT, cb):
            eliminate(schur, inverses, work, block, cb, rows)
        for k in range(cb):
            piece = jnp.where(k <= me, schur[k, :, pl.ds(pl.multiple_of(me * rows, rows), rows)], 0.0)
            lower[:, k * rows:(k + 1) * rows] = piece.T
        whole[...] = jnp.zeros_like(whole)
        for i in range(cb):
            whole[i * rows:(i + 1) * rows, i * rows:(i + 1) * rows] = inverses[i]
            if i:
                done = slice(0, i * rows)
                total = jnp.zeros((rows, i * rows), jnp.float32)
                for k in range(i):
                    total = total + lax.dot_general(
                        schur[k, :, i * rows:(i + 1) * rows],
                        whole[k * rows:(k + 1) * rows, done],
                        (((0,), (0,)), ((), ())),
                        precision=HIGHEST, preferred_element_type=jnp.float32,
                    )
                whole[i * rows:(i + 1) * rows, done] = -lax.dot_general(
                    inverses[i], total, (((1,), (0,)), ((), ())),
                    precision=HIGHEST, preferred_element_type=jnp.float32,
                )

    return pl.pallas_call(
        body,
        name="factor_last",
        out_shape=[
            jax.ShapeDtypeStruct((width, width), jnp.float32),
            jax.ShapeDtypeStruct((rows, width), jnp.float32),
        ],
        in_specs=spaces(2, pltpu.VMEM),
        out_specs=spaces(2, pltpu.VMEM),
        scratch_shapes=[
            pltpu.VMEM((cb, rows, width), jnp.float32),
            pltpu.VMEM((cb, rows, rows), jnp.float32),
            pltpu.VMEM((rows, 2 * rows), jnp.float32),
        ],
        cost_estimate=pl.CostEstimate(flops=12000000000, bytes_accessed=2000000, transcendentals=0),
    )(schur_in, inverses_in)


def solve_dot(left, right):
    return lax.dot_general(
        left, right, (((1,), (1,)), ((), ())),
        precision=HIGHEST, preferred_element_type=jnp.float32,
    )


def remaining(panel_ref, update_refs, half, cb, per, rows):
    parts = []
    for c in range(cb // HALVES):
        column = (half * (cb // HALVES) + c) * rows
        block = slice(c * per, (c + 1) * per)
        update = update_refs[0][block]
        for ref in update_refs[1:]:
            update = update + ref[block]
        original = panel_ref[1:, :, column:column + rows]
        parts.append((original - update).reshape(per * rows, rows))
    return jnp.concatenate(parts, axis=1)


def solve_left(panel, updates, whole, lower, cb, per, rows):
    width = cb * rows
    half = width // HALVES

    def body(panel_ref, *refs):
        updates_ref = refs[:len(updates)]
        whole_ref, lower_ref, out, carried = refs[len(updates):]
        left = remaining(panel_ref, updates_ref, 0, cb, per, rows)
        out[0] = lower_ref[...]
        out[1:, :, :half] = solve_dot(left, whole_ref[:half, :half]).reshape(per, rows, half)
        carried[...] = solve_dot(left, whole_ref[half:, :half])

    return pl.pallas_call(
        body,
        name="solve_left",
        out_shape=[
            jax.ShapeDtypeStruct((per + 1, rows, width), jnp.float32),
            jax.ShapeDtypeStruct((per * rows, half), jnp.float32),
        ],
        in_specs=spaces(3 + len(updates), pltpu.VMEM),
        out_specs=spaces(2, pltpu.VMEM),
        cost_estimate=pl.CostEstimate(flops=2000000000, bytes_accessed=5000000, transcendentals=0),
    )(panel, *updates, whole, lower)


def solve_right(panel, updates, whole, carried, out, cb, per, rows):
    width = cb * rows
    half = width // HALVES

    def body(panel_ref, *refs):
        updates_ref = refs[:len(updates)]
        whole_ref, carried_ref, _, result, stage, sem = refs[len(updates):]
        left = remaining(panel_ref, updates_ref, 1, cb, per, rows)
        value = carried_ref[...] + solve_dot(left, whole_ref[half:, half:])
        stage[...] = value.reshape(per, rows, half)
        copy = pltpu.make_async_copy(
            stage, result.at[pl.ds(1, per), :, pl.ds(half, half)], sem
        )
        copy.start()
        copy.wait()

    return pl.pallas_call(
        body,
        name="solve_right",
        out_shape=jax.ShapeDtypeStruct((per + 1, rows, width), jnp.float32),
        in_specs=spaces(3 + len(updates), pltpu.VMEM) + spaces(1, pl.ANY),
        out_specs=pl.BlockSpec(memory_space=pl.ANY),
        scratch_shapes=[pltpu.VMEM((per, rows, half), jnp.float32), pltpu.SemaphoreType.DMA(())],
        input_output_aliases={3 + len(updates): 0},
        cost_estimate=pl.CostEstimate(flops=2000000000, bytes_accessed=5000000, transcendentals=0),
    )(panel, *updates, whole, carried, out)


def shards(desc_panel, row_map, anc_order, anc_below, anc_panel):
    leaves = lax.axis_size("leaf")
    blk_count = lax.axis_size("blk")
    rows = anc_panel.shape[3]
    width = anc_panel.shape[4]
    cb = width // rows
    per = anc_below.shape[1] // blk_count
    assert cb == blk_count == 4 and desc_panel.shape[2] == rows
    direct = leaves <= DIRECT and leaves & (leaves - 1) == 0
    near = [(i, i ^ 1) for i in range(blk_count)]
    far = [(i, i ^ 2) for i in range(blk_count)]

    *heads, tails = pack(desc_panel, row_map, anc_order, anc_below, cb, direct)
    if direct:
        heads = [heads[0]] + [
            lax.ppermute(heads[k], "leaf", [(i, i ^ k) for i in range(leaves)])
            for k in range(1, leaves)
        ]
    else:
        heads = [lax.all_to_all(heads[0], "leaf", split_axis=0, concat_axis=0, tiled=True)]
    tails = lax.all_to_all(tails, "leaf", split_axis=0, concat_axis=0, tiled=True)

    panel = anc_panel.reshape(per + 1, rows, width)
    strip = panel[0]
    strip_far = lax.ppermute(strip, "blk", far)
    strip_near = lax.ppermute(strip, "blk", near)
    strip_both = lax.ppermute(strip_far, "blk", near)
    strips = [strip, strip_near, strip_far, strip_both]

    diagonal, codes = diagonal_update(heads, cb, leaves, rows)
    diagonal_near = lax.ppermute(diagonal, "blk", near)
    diagonal = diagonal + diagonal_near
    diagonal_far = lax.ppermute(diagonal, "blk", far)
    schur, inverses = first_factor(diagonal, diagonal_far, strips, cb, rows)

    partials = below_update(heads, tails, codes, cb, blk_count, per, leaves, rows)
    kept, for_near, for_far, for_both = (
        partials[HALVES * x:HALVES * (x + 1)] for x in range(blk_count)
    )
    from_near = []
    from_far = []
    for half in range(HALVES):
        passed = lax.ppermute(for_both[half], "blk", near)
        from_far.append(lax.ppermute(for_far[half] + passed, "blk", far))
    for half in range(HALVES):
        from_near.append(lax.ppermute(for_near[half], "blk", near))
    whole, lower = last_factor(schur, inverses, cb, rows)
    updates = [[kept[half], from_near[half], from_far[half]] for half in range(HALVES)]
    out, carried = solve_left(panel, updates[0], whole, lower, cb, per, rows)
    out = solve_right(panel, updates[1], whole, carried, out, cb, per, rows)
    return out.reshape(anc_panel.shape)


def solution(mesh):
    in_specs = (
        P(("leaf", "blk"), None, None),
        P(("leaf", "blk"), None),
        P(),
        P(),
        P("leaf", None, "blk", None, None),
    )
    out_specs = P("leaf", None, "blk", None, None)

    return jax.shard_map(shards, mesh=mesh, in_specs=in_specs, out_specs=out_specs, check_vma=False)
```

```python
import jax
import jax.numpy as jnp
from jax import lax
from jax.experimental import pallas as pl
from jax.experimental.pallas import tpu as pltpu
from jax.sharding import PartitionSpec as P


SLOTS = 2
CODES = 4
CODE_ROWS = 16
PANEL = 8
SPLIT = 2
HALVES = 2
DIRECT = 8
HIGHEST = lax.Precision.HIGHEST


def repeat(count, body, unroll_to=16):
    if count <= unroll_to:
        for index in range(count):
            body(index)
    else:
        lax.fori_loop(0, count, lambda index, carry: (body(index), carry)[1], 0)


def limit(mib):
    return pltpu.CompilerParams(vmem_limit_bytes=mib * 1024 * 1024)


def near_core(*arrays):
    return [pltpu.with_memory_space_constraint(array, pltpu.VMEM) for array in arrays]


def spaces(count, space):
    return [pl.BlockSpec(memory_space=space)] * count


def pack_kernel(cb, nb, direct, row_map, anc_order, anc_below, panel, *refs):
    leaves = anc_order.shape[0]
    block_count, desc_count = row_map.shape
    rows = panel.shape[1] // block_count
    outs = refs[: leaves if direct else 1]
    tail_out, inverse, used, chosen, codes, tail_sem = refs[len(outs):]
    me = lax.axis_index("leaf")

    def clear(leaf):
        inverse[anc_order[leaf]] = leaf
        used[leaf] = 0
        for slot in range(SLOTS):
            chosen[leaf * SLOTS + slot] = -1
            codes[(leaf * SLOTS + slot) * CODES] = cb
            for r in range(1, CODES):
                codes[(leaf * SLOTS + slot) * CODES + r] = nb

    repeat(leaves, clear)

    def assign(desc):
        head = row_map[0, desc]
        leaf = inverse[lax.div(head, cb)]
        taken = used[leaf]
        used[leaf] = taken + 1
        place = leaf * SLOTS + taken
        chosen[place] = desc
        codes[place * CODES] = head - anc_order[leaf] * cb
        for r in range(1, block_count):
            target = row_map[r, desc]
            found = jnp.int32(nb)
            for q in range(anc_below.shape[1]):
                found = jnp.where(anc_below[leaf, q] == target, q, found)
            codes[place * CODES + r] = found

    repeat(desc_count, assign)

    def dest(index):
        return jnp.bitwise_xor(me, index) if direct else index

    def tail_copy(index, slot):
        leaf = dest(index)
        desc = chosen[leaf * SLOTS + slot]
        tail_rows = (block_count - 1) * rows
        return desc, pltpu.make_async_copy(
            panel.at[jnp.maximum(desc, 0), pl.ds(rows, tail_rows)],
            tail_out.at[leaf, pl.ds(slot * tail_rows, tail_rows)],
            tail_sem.at[index, slot],
        )

    def start(index):
        for slot in range(SLOTS):
            desc, copy = tail_copy(index, slot)

            @pl.when(desc >= 0)
            def _():
                copy.start()

    repeat(leaves, start)

    def write_head(index):
        leaf = dest(index)
        row = lax.broadcasted_iota(jnp.int32, (CODE_ROWS, 128), 0)
        values = jnp.zeros((CODE_ROWS, 128), jnp.int32)
        for entry in range(SLOTS * CODES):
            values = jnp.where(row == entry, codes[leaf * SLOTS * CODES + entry], values)
        values = values.astype(jnp.float32).astype(panel.dtype)
        for slot in range(SLOTS):
            desc = jnp.maximum(chosen[leaf * SLOTS + slot], 0)
            block = panel[desc, pl.ds(0, rows)]
            if direct:
                outs[index][pl.ds(slot * rows, rows)] = block
            else:
                outs[0][index, pl.ds(slot * rows, rows)] = block
        if direct:
            outs[index][pl.ds(SLOTS * rows, CODE_ROWS)] = values
        else:
            outs[0][index, pl.ds(SLOTS * rows, CODE_ROWS)] = values

    repeat(leaves, write_head)

    def finish(index):
        for slot in range(SLOTS):
            desc, copy = tail_copy(index, slot)

            @pl.when(desc >= 0)
            def _():
                copy.wait()

    repeat(leaves, finish)


def pack(desc_panel, row_map, anc_order, anc_below, cb, direct):
    leaves = anc_order.shape[0]
    block_count = row_map.shape[1]
    rows = desc_panel.shape[1] // block_count
    width = desc_panel.shape[2]
    head_rows = SLOTS * rows + CODE_ROWS
    dtype = desc_panel.dtype
    if direct:
        heads = [pltpu.VMEM((head_rows, width), dtype)] * leaves
    else:
        heads = [jax.ShapeDtypeStruct((leaves, head_rows, width), dtype)]
    tails = jax.ShapeDtypeStruct((leaves, SLOTS * (block_count - 1) * rows, width), dtype)
    nb = anc_below.shape[1]

    def body(*refs):
        pack_kernel(cb, nb, direct, *refs)

    return pl.pallas_call(
        body,
        name="pack",
        compiler_params=limit(12 if direct else 32),
        out_shape=heads + [tails],
        in_specs=spaces(3, pltpu.SMEM) + spaces(1, pltpu.VMEM),
        out_specs=spaces(len(heads), pltpu.VMEM) + spaces(1, pl.ANY),
        scratch_shapes=[
            pltpu.SMEM((leaves,), jnp.int32),
            pltpu.SMEM((leaves,), jnp.int32),
            pltpu.SMEM((leaves * SLOTS,), jnp.int32),
            pltpu.SMEM((leaves * SLOTS * CODES,), jnp.int32),
            pltpu.SemaphoreType.DMA((leaves, SLOTS)),
        ],
    )(row_map.T, anc_order, anc_below, desc_panel)


def diagonal_kernel(cb, leaves, *refs):
    heads = refs[:-4]
    out, codes, left, right = refs[-4:]
    direct = len(heads) > 1
    rows = out.shape[1]
    group = min(leaves, 8)

    def load(index, start, size):
        if direct:
            return heads[index][pl.ds(start, size)]
        return heads[0][index, pl.ds(start, size)]

    lane = lax.broadcasted_iota(jnp.int32, (1, rows), 1)

    def step(base):
        for offset in range(group):
            marks = load(base + offset, SLOTS * rows, CODE_ROWS).astype(jnp.float32)
            packed = jnp.zeros((1, rows), jnp.float32)
            for entry in range(SLOTS * CODES):
                packed = jnp.where(lane == entry, marks[entry:entry + 1], packed)
            codes[pl.ds(base + offset, 1)] = packed.astype(jnp.int32)
            for slot in range(SLOTS):
                block = load(base + offset, slot * rows, rows)
                lanes = pl.ds((offset * SLOTS + slot) * rows, rows)
                code = jnp.broadcast_to(marks[slot * CODES:slot * CODES + 1], (rows, rows))
                code = code.astype(block.dtype)
                zero = jnp.zeros_like(block)
                right[:, lanes] = jnp.where(code < cb, block, zero)
                for c in range(cb):
                    left[c * rows:(c + 1) * rows, lanes] = jnp.where(code == c, block, zero)
        return lax.dot_general(
            left[...], right[...], (((1,), (1,)), ((), ())), preferred_element_type=jnp.float32
        )

    if leaves == group:
        out[...] = step(0).reshape(out.shape)
    else:
        out[...] = jnp.zeros_like(out)

        def accumulate(index, carry):
            out[...] += step(index * group).reshape(out.shape)
            return carry

        lax.fori_loop(0, leaves // group, accumulate, 0)


def diagonal_update(heads, cb, leaves, rows):
    group = min(leaves, 8)

    def body(*refs):
        diagonal_kernel(cb, leaves, *refs)

    return pl.pallas_call(
        body,
        name="diagonal",
        compiler_params=limit(12 if len(heads) > 1 else 40),
        out_shape=[
            pltpu.VMEM((cb * rows, rows), jnp.float32),
            jax.ShapeDtypeStruct((leaves, rows), jnp.int32),
        ],
        in_specs=spaces(len(heads), pltpu.VMEM),
        out_specs=spaces(2, pltpu.VMEM),
        scratch_shapes=[
            pltpu.VMEM((cb * rows, group * SLOTS * rows), heads[0].dtype),
            pltpu.VMEM((rows, group * SLOTS * rows), heads[0].dtype),
        ],
        cost_estimate=pl.CostEstimate(flops=2000000000, bytes_accessed=1000000, transcendentals=0),
    )(*(near_core(*heads) if len(heads) > 1 else heads))


def below_kernel(cb, blk_count, per, leaves, count, codes, tails, *refs):
    heads = refs[:count]
    outs = refs[count:count + blk_count * HALVES]
    acc, products = refs[count + blk_count * HALVES:]
    direct = count > 1
    me_leaf = lax.axis_index("leaf")
    me_blk = lax.axis_index("blk")
    rows = acc.shape[1]
    group = min(leaves, 8)
    tail_rows = tails.shape[1] // SLOTS
    extra = tail_rows // rows
    blocks = blk_count * cb * per

    for first in range(0, blocks, cb):
        acc[pl.ds(first, cb)] = jnp.zeros((cb, rows, rows), jnp.float32)

    def step(base):
        for offset in range(group):
            index = base + offset
            source = jnp.bitwise_xor(me_leaf, index) if direct else index
            for slot in range(SLOTS):
                if direct:
                    head = heads[index][pl.ds(slot * rows, rows)]
                else:
                    head = heads[0][index, pl.ds(slot * rows, rows)]
                tail = tails[source, pl.ds(slot * tail_rows, tail_rows)]
                products[offset * SLOTS + slot] = lax.dot_general(
                    tail, head, (((1,), (1,)), ((), ())), preferred_element_type=jnp.float32
                )
        for offset in range(group):
            for slot in range(SLOTS):
                column = codes[base + offset, slot * CODES]
                for r in range(extra):
                    position = codes[base + offset, slot * CODES + 1 + r]
                    relative = jnp.bitwise_xor(lax.rem(position, blk_count), me_blk)
                    place = (relative * cb + column) * per + lax.div(position, blk_count)
                    place = jnp.where(column < cb, place, blocks)
                    acc[place] += products[offset * SLOTS + slot, pl.ds(r * rows, rows)]

    if leaves == group:
        step(0)
    else:
        lax.fori_loop(0, leaves // group, lambda index, carry: (step(index * group), carry)[1], 0)
    size = cb * per // HALVES
    for part, out in enumerate(outs):
        out[...] = acc[pl.ds(part * size, size)]


def below_update(heads, tails, codes, cb, blk_count, per, leaves, rows):
    group = min(leaves, 8)
    blocks = blk_count * cb * per
    outs = blk_count * HALVES

    def body(*refs):
        below_kernel(cb, blk_count, per, leaves, len(heads), *refs)

    return pl.pallas_call(
        body,
        name="below",
        compiler_params=limit(16 if len(heads) > 1 else 56),
        out_shape=[pltpu.VMEM((cb * per // HALVES, rows, rows), jnp.float32)] * outs,
        in_specs=spaces(1, pltpu.SMEM) + spaces(1 + len(heads), pltpu.VMEM),
        out_specs=spaces(outs, pltpu.VMEM),
        scratch_shapes=[
            pltpu.VMEM((blocks + 1, rows, rows), jnp.float32),
            pltpu.VMEM((group * SLOTS, tails.shape[1] // SLOTS, rows), jnp.float32),
        ],
        cost_estimate=pl.CostEstimate(flops=2000000000, bytes_accessed=4000000, transcendentals=0),
    )(codes, *(near_core(tails, *heads) if len(heads) > 1 else [tails, *heads]))


def factor_block(work, rows):
    lane = lax.broadcasted_iota(jnp.int32, (1, rows), 1)
    sub = lax.broadcasted_iota(jnp.int32, (PANEL, 1), 0)
    segments = 4
    size = rows // segments

    for segment in range(segments):
        top = segment * size

        def panel(index, carry):
            base = pl.multiple_of(top + index * PANEL, PANEL)
            strip = work[pl.ds(base, PANEL), :]
            raw = work[top:, :rows]
            picks = [(lane == base + k) for k in range(PANEL)]
            corner = [
                jnp.sum(jnp.where(picks[k], strip[:, :rows], 0.0), axis=1, keepdims=True)
                for k in range(PANEL)
            ]
            factor = jnp.zeros((PANEL, 2 * rows), jnp.float32)
            for k in range(PANEL):
                scale = lax.rsqrt(corner[k][k:k + 1])
                inverse = scale * scale
                row = strip[k:k + 1]
                factor = jnp.where(sub == k, row * scale, factor)
                scaled = row * inverse
                strip = jnp.where(sub == k, scaled, strip - corner[k] * scaled)
                for m in range(k + 1, PANEL):
                    entry = corner[m][k:k + 1]
                    corner[m] = jnp.where(
                        sub == k, entry * inverse, corner[m] - (corner[k] * entry) * inverse
                    )
            work[pl.ds(base, PANEL), :] = factor
            for start, stop, masked in ((top, top + size, True), (top + size, rows, False)):
                if start == stop:
                    continue
                full = work[start:stop, :]
                row_id = lax.broadcasted_iota(jnp.int32, (stop - start, 1), 0) + start
                for k in range(PANEL):
                    column = jnp.sum(
                        jnp.where(picks[k], raw[start - top:stop - top], 0.0), axis=1, keepdims=True
                    )
                    if masked:
                        column = jnp.where(row_id >= base + PANEL, column, 0.0)
                    full = full - column * strip[k:k + 1]
                work[start:stop, :] = full
            return carry

        lax.fori_loop(0, size // PANEL, panel, 0)


def eliminate(schur, inverses, work, block, cb, rows):
    eye = lax.broadcasted_iota(jnp.int32, (rows, rows), 0) == lax.broadcasted_iota(
        jnp.int32, (rows, rows), 1
    )
    upper = lax.broadcasted_iota(jnp.int32, (rows, rows), 0) <= lax.broadcasted_iota(
        jnp.int32, (rows, rows), 1
    )
    here = block * rows
    work[:, :rows] = schur[block, :, here:here + rows]
    work[:, rows:] = eye.astype(jnp.float32)
    factor_block(work, rows)
    schur[block, :, here:here + rows] = jnp.where(upper, work[:, :rows], 0.0)
    inverse = work[:, rows:]
    inverses[block] = inverse
    if block + 1 < cb:
        after = here + rows
        strip = lax.dot_general(
            inverse, schur[block, :, after:], (((1,), (0,)), ((), ())),
            precision=HIGHEST, preferred_element_type=jnp.float32,
        )
        schur[block, :, after:] = strip
        for other in range(block + 1, cb):
            offset = (other - block - 1) * rows
            schur[other, :, other * rows:] -= lax.dot_general(
                strip[:, offset:offset + rows], strip[:, offset:], (((0,), (0,)), ((), ())),
                precision=HIGHEST, preferred_element_type=jnp.float32,
            )


def first_factor(own_sum, other_sum, strips, cb, rows):
    blk_count = len(strips)

    def body(own_ref, other_ref, *refs):
        strip_refs = refs[:blk_count]
        schur, inverses, work = refs[blk_count:]
        me = lax.axis_index("blk")
        for x in range(blk_count):
            schur[jnp.bitwise_xor(me, x)] = strip_refs[x][...]
        for c in range(cb):
            part = slice(c * rows, (c + 1) * rows)
            schur[c, :, part] -= own_ref[part] + other_ref[part]
        for block in range(cb // SPLIT):
            eliminate(schur, inverses, work, block, cb, rows)

    return pl.pallas_call(
        body,
        name="factor_first",
        compiler_params=limit(12),
        out_shape=[
            pltpu.VMEM((cb, rows, cb * rows), jnp.float32),
            pltpu.VMEM((cb, rows, rows), jnp.float32),
        ],
        in_specs=spaces(2 + blk_count, pltpu.VMEM),
        out_specs=spaces(2, pltpu.VMEM),
        scratch_shapes=[pltpu.VMEM((rows, 2 * rows), jnp.float32)],
        cost_estimate=pl.CostEstimate(flops=10000000000, bytes_accessed=2000000, transcendentals=0),
    )(*near_core(own_sum, other_sum), strips[0], *near_core(*strips[1:]))


def last_factor(schur_in, inverses_in, cb, rows):
    width = cb * rows

    def body(schur_ref, inverses_ref, whole, lower, schur, inverses, work):
        me = lax.axis_index("blk")
        schur[...] = schur_ref[...]
        for block in range(cb // SPLIT):
            inverses[block] = inverses_ref[block]
        for block in range(cb // SPLIT, cb):
            eliminate(schur, inverses, work, block, cb, rows)
        for k in range(cb):
            piece = jnp.where(k <= me, schur[k, :, pl.ds(pl.multiple_of(me * rows, rows), rows)], 0.0)
            lower[:, k * rows:(k + 1) * rows] = piece.T
        whole[...] = jnp.zeros_like(whole)
        for i in range(cb):
            whole[i * rows:(i + 1) * rows, i * rows:(i + 1) * rows] = inverses[i]
            if i:
                done = slice(0, i * rows)
                total = jnp.zeros((rows, i * rows), jnp.float32)
                for k in range(i):
                    total = total + lax.dot_general(
                        schur[k, :, i * rows:(i + 1) * rows],
                        whole[k * rows:(k + 1) * rows, done],
                        (((0,), (0,)), ((), ())),
                        precision=HIGHEST, preferred_element_type=jnp.float32,
                    )
                whole[i * rows:(i + 1) * rows, done] = -lax.dot_general(
                    inverses[i], total, (((1,), (0,)), ((), ())),
                    precision=HIGHEST, preferred_element_type=jnp.float32,
                )

    return pl.pallas_call(
        body,
        name="factor_last",
        compiler_params=limit(12),
        out_shape=[
            pltpu.VMEM((width, width), jnp.float32),
            pltpu.VMEM((rows, width), jnp.float32),
        ],
        in_specs=spaces(2, pltpu.VMEM),
        out_specs=spaces(2, pltpu.VMEM),
        scratch_shapes=[
            pltpu.VMEM((cb, rows, width), jnp.float32),
            pltpu.VMEM((cb, rows, rows), jnp.float32),
            pltpu.VMEM((rows, 2 * rows), jnp.float32),
        ],
        cost_estimate=pl.CostEstimate(flops=12000000000, bytes_accessed=2000000, transcendentals=0),
    )(*near_core(schur_in, inverses_in))


def solve_dot(left, right):
    return lax.dot_general(
        left, right, (((1,), (1,)), ((), ())),
        precision=HIGHEST, preferred_element_type=jnp.float32,
    )


def remaining(panel_ref, update_refs, half, cb, per, rows):
    parts = []
    for c in range(cb // HALVES):
        column = (half * (cb // HALVES) + c) * rows
        block = slice(c * per, (c + 1) * per)
        update = update_refs[0][block]
        for ref in update_refs[1:]:
            update = update + ref[block]
        original = panel_ref[1:, :, column:column + rows]
        parts.append((original - update).reshape(per * rows, rows))
    return jnp.concatenate(parts, axis=1)


def solve_left(panel, updates, whole, lower, cb, per, rows):
    width = cb * rows
    half = width // HALVES

    def body(panel_ref, *refs):
        updates_ref = refs[:len(updates)]
        whole_ref, lower_ref, out, carried = refs[len(updates):]
        left = remaining(panel_ref, updates_ref, 0, cb, per, rows)
        out[0] = lower_ref[...]
        out[1:, :, :half] = solve_dot(left, whole_ref[:half, :half]).reshape(per, rows, half)
        carried[...] = solve_dot(left, whole_ref[half:, :half])

    return pl.pallas_call(
        body,
        name="solve_left",
        compiler_params=limit(16),
        out_shape=[
            jax.ShapeDtypeStruct((per + 1, rows, width), jnp.float32),
            pltpu.VMEM((per * rows, half), jnp.float32),
        ],
        in_specs=spaces(3 + len(updates), pltpu.VMEM),
        out_specs=spaces(2, pltpu.VMEM),
        cost_estimate=pl.CostEstimate(flops=2000000000, bytes_accessed=5000000, transcendentals=0),
    )(panel, *near_core(*updates, whole, lower))


def solve_right(panel, updates, whole, carried, out, cb, per, rows):
    width = cb * rows
    half = width // HALVES

    def body(panel_ref, *refs):
        updates_ref = refs[:len(updates)]
        whole_ref, carried_ref, _, result, stage, sem = refs[len(updates):]
        left = remaining(panel_ref, updates_ref, 1, cb, per, rows)
        value = carried_ref[...] + solve_dot(left, whole_ref[half:, half:])
        stage[...] = value.reshape(per, rows, half)
        copy = pltpu.make_async_copy(
            stage, result.at[pl.ds(1, per), :, pl.ds(half, half)], sem
        )
        copy.start()
        copy.wait()

    return pl.pallas_call(
        body,
        name="solve_right",
        compiler_params=limit(16),
        out_shape=jax.ShapeDtypeStruct((per + 1, rows, width), jnp.float32),
        in_specs=spaces(3 + len(updates), pltpu.VMEM) + spaces(1, pl.ANY),
        out_specs=pl.BlockSpec(memory_space=pl.ANY),
        scratch_shapes=[pltpu.VMEM((per, rows, half), jnp.float32), pltpu.SemaphoreType.DMA(())],
        input_output_aliases={3 + len(updates): 0},
        cost_estimate=pl.CostEstimate(flops=2000000000, bytes_accessed=5000000, transcendentals=0),
    )(panel, *near_core(*updates, whole, carried), out)


def shards(desc_panel, row_map, anc_order, anc_below, anc_panel):
    leaves = lax.axis_size("leaf")
    blk_count = lax.axis_size("blk")
    rows = anc_panel.shape[3]
    width = anc_panel.shape[4]
    cb = width // rows
    per = anc_below.shape[1] // blk_count
    assert cb == blk_count == 4 and desc_panel.shape[2] == rows
    direct = leaves <= DIRECT and leaves & (leaves - 1) == 0
    near = [(i, i ^ 1) for i in range(blk_count)]
    far = [(i, i ^ 2) for i in range(blk_count)]

    *heads, tails = pack(desc_panel, row_map, anc_order, anc_below, cb, direct)
    if direct:
        received = [heads[0]]
        for k in range(1, leaves):
            swap = [(i, i ^ k) for i in range(leaves)]
            received.append(lax.ppermute(heads[k], "leaf", swap))
        heads = received
    else:
        heads = [lax.all_to_all(heads[0], "leaf", split_axis=0, concat_axis=0, tiled=True)]
    tails = lax.all_to_all(tails, "leaf", split_axis=0, concat_axis=0, tiled=True)

    panel = anc_panel.reshape(per + 1, rows, width)
    strip = panel[0]
    strip_far = lax.ppermute(strip, "blk", far)
    strip_near = lax.ppermute(strip, "blk", near)
    strip_both = lax.ppermute(strip_far, "blk", near)
    strips = [strip, strip_near, strip_far, strip_both]

    diagonal, codes = diagonal_update(heads, cb, leaves, rows)
    diagonal_near = lax.ppermute(diagonal, "blk", near)
    diagonal = diagonal + diagonal_near
    diagonal_far = lax.ppermute(diagonal, "blk", far)
    schur, inverses = first_factor(diagonal, diagonal_far, strips, cb, rows)

    partials = below_update(heads, tails, codes, cb, blk_count, per, leaves, rows)
    kept, for_near, for_far, for_both = (
        partials[HALVES * x:HALVES * (x + 1)] for x in range(blk_count)
    )
    from_near = []
    from_far = []
    for half in range(HALVES):
        passed = lax.ppermute(for_both[half], "blk", near)
        from_far.append(lax.ppermute(for_far[half] + passed, "blk", far))
    for half in range(HALVES):
        from_near.append(lax.ppermute(for_near[half], "blk", near))
    whole, lower = last_factor(schur, inverses, cb, rows)
    updates = [[kept[half], from_near[half], from_far[half]] for half in range(HALVES)]
    out, carried = solve_left(panel, updates[0], whole, lower, cb, per, rows)
    out = solve_right(panel, updates[1], whole, carried, out, cb, per, rows)
    return out.reshape(anc_panel.shape)


def solution(mesh):
    in_specs = (
        P(("leaf", "blk"), None, None),
        P(("leaf", "blk"), None),
        P(),
        P(),
        P("leaf", None, "blk", None, None),
    )
    out_specs = P("leaf", None, "blk", None, None)

    return jax.shard_map(shards, mesh=mesh, in_specs=in_specs, out_specs=out_specs, check_vma=False)
```

```python
import jax
import jax.numpy as jnp
from jax import lax
from jax.experimental import pallas as pl
from jax.experimental.pallas import tpu as pltpu
from jax.sharding import PartitionSpec as P


SLOTS = 2
CODES = 4
CODE_ROWS = 16
PANEL = 8
SPLIT = 2
HALVES = 2
DIRECT = 8
HIGHEST = lax.Precision.HIGHEST


def repeat(count, body, unroll_to=16):
    if count <= unroll_to:
        for index in range(count):
            body(index)
    else:
        lax.fori_loop(0, count, lambda index, carry: (body(index), carry)[1], 0)


def limit(mib):
    return pltpu.CompilerParams(vmem_limit_bytes=mib * 1024 * 1024)


def near_core(*arrays):
    return [pltpu.with_memory_space_constraint(array, pltpu.VMEM) for array in arrays]


def spaces(count, space):
    return [pl.BlockSpec(memory_space=space)] * count


def pack_kernel(cb, nb, direct, row_map, anc_order, anc_below, panel_hbm, anc_hbm, *refs):
    leaves = anc_order.shape[0]
    block_count, desc_count = row_map.shape
    rows = panel_hbm.shape[1] // block_count
    tail_rows = (block_count - 1) * rows
    count = leaves if direct else 1
    heads, tails = refs[:count], refs[count:2 * count]
    strip, inverse, used, chosen, codes, panel, panel_sem, strip_sem = refs[2 * count:]
    me = lax.axis_index("leaf")
    panel_copy = pltpu.make_async_copy(panel_hbm, panel, panel_sem)
    panel_copy.start()
    strip_copy = pltpu.make_async_copy(anc_hbm.at[0], strip, strip_sem)
    strip_copy.start()

    def clear(leaf):
        inverse[anc_order[leaf]] = leaf
        used[leaf] = 0
        for slot in range(SLOTS):
            chosen[leaf * SLOTS + slot] = 0
            codes[(leaf * SLOTS + slot) * CODES] = cb
            for r in range(1, CODES):
                codes[(leaf * SLOTS + slot) * CODES + r] = nb

    repeat(leaves, clear)

    def assign(desc):
        head = row_map[0, desc]
        leaf = inverse[lax.div(head, cb)]
        taken = used[leaf]
        used[leaf] = taken + 1
        place = leaf * SLOTS + taken
        chosen[place] = desc
        codes[place * CODES] = head - anc_order[leaf] * cb
        for r in range(1, block_count):
            target = row_map[r, desc]
            found = jnp.int32(nb)
            for q in range(anc_below.shape[1]):
                found = jnp.where(anc_below[leaf, q] == target, q, found)
            codes[place * CODES + r] = found

    repeat(desc_count, assign)
    panel_copy.wait()

    def write(index):
        leaf = jnp.bitwise_xor(me, index) if direct else index
        head = heads[index] if direct else heads[0].at[index]
        tail = tails[index] if direct else tails[0].at[index]
        row = lax.broadcasted_iota(jnp.int32, (CODE_ROWS, 128), 0)
        values = jnp.zeros((CODE_ROWS, 128), jnp.int32)
        for entry in range(SLOTS * CODES):
            values = jnp.where(row == entry, codes[leaf * SLOTS * CODES + entry], values)
        head[pl.ds(SLOTS * rows, CODE_ROWS)] = values.astype(jnp.float32).astype(panel.dtype)
        for slot in range(SLOTS):
            desc = chosen[leaf * SLOTS + slot]
            head[pl.ds(slot * rows, rows)] = panel[desc, pl.ds(0, rows)]
            tail[pl.ds(slot * tail_rows, tail_rows)] = panel[desc, pl.ds(rows, tail_rows)]

    repeat(leaves, write)
    strip_copy.wait()


def pack(desc_panel, row_map, anc_order, anc_below, anc, cb, direct):
    leaves = anc_order.shape[0]
    block_count = row_map.shape[1]
    rows = desc_panel.shape[1] // block_count
    width = desc_panel.shape[2]
    head = (SLOTS * rows + CODE_ROWS, width)
    tail = (SLOTS * (block_count - 1) * rows, width)
    dtype = desc_panel.dtype
    if direct:
        outs = [pltpu.VMEM(head, dtype)] * leaves + [pltpu.VMEM(tail, dtype)] * leaves
    else:
        outs = [jax.ShapeDtypeStruct((leaves,) + shape, dtype) for shape in (head, tail)]
    outs.append(pltpu.VMEM(anc.shape[1:], anc.dtype))
    nb = anc_below.shape[1]

    def body(*refs):
        pack_kernel(cb, nb, direct, *refs)

    return pl.pallas_call(
        body,
        name="pack",
        compiler_params=limit(12 if direct else 40),
        out_shape=outs,
        in_specs=spaces(3, pltpu.SMEM) + spaces(2, pl.ANY),
        out_specs=spaces(len(outs), pltpu.VMEM),
        scratch_shapes=[
            pltpu.SMEM((leaves,), jnp.int32),
            pltpu.SMEM((leaves,), jnp.int32),
            pltpu.SMEM((leaves * SLOTS,), jnp.int32),
            pltpu.SMEM((leaves * SLOTS * CODES,), jnp.int32),
            pltpu.VMEM(desc_panel.shape, dtype),
            pltpu.SemaphoreType.DMA(()),
            pltpu.SemaphoreType.DMA(()),
        ],
    )(
        *(
            pltpu.with_memory_space_constraint(array, pltpu.HBM)
            for array in (row_map.T, anc_order, anc_below, desc_panel, anc)
        )
    )


def diagonal_kernel(cb, leaves, *refs):
    heads = refs[:-4]
    out, codes, left, right = refs[-4:]
    direct = len(heads) > 1
    rows = out.shape[1]
    group = min(leaves, 8)

    def load(index, start, size):
        if direct:
            return heads[index][pl.ds(start, size)]
        return heads[0][index, pl.ds(start, size)]

    lane = lax.broadcasted_iota(jnp.int32, (1, rows), 1)

    def step(base):
        for offset in range(group):
            marks = load(base + offset, SLOTS * rows, CODE_ROWS).astype(jnp.float32)
            packed = jnp.zeros((1, rows), jnp.float32)
            for entry in range(SLOTS * CODES):
                packed = jnp.where(lane == entry, marks[entry:entry + 1], packed)
            codes[pl.ds(base + offset, 1)] = packed.astype(jnp.int32)
            for slot in range(SLOTS):
                block = load(base + offset, slot * rows, rows)
                lanes = pl.ds((offset * SLOTS + slot) * rows, rows)
                code = jnp.broadcast_to(marks[slot * CODES:slot * CODES + 1], (rows, rows))
                code = code.astype(block.dtype)
                zero = jnp.zeros_like(block)
                right[:, lanes] = jnp.where(code < cb, block, zero)
                for c in range(cb):
                    left[c * rows:(c + 1) * rows, lanes] = jnp.where(code == c, block, zero)
        return lax.dot_general(
            left[...], right[...], (((1,), (1,)), ((), ())), preferred_element_type=jnp.float32
        )

    if leaves == group:
        out[...] = step(0).reshape(out.shape)
    else:
        out[...] = jnp.zeros_like(out)

        def accumulate(index, carry):
            out[...] += step(index * group).reshape(out.shape)
            return carry

        lax.fori_loop(0, leaves // group, accumulate, 0)


def diagonal_update(heads, cb, leaves, rows):
    group = min(leaves, 8)

    def body(*refs):
        diagonal_kernel(cb, leaves, *refs)

    return pl.pallas_call(
        body,
        name="diagonal",
        compiler_params=limit(12 if len(heads) > 1 else 40),
        out_shape=[
            pltpu.VMEM((cb * rows, rows), jnp.float32),
            jax.ShapeDtypeStruct((leaves, rows), jnp.int32),
        ],
        in_specs=spaces(len(heads), pltpu.VMEM),
        out_specs=spaces(2, pltpu.VMEM),
        scratch_shapes=[
            pltpu.VMEM((cb * rows, group * SLOTS * rows), heads[0].dtype),
            pltpu.VMEM((rows, group * SLOTS * rows), heads[0].dtype),
        ],
        cost_estimate=pl.CostEstimate(flops=2000000000, bytes_accessed=1000000, transcendentals=0),
    )(*(near_core(*heads) if len(heads) > 1 else heads))


def below_kernel(cb, blk_count, per, leaves, count, codes, *refs):
    tails, refs = refs[:count], refs[count:]
    heads = refs[:count]
    outs = refs[count:count + blk_count * HALVES]
    acc, products = refs[count + blk_count * HALVES:]
    direct = count > 1
    me_blk = lax.axis_index("blk")
    rows = acc.shape[1]
    group = min(leaves, 8)
    tail_rows = tails[0].shape[-2] // SLOTS
    extra = tail_rows // rows
    blocks = blk_count * cb * per

    for first in range(0, blocks, cb):
        acc[pl.ds(first, cb)] = jnp.zeros((cb, rows, rows), jnp.float32)

    def step(base):
        for offset in range(group):
            index = base + offset
            for slot in range(SLOTS):
                if direct:
                    head = heads[index][pl.ds(slot * rows, rows)]
                    tail = tails[index][pl.ds(slot * tail_rows, tail_rows)]
                else:
                    head = heads[0][index, pl.ds(slot * rows, rows)]
                    tail = tails[0][index, pl.ds(slot * tail_rows, tail_rows)]
                products[offset * SLOTS + slot] = lax.dot_general(
                    tail, head, (((1,), (1,)), ((), ())), preferred_element_type=jnp.float32
                )
        for offset in range(group):
            for slot in range(SLOTS):
                column = codes[base + offset, slot * CODES]
                for r in range(extra):
                    position = codes[base + offset, slot * CODES + 1 + r]
                    relative = jnp.bitwise_xor(lax.rem(position, blk_count), me_blk)
                    place = (relative * cb + column) * per + lax.div(position, blk_count)
                    place = jnp.where(column < cb, place, blocks)
                    acc[place] += products[offset * SLOTS + slot, pl.ds(r * rows, rows)]

    if leaves == group:
        step(0)
    else:
        lax.fori_loop(0, leaves // group, lambda index, carry: (step(index * group), carry)[1], 0)
    size = cb * per // HALVES
    for part, out in enumerate(outs):
        out[...] = acc[pl.ds(part * size, size)]


def below_update(heads, tails, codes, cb, blk_count, per, leaves, rows):
    group = min(leaves, 8)
    blocks = blk_count * cb * per
    outs = blk_count * HALVES

    def body(*refs):
        below_kernel(cb, blk_count, per, leaves, len(heads), *refs)

    return pl.pallas_call(
        body,
        name="below",
        compiler_params=limit(16 if len(heads) > 1 else 56),
        out_shape=[pltpu.VMEM((cb * per // HALVES, rows, rows), jnp.float32)] * outs,
        in_specs=spaces(1, pltpu.SMEM) + spaces(2 * len(heads), pltpu.VMEM),
        out_specs=spaces(outs, pltpu.VMEM),
        scratch_shapes=[
            pltpu.VMEM((blocks + 1, rows, rows), jnp.float32),
            pltpu.VMEM((group * SLOTS, tails[0].shape[-2] // SLOTS, rows), jnp.float32),
        ],
        cost_estimate=pl.CostEstimate(flops=2000000000, bytes_accessed=4000000, transcendentals=0),
    )(codes, *(near_core(*tails, *heads) if len(heads) > 1 else [*tails, *heads]))


def factor_block(work, rows):
    lane = lax.broadcasted_iota(jnp.int32, (1, rows), 1)
    sub = lax.broadcasted_iota(jnp.int32, (PANEL, 1), 0)
    segments = 4
    size = rows // segments

    for segment in range(segments):
        top = segment * size

        def panel(index, carry):
            base = pl.multiple_of(top + index * PANEL, PANEL)
            strip = work[pl.ds(base, PANEL), :]
            raw = work[top:, :rows]
            picks = [(lane == base + k) for k in range(PANEL)]
            corner = [
                jnp.sum(jnp.where(picks[k], strip[:, :rows], 0.0), axis=1, keepdims=True)
                for k in range(PANEL)
            ]
            factor = jnp.zeros((PANEL, 2 * rows), jnp.float32)
            for k in range(PANEL):
                scale = lax.rsqrt(corner[k][k:k + 1])
                inverse = scale * scale
                row = strip[k:k + 1]
                factor = jnp.where(sub == k, row * scale, factor)
                scaled = row * inverse
                strip = jnp.where(sub == k, scaled, strip - corner[k] * scaled)
                for m in range(k + 1, PANEL):
                    entry = corner[m][k:k + 1]
                    corner[m] = jnp.where(
                        sub == k, entry * inverse, corner[m] - (corner[k] * entry) * inverse
                    )
            work[pl.ds(base, PANEL), :] = factor
            for start, stop, masked in ((top, top + size, True), (top + size, rows, False)):
                if start == stop:
                    continue
                full = work[start:stop, :]
                row_id = lax.broadcasted_iota(jnp.int32, (stop - start, 1), 0) + start
                for k in range(PANEL):
                    column = jnp.sum(
                        jnp.where(picks[k], raw[start - top:stop - top], 0.0), axis=1, keepdims=True
                    )
                    if masked:
                        column = jnp.where(row_id >= base + PANEL, column, 0.0)
                    full = full - column * strip[k:k + 1]
                work[start:stop, :] = full
            return carry

        lax.fori_loop(0, size // PANEL, panel, 0)


def eliminate(schur, inverse_ref, work, block, cb, rows):
    eye = lax.broadcasted_iota(jnp.int32, (rows, rows), 0) == lax.broadcasted_iota(
        jnp.int32, (rows, rows), 1
    )
    upper = lax.broadcasted_iota(jnp.int32, (rows, rows), 0) <= lax.broadcasted_iota(
        jnp.int32, (rows, rows), 1
    )
    here = block * rows
    work[:, :rows] = schur[block, :, here:here + rows]
    work[:, rows:] = eye.astype(jnp.float32)
    factor_block(work, rows)
    schur[block, :, here:here + rows] = jnp.where(upper, work[:, :rows], 0.0)
    inverse = work[:, rows:]
    inverse_ref[...] = inverse
    if block + 1 < cb:
        after = here + rows
        strip = lax.dot_general(
            inverse, schur[block, :, after:], (((1,), (0,)), ((), ())),
            precision=HIGHEST, preferred_element_type=jnp.float32,
        )
        schur[block, :, after:] = strip
        for other in range(block + 1, cb):
            offset = (other - block - 1) * rows
            schur[other, :, other * rows:] -= lax.dot_general(
                strip[:, offset:offset + rows], strip[:, offset:], (((0,), (0,)), ((), ())),
                precision=HIGHEST, preferred_element_type=jnp.float32,
            )


def kept_inverse(schur, block, cb, rows):
    return schur.at[cb - 1, :, block * rows:(block + 1) * rows]


def first_factor(own_sum, other_sum, strips, cb, rows):
    blk_count = len(strips)

    def body(own_ref, other_ref, *refs):
        strip_refs = refs[:blk_count]
        schur, work = refs[blk_count:]
        me = lax.axis_index("blk")
        for x in range(blk_count):
            schur[jnp.bitwise_xor(me, x)] = strip_refs[x][...]
        for c in range(cb):
            part = slice(c * rows, (c + 1) * rows)
            schur[c, :, part] -= own_ref[part] + other_ref[part]
        for block in range(cb // SPLIT):
            eliminate(schur, kept_inverse(schur, block, cb, rows), work, block, cb, rows)

    return pl.pallas_call(
        body,
        name="factor_first",
        compiler_params=limit(12),
        out_shape=[
            pltpu.VMEM((cb, rows, cb * rows), jnp.float32),
        ],
        in_specs=spaces(2 + blk_count, pltpu.VMEM),
        out_specs=spaces(1, pltpu.VMEM),
        scratch_shapes=[pltpu.VMEM((rows, 2 * rows), jnp.float32)],
        cost_estimate=pl.CostEstimate(flops=10000000000, bytes_accessed=2000000, transcendentals=0),
    )(*near_core(own_sum, other_sum, *strips))[0]


def last_factor(schur_in, cb, rows):
    width = cb * rows

    def body(schur_ref, whole, lower, schur, inverses, work):
        me = lax.axis_index("blk")
        schur[...] = schur_ref[...]
        for block in range(cb // SPLIT):
            inverses[block] = kept_inverse(schur_ref, block, cb, rows)[...]
        for block in range(cb // SPLIT, cb):
            eliminate(schur, inverses.at[block], work, block, cb, rows)
        for k in range(cb):
            piece = jnp.where(k <= me, schur[k, :, pl.ds(pl.multiple_of(me * rows, rows), rows)], 0.0)
            lower[:, k * rows:(k + 1) * rows] = piece.T
        whole[...] = jnp.zeros_like(whole)
        for i in range(cb):
            whole[i * rows:(i + 1) * rows, i * rows:(i + 1) * rows] = inverses[i]
            if i:
                done = slice(0, i * rows)
                total = jnp.zeros((rows, i * rows), jnp.float32)
                for k in range(i):
                    total = total + lax.dot_general(
                        schur[k, :, i * rows:(i + 1) * rows],
                        whole[k * rows:(k + 1) * rows, done],
                        (((0,), (0,)), ((), ())),
                        precision=HIGHEST, preferred_element_type=jnp.float32,
                    )
                whole[i * rows:(i + 1) * rows, done] = -lax.dot_general(
                    inverses[i], total, (((1,), (0,)), ((), ())),
                    precision=HIGHEST, preferred_element_type=jnp.float32,
                )

    return pl.pallas_call(
        body,
        name="factor_last",
        compiler_params=limit(12),
        out_shape=[
            pltpu.VMEM((width, width), jnp.float32),
            pltpu.VMEM((rows, width), jnp.float32),
        ],
        in_specs=spaces(1, pltpu.VMEM),
        out_specs=spaces(2, pltpu.VMEM),
        scratch_shapes=[
            pltpu.VMEM((cb, rows, width), jnp.float32),
            pltpu.VMEM((cb, rows, rows), jnp.float32),
            pltpu.VMEM((rows, 2 * rows), jnp.float32),
        ],
        cost_estimate=pl.CostEstimate(flops=12000000000, bytes_accessed=2000000, transcendentals=0),
    )(*near_core(schur_in))


def solve_dot(left, right):
    return lax.dot_general(
        left, right, (((1,), (1,)), ((), ())),
        precision=HIGHEST, preferred_element_type=jnp.float32,
    )


def remaining(panel_ref, update_refs, half, cb, per, rows):
    parts = []
    for c in range(cb // HALVES):
        column = (half * (cb // HALVES) + c) * rows
        block = slice(c * per, (c + 1) * per)
        update = update_refs[0][block]
        for ref in update_refs[1:]:
            update = update + ref[block]
        original = panel_ref[1:, :, column:column + rows]
        parts.append((original - update).reshape(per * rows, rows))
    return jnp.concatenate(parts, axis=1)


def solve_left(panel, updates, whole, lower, cb, per, rows):
    width = cb * rows
    half = width // HALVES

    def body(panel_ref, *refs):
        updates_ref = refs[:len(updates)]
        whole_ref, lower_ref, out, carried = refs[len(updates):]
        left = remaining(panel_ref, updates_ref, 0, cb, per, rows)
        out[0] = lower_ref[...]
        out[1:, :, :half] = solve_dot(left, whole_ref[:half, :half]).reshape(per, rows, half)
        carried[...] = solve_dot(left, whole_ref[half:, :half])

    return pl.pallas_call(
        body,
        name="solve_left",
        compiler_params=limit(16),
        out_shape=[
            jax.ShapeDtypeStruct((per + 1, rows, width), jnp.float32),
            pltpu.VMEM((per * rows, half), jnp.float32),
        ],
        in_specs=spaces(3 + len(updates), pltpu.VMEM),
        out_specs=spaces(2, pltpu.VMEM),
        cost_estimate=pl.CostEstimate(flops=2000000000, bytes_accessed=5000000, transcendentals=0),
    )(panel, *near_core(*updates, whole, lower))


def solve_right(panel, updates, whole, carried, out, cb, per, rows):
    width = cb * rows
    half = width // HALVES

    def body(panel_ref, *refs):
        updates_ref = refs[:len(updates)]
        whole_ref, carried_ref, _, result, stage, sem = refs[len(updates):]
        left = remaining(panel_ref, updates_ref, 1, cb, per, rows)
        value = carried_ref[...] + solve_dot(left, whole_ref[half:, half:])
        stage[...] = value.reshape(per, rows, half)
        copy = pltpu.make_async_copy(
            stage, result.at[pl.ds(1, per), :, pl.ds(half, half)], sem
        )
        copy.start()
        copy.wait()

    return pl.pallas_call(
        body,
        name="solve_right",
        compiler_params=limit(16),
        out_shape=jax.ShapeDtypeStruct((per + 1, rows, width), jnp.float32),
        in_specs=spaces(3 + len(updates), pltpu.VMEM) + spaces(1, pl.ANY),
        out_specs=pl.BlockSpec(memory_space=pl.ANY),
        scratch_shapes=[pltpu.VMEM((per, rows, half), jnp.float32), pltpu.SemaphoreType.DMA(())],
        input_output_aliases={3 + len(updates): 0},
        cost_estimate=pl.CostEstimate(flops=2000000000, bytes_accessed=5000000, transcendentals=0),
    )(panel, *near_core(*updates, whole, carried), out)


def shards(desc_panel, row_map, anc_order, anc_below, anc_panel):
    leaves = lax.axis_size("leaf")
    blk_count = lax.axis_size("blk")
    rows = anc_panel.shape[3]
    width = anc_panel.shape[4]
    cb = width // rows
    per = anc_below.shape[1] // blk_count
    assert cb == blk_count == 4 and desc_panel.shape[2] == rows
    direct = leaves <= DIRECT and leaves & (leaves - 1) == 0
    near = [(i, i ^ 1) for i in range(blk_count)]
    far = [(i, i ^ 2) for i in range(blk_count)]

    panel = anc_panel.reshape(per + 1, rows, width)
    *packed, strip = pack(desc_panel, row_map, anc_order, anc_below, panel, cb, direct)
    count = len(packed) // 2
    heads, tails = packed[:count], packed[count:]

    def exchange(arrays):
        if not direct:
            return [lax.all_to_all(arrays[0], "leaf", split_axis=0, concat_axis=0, tiled=True)]
        received = [arrays[0]]
        for k in range(1, leaves):
            swap = [(i, i ^ k) for i in range(leaves)]
            received.append(lax.ppermute(arrays[k], "leaf", swap))
        return received

    heads = exchange(heads)
    tails = exchange(tails)
    strip_far = lax.ppermute(strip, "blk", far)
    strip_near = lax.ppermute(strip, "blk", near)
    strip_both = lax.ppermute(strip_far, "blk", near)
    strips = [strip, strip_near, strip_far, strip_both]

    diagonal, codes = diagonal_update(heads, cb, leaves, rows)
    diagonal_near = lax.ppermute(diagonal, "blk", near)
    diagonal = diagonal + diagonal_near
    diagonal_far = lax.ppermute(diagonal, "blk", far)
    schur = first_factor(diagonal, diagonal_far, strips, cb, rows)

    partials = below_update(heads, tails, codes, cb, blk_count, per, leaves, rows)
    kept, for_near, for_far, for_both = (
        partials[HALVES * x:HALVES * (x + 1)] for x in range(blk_count)
    )
    from_near = []
    from_far = []
    for half in range(HALVES):
        passed = lax.ppermute(for_both[half], "blk", near)
        from_far.append(lax.ppermute(for_far[half] + passed, "blk", far))
    for half in range(HALVES):
        from_near.append(lax.ppermute(for_near[half], "blk", near))
    whole, lower = last_factor(schur, cb, rows)
    updates = [[kept[half], from_near[half], from_far[half]] for half in range(HALVES)]
    out, carried = solve_left(panel, updates[0], whole, lower, cb, per, rows)
    out = solve_right(panel, updates[1], whole, carried, out, cb, per, rows)
    return out.reshape(anc_panel.shape)


def solution(mesh):
    in_specs = (
        P(("leaf", "blk"), None, None),
        P(("leaf", "blk"), None),
        P(),
        P(),
        P("leaf", None, "blk", None, None),
    )
    out_specs = P("leaf", None, "blk", None, None)

    return jax.shard_map(shards, mesh=mesh, in_specs=in_specs, out_specs=out_specs, check_vma=False)
```

```python
import jax
import jax.numpy as jnp
from jax import lax
from jax.experimental import pallas as pl
from jax.experimental.pallas import tpu as pltpu
from jax.sharding import PartitionSpec as P


SLOTS = 2
CODES = 4
CODE_ROWS = 8
PANEL = 8
SPLIT = 2
HALVES = 2
SCALE_ROWS = 16
BITS = 23.0
LOG2E = 1.4426950408889634
DIRECT = 8
HIGHEST = lax.Precision.HIGHEST


def repeat(count, body, unroll_to=16):
    if count <= unroll_to:
        for index in range(count):
            body(index)
    else:
        lax.fori_loop(0, count, lambda index, carry: (body(index), carry)[1], 0)


def limit(mib):
    return pltpu.CompilerParams(vmem_limit_bytes=mib * 1024 * 1024)


def near_core(*arrays):
    return [pltpu.with_memory_space_constraint(array, pltpu.VMEM) for array in arrays]


def spaces(count, space):
    return [pl.BlockSpec(memory_space=space)] * count


def pack_kernel(cb, nb, direct, row_map, anc_order, anc_below, panel_hbm, anc_hbm, *refs):
    leaves = anc_order.shape[0]
    block_count, desc_count = row_map.shape
    rows = panel_hbm.shape[1] // block_count
    tail_rows = (block_count - 1) * rows
    count = leaves if direct else 1
    heads, tails = refs[:count], refs[count:2 * count]
    strip, inverse, used, chosen, codes, panel, panel_sem, strip_sem = refs[2 * count:]
    me = lax.axis_index("leaf")
    panel_copy = pltpu.make_async_copy(panel_hbm, panel, panel_sem)
    panel_copy.start()
    strip_copy = pltpu.make_async_copy(anc_hbm.at[0], strip, strip_sem)
    strip_copy.start()

    def clear(leaf):
        inverse[anc_order[leaf]] = leaf
        used[leaf] = 0
        for slot in range(SLOTS):
            chosen[leaf * SLOTS + slot] = 0
            codes[(leaf * SLOTS + slot) * CODES] = cb
            for r in range(1, CODES):
                codes[(leaf * SLOTS + slot) * CODES + r] = nb

    repeat(leaves, clear)

    def assign(desc):
        head = row_map[0, desc]
        leaf = inverse[lax.div(head, cb)]
        taken = used[leaf]
        used[leaf] = taken + 1
        place = leaf * SLOTS + taken
        chosen[place] = desc
        codes[place * CODES] = head - anc_order[leaf] * cb
        for r in range(1, block_count):
            target = row_map[r, desc]
            found = jnp.int32(nb)
            for q in range(anc_below.shape[1]):
                found = jnp.where(anc_below[leaf, q] == target, q, found)
            codes[place * CODES + r] = found

    repeat(desc_count, assign)
    panel_copy.wait()

    def write(index):
        leaf = jnp.bitwise_xor(me, index) if direct else index
        head = heads[index] if direct else heads[0].at[index]
        tail = tails[index] if direct else tails[0].at[index]
        row = lax.broadcasted_iota(jnp.int32, (CODE_ROWS, 128), 0)
        values = jnp.zeros((CODE_ROWS, 128), jnp.int32)
        for entry in range(SLOTS * CODES):
            values = jnp.where(row == entry, codes[leaf * SLOTS * CODES + entry], values)
        head[pl.ds(SLOTS * rows, CODE_ROWS)] = values.astype(jnp.float32).astype(panel.dtype)
        for slot in range(SLOTS):
            desc = chosen[leaf * SLOTS + slot]
            head[pl.ds(slot * rows, rows)] = panel[desc, pl.ds(0, rows)]
            tail[pl.ds(slot * tail_rows, tail_rows)] = panel[desc, pl.ds(rows, tail_rows)]

    repeat(leaves, write)
    strip_copy.wait()


def pack(desc_panel, row_map, anc_order, anc_below, anc, cb, direct):
    leaves = anc_order.shape[0]
    block_count = row_map.shape[1]
    rows = desc_panel.shape[1] // block_count
    width = desc_panel.shape[2]
    head = (SLOTS * rows + CODE_ROWS, width)
    tail = (SLOTS * (block_count - 1) * rows, width)
    dtype = desc_panel.dtype
    if direct:
        outs = [pltpu.VMEM(head, dtype)] * leaves + [pltpu.VMEM(tail, dtype)] * leaves
    else:
        outs = [jax.ShapeDtypeStruct((leaves,) + shape, dtype) for shape in (head, tail)]
    outs.append(pltpu.VMEM(anc.shape[1:], anc.dtype))
    nb = anc_below.shape[1]

    def body(*refs):
        pack_kernel(cb, nb, direct, *refs)

    return pl.pallas_call(
        body,
        name="pack",
        compiler_params=limit(12 if direct else 40),
        out_shape=outs,
        in_specs=spaces(3, pltpu.SMEM) + spaces(2, pl.ANY),
        out_specs=spaces(len(outs), pltpu.VMEM),
        scratch_shapes=[
            pltpu.SMEM((leaves,), jnp.int32),
            pltpu.SMEM((leaves,), jnp.int32),
            pltpu.SMEM((leaves * SLOTS,), jnp.int32),
            pltpu.SMEM((leaves * SLOTS * CODES,), jnp.int32),
            pltpu.VMEM(desc_panel.shape, dtype),
            pltpu.SemaphoreType.DMA(()),
            pltpu.SemaphoreType.DMA(()),
        ],
    )(
        *(
            pltpu.with_memory_space_constraint(array, pltpu.HBM)
            for array in (row_map.T, anc_order, anc_below, desc_panel, anc)
        )
    )


def diagonal_kernel(cb, leaves, *refs):
    heads = refs[:-4]
    out, codes, left, right = refs[-4:]
    direct = len(heads) > 1
    rows = out.shape[1]
    group = min(leaves, 8)

    def load(index, start, size):
        if direct:
            return heads[index][pl.ds(start, size)]
        return heads[0][index, pl.ds(start, size)]

    lane = lax.broadcasted_iota(jnp.int32, (1, rows), 1)

    def step(base):
        for offset in range(group):
            marks = load(base + offset, SLOTS * rows, CODE_ROWS).astype(jnp.float32)
            packed = jnp.zeros((1, rows), jnp.float32)
            for entry in range(SLOTS * CODES):
                packed = jnp.where(lane == entry, marks[entry:entry + 1], packed)
            codes[pl.ds(base + offset, 1)] = packed.astype(jnp.int32)
            for slot in range(SLOTS):
                block = load(base + offset, slot * rows, rows)
                lanes = pl.ds((offset * SLOTS + slot) * rows, rows)
                code = jnp.broadcast_to(marks[slot * CODES:slot * CODES + 1], (rows, rows))
                code = code.astype(block.dtype)
                zero = jnp.zeros_like(block)
                right[:, lanes] = jnp.where(code < cb, block, zero)
                for c in range(cb):
                    left[c * rows:(c + 1) * rows, lanes] = jnp.where(code == c, block, zero)
        return lax.dot_general(
            left[...], right[...], (((1,), (1,)), ((), ())), preferred_element_type=jnp.float32
        )

    if leaves == group:
        out[...] = step(0).reshape(out.shape)
    else:
        out[...] = jnp.zeros_like(out)

        def accumulate(index, carry):
            out[...] += step(index * group).reshape(out.shape)
            return carry

        lax.fori_loop(0, leaves // group, accumulate, 0)


def diagonal_update(heads, cb, leaves, rows):
    group = min(leaves, 8)

    def body(*refs):
        diagonal_kernel(cb, leaves, *refs)

    return pl.pallas_call(
        body,
        name="diagonal",
        compiler_params=limit(12 if len(heads) > 1 else 40),
        out_shape=[
            pltpu.VMEM((cb * rows, rows), jnp.float32),
            jax.ShapeDtypeStruct((leaves, rows), jnp.int32),
        ],
        in_specs=spaces(len(heads), pltpu.VMEM),
        out_specs=spaces(2, pltpu.VMEM),
        scratch_shapes=[
            pltpu.VMEM((cb * rows, group * SLOTS * rows), heads[0].dtype),
            pltpu.VMEM((rows, group * SLOTS * rows), heads[0].dtype),
        ],
        cost_estimate=pl.CostEstimate(flops=2000000000, bytes_accessed=1000000, transcendentals=0),
    )(*(near_core(*heads) if len(heads) > 1 else heads))


def below_kernel(cb, blk_count, per, leaves, count, codes, *refs):
    tails, refs = refs[:count], refs[count:]
    heads = refs[:count]
    outs = refs[count:count + blk_count * HALVES]
    acc, products = refs[count + blk_count * HALVES:]
    direct = count > 1
    me_blk = lax.axis_index("blk")
    rows = acc.shape[1]
    group = min(leaves, 8)
    tail_rows = tails[0].shape[-2] // SLOTS
    extra = tail_rows // rows
    blocks = blk_count * cb * per

    for first in range(0, blocks, cb):
        acc[pl.ds(first, cb)] = jnp.zeros((cb, rows, rows), jnp.float32)

    def step(base):
        for offset in range(group):
            index = base + offset
            for slot in range(SLOTS):
                if direct:
                    head = heads[index][pl.ds(slot * rows, rows)]
                    tail = tails[index][pl.ds(slot * tail_rows, tail_rows)]
                else:
                    head = heads[0][index, pl.ds(slot * rows, rows)]
                    tail = tails[0][index, pl.ds(slot * tail_rows, tail_rows)]
                products[offset * SLOTS + slot] = lax.dot_general(
                    tail, head, (((1,), (1,)), ((), ())), preferred_element_type=jnp.float32
                )
        for offset in range(group):
            for slot in range(SLOTS):
                column = codes[base + offset, slot * CODES]
                for r in range(extra):
                    position = codes[base + offset, slot * CODES + 1 + r]
                    relative = jnp.bitwise_xor(lax.rem(position, blk_count), me_blk)
                    place = (relative * cb + column) * per + lax.div(position, blk_count)
                    place = jnp.where(column < cb, place, blocks)
                    acc[place] += products[offset * SLOTS + slot, pl.ds(r * rows, rows)]

    if leaves == group:
        step(0)
    else:
        lax.fori_loop(0, leaves // group, lambda index, carry: (step(index * group), carry)[1], 0)
    size = cb * per // HALVES
    for part, out in enumerate(outs):
        out[...] = acc[pl.ds(part * size, size)]


def below_update(heads, tails, codes, cb, blk_count, per, leaves, rows):
    group = min(leaves, 8)
    blocks = blk_count * cb * per
    outs = blk_count * HALVES

    def body(*refs):
        below_kernel(cb, blk_count, per, leaves, len(heads), *refs)

    return pl.pallas_call(
        body,
        name="below",
        compiler_params=limit(16 if len(heads) > 1 else 56),
        out_shape=[pltpu.VMEM((cb * per // HALVES, rows, rows), jnp.float32)] * outs,
        in_specs=spaces(1, pltpu.SMEM) + spaces(2 * len(heads), pltpu.VMEM),
        out_specs=spaces(outs, pltpu.VMEM),
        scratch_shapes=[
            pltpu.VMEM((blocks + 1, rows, rows), jnp.float32),
            pltpu.VMEM((group * SLOTS, tails[0].shape[-2] // SLOTS, rows), jnp.float32),
        ],
        cost_estimate=pl.CostEstimate(flops=2000000000, bytes_accessed=4000000, transcendentals=0),
    )(codes, *(near_core(*tails, *heads) if len(heads) > 1 else [*tails, *heads]))


def factor_block(work, rows):
    lane = lax.broadcasted_iota(jnp.int32, (1, rows), 1)
    sub = lax.broadcasted_iota(jnp.int32, (PANEL, 1), 0)
    segments = 4
    size = rows // segments

    for segment in range(segments):
        top = segment * size

        def panel(index, carry):
            base = pl.multiple_of(top + index * PANEL, PANEL)
            strip = work[pl.ds(base, PANEL), :]
            raw = work[top:, :rows]
            picks = [(lane == base + k) for k in range(PANEL)]
            corner = [
                jnp.sum(jnp.where(picks[k], strip[:, :rows], 0.0), axis=1, keepdims=True)
                for k in range(PANEL)
            ]
            factor = jnp.zeros((PANEL, 2 * rows), jnp.float32)
            for k in range(PANEL):
                scale = lax.rsqrt(corner[k][k:k + 1])
                inverse = scale * scale
                row = strip[k:k + 1]
                factor = jnp.where(sub == k, row * scale, factor)
                scaled = row * inverse
                strip = jnp.where(sub == k, scaled, strip - corner[k] * scaled)
                for m in range(k + 1, PANEL):
                    entry = corner[m][k:k + 1]
                    corner[m] = jnp.where(
                        sub == k, entry * inverse, corner[m] - (corner[k] * entry) * inverse
                    )
            work[pl.ds(base, PANEL), :] = factor
            for start, stop, masked in ((top, top + size, True), (top + size, rows, False)):
                if start == stop:
                    continue
                full = work[start:stop, :]
                row_id = lax.broadcasted_iota(jnp.int32, (stop - start, 1), 0) + start
                for k in range(PANEL):
                    column = jnp.sum(
                        jnp.where(picks[k], raw[start - top:stop - top], 0.0), axis=1, keepdims=True
                    )
                    if masked:
                        column = jnp.where(row_id >= base + PANEL, column, 0.0)
                    full = full - column * strip[k:k + 1]
                work[start:stop, :] = full
            return carry

        lax.fori_loop(0, size // PANEL, panel, 0)


def eliminate(schur, inverse_ref, work, block, cb, rows):
    eye = lax.broadcasted_iota(jnp.int32, (rows, rows), 0) == lax.broadcasted_iota(
        jnp.int32, (rows, rows), 1
    )
    upper = lax.broadcasted_iota(jnp.int32, (rows, rows), 0) <= lax.broadcasted_iota(
        jnp.int32, (rows, rows), 1
    )
    here = block * rows
    work[:, :rows] = schur[block, :, here:here + rows]
    work[:, rows:] = eye.astype(jnp.float32)
    factor_block(work, rows)
    schur[block, :, here:here + rows] = jnp.where(upper, work[:, :rows], 0.0)
    inverse = work[:, rows:]
    inverse_ref[...] = inverse
    if block + 1 < cb:
        after = here + rows
        strip = lax.dot_general(
            inverse, schur[block, :, after:], (((1,), (0,)), ((), ())),
            precision=HIGHEST, preferred_element_type=jnp.float32,
        )
        schur[block, :, after:] = strip
        for other in range(block + 1, cb):
            offset = (other - block - 1) * rows
            schur[other, :, other * rows:] -= lax.dot_general(
                strip[:, offset:offset + rows], strip[:, offset:], (((0,), (0,)), ((), ())),
                precision=HIGHEST, preferred_element_type=jnp.float32,
            )


def kept_inverse(schur, block, cb, rows):
    return schur.at[cb - 1, :, block * rows:(block + 1) * rows]


def first_factor(own_sum, other_sum, strips, cb, rows):
    blk_count = len(strips)

    def body(own_ref, other_ref, *refs):
        strip_refs = refs[:blk_count]
        schur, work = refs[blk_count:]
        me = lax.axis_index("blk")
        for x in range(blk_count):
            schur[jnp.bitwise_xor(me, x)] = strip_refs[x][...]
        for c in range(cb):
            part = slice(c * rows, (c + 1) * rows)
            schur[c, :, part] -= own_ref[part] + other_ref[part]
        for block in range(cb // SPLIT):
            eliminate(schur, kept_inverse(schur, block, cb, rows), work, block, cb, rows)

    return pl.pallas_call(
        body,
        name="factor_first",
        compiler_params=limit(12),
        out_shape=[
            pltpu.VMEM((cb, rows, cb * rows), jnp.float32),
        ],
        in_specs=spaces(2 + blk_count, pltpu.VMEM),
        out_specs=spaces(1, pltpu.VMEM),
        scratch_shapes=[pltpu.VMEM((rows, 2 * rows), jnp.float32)],
        cost_estimate=pl.CostEstimate(flops=10000000000, bytes_accessed=2000000, transcendentals=0),
    )(*near_core(own_sum, other_sum, *strips))[0]


def last_factor(schur_in, cb, rows):
    width = cb * rows

    def body(schur_ref, whole, lower, schur, inverses, work):
        me = lax.axis_index("blk")
        schur[...] = schur_ref[...]
        for block in range(cb // SPLIT):
            inverses[block] = kept_inverse(schur_ref, block, cb, rows)[...]
        for block in range(cb // SPLIT, cb):
            eliminate(schur, inverses.at[block], work, block, cb, rows)
        for k in range(cb):
            piece = jnp.where(k <= me, schur[k, :, pl.ds(pl.multiple_of(me * rows, rows), rows)], 0.0)
            lower[:, k * rows:(k + 1) * rows] = piece.T
        whole[...] = jnp.zeros_like(whole)
        for i in range(cb):
            whole[i * rows:(i + 1) * rows, i * rows:(i + 1) * rows] = inverses[i]
            if i:
                done = slice(0, i * rows)
                total = jnp.zeros((rows, i * rows), jnp.float32)
                for k in range(i):
                    total = total + lax.dot_general(
                        schur[k, :, i * rows:(i + 1) * rows],
                        whole[k * rows:(k + 1) * rows, done],
                        (((0,), (0,)), ((), ())),
                        precision=HIGHEST, preferred_element_type=jnp.float32,
                    )
                whole[i * rows:(i + 1) * rows, done] = -lax.dot_general(
                    inverses[i], total, (((1,), (0,)), ((), ())),
                    precision=HIGHEST, preferred_element_type=jnp.float32,
                )

    return pl.pallas_call(
        body,
        name="factor_last",
        compiler_params=limit(12),
        out_shape=[
            pltpu.VMEM((width, width), jnp.float32),
            pltpu.VMEM((rows, width), jnp.float32),
        ],
        in_specs=spaces(1, pltpu.VMEM),
        out_specs=spaces(2, pltpu.VMEM),
        scratch_shapes=[
            pltpu.VMEM((cb, rows, width), jnp.float32),
            pltpu.VMEM((cb, rows, rows), jnp.float32),
            pltpu.VMEM((rows, 2 * rows), jnp.float32),
        ],
        cost_estimate=pl.CostEstimate(flops=12000000000, bytes_accessed=2000000, transcendentals=0),
    )(*near_core(schur_in))


def pack_sums(first, second):
    count, rows, width = first.shape
    pairs = count // 2

    def body(first_ref, second_ref, out):
        row = lax.broadcasted_iota(jnp.int32, (SCALE_ROWS, width), 0)
        scales = jnp.zeros((SCALE_ROWS, width), jnp.int32)
        lows = []
        for j in range(count):
            value = first_ref[j] + second_ref[j]
            peak = jnp.maximum(jnp.max(jnp.abs(value), axis=0, keepdims=True), 1e-30)
            power = jnp.floor(jnp.log(peak) * LOG2E + 1e-3) + 1.0
            scales = jnp.where(row == j, power.astype(jnp.int32), scales)
            whole = jnp.floor(value * jnp.exp2(BITS - power) + 0.5).astype(jnp.int32)
            high = lax.shift_right_arithmetic(whole, 8)
            lows.append(whole - high * 256)
            out[j * rows:(j + 1) * rows] = high.astype(jnp.int16)
        for j in range(pairs):
            low = lows[j] + lows[j + pairs] * 256 - 32768
            out[(count + j) * rows:(count + j + 1) * rows] = low.astype(jnp.int16)
        out[(count + pairs) * rows:] = scales.astype(jnp.int16)

    return pl.pallas_call(
        body,
        name="pack_sums",
        compiler_params=limit(8),
        out_shape=pltpu.VMEM(((count + pairs) * rows + SCALE_ROWS, width), jnp.int16),
        in_specs=spaces(2, pltpu.VMEM),
        out_specs=pl.BlockSpec(memory_space=pltpu.VMEM),
    )(*near_core(first, second))


def unpack_sums(ref, index, count, rows):
    pairs = count // 2
    high = ref[index * rows:(index + 1) * rows].astype(jnp.int32)
    at = (count + index % pairs) * rows
    low = ref[at:at + rows].astype(jnp.int32) + 32768
    upper = lax.shift_right_logical(low, 8)
    low = upper if index >= pairs else low - upper * 256
    scales = ref[(count + pairs) * rows:].astype(jnp.float32)
    scale = jnp.exp2(scales[index:index + 1] - BITS)
    return (high * 256 + low).astype(jnp.float32) * scale


def solve_dot(left, right):
    return lax.dot_general(
        left, right, (((1,), (1,)), ((), ())),
        precision=HIGHEST, preferred_element_type=jnp.float32,
    )


def remaining(panel_ref, update_refs, half, cb, per, rows):
    parts = []
    for c in range(cb // HALVES):
        column = (half * (cb // HALVES) + c) * rows
        block = slice(c * per, (c + 1) * per)
        count = (cb // HALVES) * per
        coded = [unpack_sums(update_refs[2], index, count, rows)[None] for index in range(c * per, (c + 1) * per)]
        update = update_refs[0][block] + update_refs[1][block] + jnp.concatenate(coded, axis=0)
        original = panel_ref[1:, :, column:column + rows]
        parts.append((original - update).reshape(per * rows, rows))
    return jnp.concatenate(parts, axis=1)


def solve_left(panel, updates, whole, lower, cb, per, rows):
    width = cb * rows
    half = width // HALVES

    def body(panel_ref, *refs):
        updates_ref = refs[:len(updates)]
        whole_ref, lower_ref, out, carried = refs[len(updates):]
        left = remaining(panel_ref, updates_ref, 0, cb, per, rows)
        out[0] = lower_ref[...]
        out[1:, :, :half] = solve_dot(left, whole_ref[:half, :half]).reshape(per, rows, half)
        carried[...] = solve_dot(left, whole_ref[half:, :half])

    return pl.pallas_call(
        body,
        name="solve_left",
        compiler_params=limit(16),
        out_shape=[
            jax.ShapeDtypeStruct((per + 1, rows, width), jnp.float32),
            pltpu.VMEM((per * rows, half), jnp.float32),
        ],
        in_specs=spaces(3 + len(updates), pltpu.VMEM),
        out_specs=spaces(2, pltpu.VMEM),
        cost_estimate=pl.CostEstimate(flops=2000000000, bytes_accessed=5000000, transcendentals=0),
    )(panel, *near_core(*updates, whole, lower))


def solve_right(panel, updates, whole, carried, out, cb, per, rows):
    width = cb * rows
    half = width // HALVES

    def body(panel_ref, *refs):
        updates_ref = refs[:len(updates)]
        whole_ref, carried_ref, _, result, stage, sem = refs[len(updates):]
        left = remaining(panel_ref, updates_ref, 1, cb, per, rows)
        value = carried_ref[...] + solve_dot(left, whole_ref[half:, half:])
        stage[...] = value.reshape(per, rows, half)
        copy = pltpu.make_async_copy(
            stage, result.at[pl.ds(1, per), :, pl.ds(half, half)], sem
        )
        copy.start()
        copy.wait()

    return pl.pallas_call(
        body,
        name="solve_right",
        compiler_params=limit(16),
        out_shape=jax.ShapeDtypeStruct((per + 1, rows, width), jnp.float32),
        in_specs=spaces(3 + len(updates), pltpu.VMEM) + spaces(1, pl.ANY),
        out_specs=pl.BlockSpec(memory_space=pl.ANY),
        scratch_shapes=[pltpu.VMEM((per, rows, half), jnp.float32), pltpu.SemaphoreType.DMA(())],
        input_output_aliases={3 + len(updates): 0},
        cost_estimate=pl.CostEstimate(flops=2000000000, bytes_accessed=5000000, transcendentals=0),
    )(panel, *near_core(*updates, whole, carried), out)


def shards(desc_panel, row_map, anc_order, anc_below, anc_panel):
    leaves = lax.axis_size("leaf")
    blk_count = lax.axis_size("blk")
    rows = anc_panel.shape[3]
    width = anc_panel.shape[4]
    cb = width // rows
    per = anc_below.shape[1] // blk_count
    assert cb == blk_count == 4 and desc_panel.shape[2] == rows
    direct = leaves <= DIRECT and leaves & (leaves - 1) == 0
    near = [(i, i ^ 1) for i in range(blk_count)]
    far = [(i, i ^ 2) for i in range(blk_count)]

    panel = anc_panel.reshape(per + 1, rows, width)
    *packed, strip = pack(desc_panel, row_map, anc_order, anc_below, panel, cb, direct)
    count = len(packed) // 2
    heads, tails = packed[:count], packed[count:]

    def exchange(arrays):
        if not direct:
            return [lax.all_to_all(arrays[0], "leaf", split_axis=0, concat_axis=0, tiled=True)]
        received = [arrays[0]]
        for k in range(1, leaves):
            swap = [(i, i ^ k) for i in range(leaves)]
            received.append(lax.ppermute(arrays[k], "leaf", swap))
        return received

    heads = exchange(heads)
    tails = exchange(tails)
    strip_far = lax.ppermute(strip, "blk", far)
    strip_near = lax.ppermute(strip, "blk", near)
    strip_both = lax.ppermute(strip_far, "blk", near)
    strips = [strip, strip_near, strip_far, strip_both]

    diagonal, codes = diagonal_update(heads, cb, leaves, rows)
    diagonal_near = lax.ppermute(diagonal, "blk", near)
    diagonal = diagonal + diagonal_near
    diagonal_far = lax.ppermute(diagonal, "blk", far)
    schur = first_factor(diagonal, diagonal_far, strips, cb, rows)

    partials = below_update(heads, tails, codes, cb, blk_count, per, leaves, rows)
    kept, for_near, for_far, for_both = (
        partials[HALVES * x:HALVES * (x + 1)] for x in range(blk_count)
    )
    from_near = []
    from_far = []
    for half in range(HALVES):
        passed = lax.ppermute(for_both[half], "blk", near)
        from_far.append(lax.ppermute(pack_sums(for_far[half], passed), "blk", far))
    for half in range(HALVES):
        from_near.append(lax.ppermute(for_near[half], "blk", near))
    whole, lower = last_factor(schur, cb, rows)
    updates = [[kept[half], from_near[half], from_far[half]] for half in range(HALVES)]
    out, carried = solve_left(panel, updates[0], whole, lower, cb, per, rows)
    out = solve_right(panel, updates[1], whole, carried, out, cb, per, rows)
    return out.reshape(anc_panel.shape)


def solution(mesh):
    in_specs = (
        P(("leaf", "blk"), None, None),
        P(("leaf", "blk"), None),
        P(),
        P(),
        P("leaf", None, "blk", None, None),
    )
    out_specs = P("leaf", None, "blk", None, None)

    return jax.shard_map(shards, mesh=mesh, in_specs=in_specs, out_specs=out_specs, check_vma=False)
```

```python
import jax
import jax.numpy as jnp
from jax import lax
from jax.experimental import pallas as pl
from jax.experimental.pallas import tpu as pltpu
from jax.sharding import PartitionSpec as P


SLOTS = 2
CODES = 4
CODE_ROWS = 8
PANEL = 8
HALVES = 2
SCALE_ROWS = 16
BITS = 23.0
LOG2E = 1.4426950408889634
DIRECT = 8
HIGHEST = lax.Precision.HIGHEST


def repeat(count, body, unroll_to=16):
    if count <= unroll_to:
        for index in range(count):
            body(index)
    else:
        lax.fori_loop(0, count, lambda index, carry: (body(index), carry)[1], 0)


def limit(mib):
    return pltpu.CompilerParams(vmem_limit_bytes=mib * 1024 * 1024)


def near_core(*arrays):
    return [pltpu.with_memory_space_constraint(array, pltpu.VMEM) for array in arrays]


def spaces(count, space):
    return [pl.BlockSpec(memory_space=space)] * count


def pack_kernel(cb, nb, direct, row_map, anc_order, anc_below, panel_hbm, anc_hbm, *refs):
    leaves = anc_order.shape[0]
    block_count, desc_count = row_map.shape
    rows = panel_hbm.shape[1] // block_count
    tail_rows = (block_count - 1) * rows
    count = leaves if direct else 1
    heads, tails = refs[:count], refs[count:2 * count]
    strip, inverse, used, chosen, codes, panel, panel_sem, strip_sem = refs[2 * count:]
    me = lax.axis_index("leaf")
    panel_copy = pltpu.make_async_copy(panel_hbm, panel, panel_sem)
    panel_copy.start()
    strip_copy = pltpu.make_async_copy(anc_hbm.at[0], strip, strip_sem)
    strip_copy.start()

    def clear(leaf):
        inverse[anc_order[leaf]] = leaf
        used[leaf] = 0
        for slot in range(SLOTS):
            chosen[leaf * SLOTS + slot] = 0
            codes[(leaf * SLOTS + slot) * CODES] = cb
            for r in range(1, CODES):
                codes[(leaf * SLOTS + slot) * CODES + r] = nb

    repeat(leaves, clear)

    def assign(desc):
        head = row_map[0, desc]
        leaf = inverse[lax.div(head, cb)]
        taken = used[leaf]
        used[leaf] = taken + 1
        place = leaf * SLOTS + taken
        chosen[place] = desc
        codes[place * CODES] = head - anc_order[leaf] * cb
        for r in range(1, block_count):
            target = row_map[r, desc]
            found = jnp.int32(nb)
            for q in range(anc_below.shape[1]):
                found = jnp.where(anc_below[leaf, q] == target, q, found)
            codes[place * CODES + r] = found

    repeat(desc_count, assign)
    panel_copy.wait()

    def write(index):
        leaf = jnp.bitwise_xor(me, index) if direct else index
        head = heads[index] if direct else heads[0].at[index]
        tail = tails[index] if direct else tails[0].at[index]
        row = lax.broadcasted_iota(jnp.int32, (CODE_ROWS, 128), 0)
        values = jnp.zeros((CODE_ROWS, 128), jnp.int32)
        for entry in range(SLOTS * CODES):
            values = jnp.where(row == entry, codes[leaf * SLOTS * CODES + entry], values)
        head[pl.ds(SLOTS * rows, CODE_ROWS)] = values.astype(jnp.float32).astype(panel.dtype)
        for slot in range(SLOTS):
            desc = chosen[leaf * SLOTS + slot]
            head[pl.ds(slot * rows, rows)] = panel[desc, pl.ds(0, rows)]
            tail[pl.ds(slot * tail_rows, tail_rows)] = panel[desc, pl.ds(rows, tail_rows)]

    repeat(leaves, write)
    strip_copy.wait()


def pack(desc_panel, row_map, anc_order, anc_below, anc, cb, direct):
    leaves = anc_order.shape[0]
    block_count = row_map.shape[1]
    rows = desc_panel.shape[1] // block_count
    width = desc_panel.shape[2]
    head = (SLOTS * rows + CODE_ROWS, width)
    tail = (SLOTS * (block_count - 1) * rows, width)
    dtype = desc_panel.dtype
    if direct:
        outs = [pltpu.VMEM(head, dtype)] * leaves + [pltpu.VMEM(tail, dtype)] * leaves
    else:
        outs = [jax.ShapeDtypeStruct((leaves,) + shape, dtype) for shape in (head, tail)]
    outs.append(pltpu.VMEM(anc.shape[1:], anc.dtype))
    nb = anc_below.shape[1]

    def body(*refs):
        pack_kernel(cb, nb, direct, *refs)

    return pl.pallas_call(
        body,
        name="pack",
        compiler_params=limit(12 if direct else 40),
        out_shape=outs,
        in_specs=spaces(3, pltpu.SMEM) + spaces(2, pl.ANY),
        out_specs=spaces(len(outs), pltpu.VMEM),
        scratch_shapes=[
            pltpu.SMEM((leaves,), jnp.int32),
            pltpu.SMEM((leaves,), jnp.int32),
            pltpu.SMEM((leaves * SLOTS,), jnp.int32),
            pltpu.SMEM((leaves * SLOTS * CODES,), jnp.int32),
            pltpu.VMEM(desc_panel.shape, dtype),
            pltpu.SemaphoreType.DMA(()),
            pltpu.SemaphoreType.DMA(()),
        ],
    )(
        *(
            pltpu.with_memory_space_constraint(array, pltpu.HBM)
            for array in (row_map.T, anc_order, anc_below, desc_panel, anc)
        )
    )


def diagonal_kernel(cb, leaves, *refs):
    heads = refs[:-4]
    out, codes, left, right = refs[-4:]
    direct = len(heads) > 1
    rows = out.shape[1]
    group = min(leaves, 8)

    def load(index, start, size):
        if direct:
            return heads[index][pl.ds(start, size)]
        return heads[0][index, pl.ds(start, size)]

    lane = lax.broadcasted_iota(jnp.int32, (1, rows), 1)

    def step(base):
        for offset in range(group):
            marks = load(base + offset, SLOTS * rows, CODE_ROWS).astype(jnp.float32)
            packed = jnp.zeros((1, rows), jnp.float32)
            for entry in range(SLOTS * CODES):
                packed = jnp.where(lane == entry, marks[entry:entry + 1], packed)
            codes[pl.ds(base + offset, 1)] = packed.astype(jnp.int32)
            for slot in range(SLOTS):
                block = load(base + offset, slot * rows, rows)
                lanes = pl.ds((offset * SLOTS + slot) * rows, rows)
                code = jnp.broadcast_to(marks[slot * CODES:slot * CODES + 1], (rows, rows))
                code = code.astype(block.dtype)
                zero = jnp.zeros_like(block)
                right[:, lanes] = jnp.where(code < cb, block, zero)
                for c in range(cb):
                    left[c * rows:(c + 1) * rows, lanes] = jnp.where(code == c, block, zero)
        return lax.dot_general(
            left[...], right[...], (((1,), (1,)), ((), ())), preferred_element_type=jnp.float32
        )

    if leaves == group:
        out[...] = step(0).reshape(out.shape)
    else:
        out[...] = jnp.zeros_like(out)

        def accumulate(index, carry):
            out[...] += step(index * group).reshape(out.shape)
            return carry

        lax.fori_loop(0, leaves // group, accumulate, 0)


def diagonal_update(heads, cb, leaves, rows):
    group = min(leaves, 8)

    def body(*refs):
        diagonal_kernel(cb, leaves, *refs)

    return pl.pallas_call(
        body,
        name="diagonal",
        compiler_params=limit(12 if len(heads) > 1 else 40),
        out_shape=[
            pltpu.VMEM((cb * rows, rows), jnp.float32),
            jax.ShapeDtypeStruct((leaves, rows), jnp.int32),
        ],
        in_specs=spaces(len(heads), pltpu.VMEM),
        out_specs=spaces(2, pltpu.VMEM),
        scratch_shapes=[
            pltpu.VMEM((cb * rows, group * SLOTS * rows), heads[0].dtype),
            pltpu.VMEM((rows, group * SLOTS * rows), heads[0].dtype),
        ],
        cost_estimate=pl.CostEstimate(flops=2000000000, bytes_accessed=1000000, transcendentals=0),
    )(*(near_core(*heads) if len(heads) > 1 else heads))


def below_kernel(cb, blk_count, per, leaves, count, codes, *refs):
    tails, refs = refs[:count], refs[count:]
    heads = refs[:count]
    outs = refs[count:count + blk_count * HALVES]
    acc, products = refs[count + blk_count * HALVES:]
    direct = count > 1
    me_blk = lax.axis_index("blk")
    rows = acc.shape[1]
    group = min(leaves, 8)
    tail_rows = tails[0].shape[-2] // SLOTS
    extra = tail_rows // rows
    blocks = blk_count * cb * per

    for first in range(0, blocks, cb):
        acc[pl.ds(first, cb)] = jnp.zeros((cb, rows, rows), jnp.float32)

    def step(base):
        for offset in range(group):
            index = base + offset
            for slot in range(SLOTS):
                if direct:
                    head = heads[index][pl.ds(slot * rows, rows)]
                    tail = tails[index][pl.ds(slot * tail_rows, tail_rows)]
                else:
                    head = heads[0][index, pl.ds(slot * rows, rows)]
                    tail = tails[0][index, pl.ds(slot * tail_rows, tail_rows)]
                products[offset * SLOTS + slot] = lax.dot_general(
                    tail, head, (((1,), (1,)), ((), ())), preferred_element_type=jnp.float32
                )
        for offset in range(group):
            for slot in range(SLOTS):
                column = codes[base + offset, slot * CODES]
                for r in range(extra):
                    position = codes[base + offset, slot * CODES + 1 + r]
                    relative = jnp.bitwise_xor(lax.rem(position, blk_count), me_blk)
                    place = (relative * cb + column) * per + lax.div(position, blk_count)
                    place = jnp.where(column < cb, place, blocks)
                    acc[place] += products[offset * SLOTS + slot, pl.ds(r * rows, rows)]

    if leaves == group:
        step(0)
    else:
        lax.fori_loop(0, leaves // group, lambda index, carry: (step(index * group), carry)[1], 0)
    size = cb * per // HALVES
    for part, out in enumerate(outs):
        out[...] = acc[pl.ds(part * size, size)]


def below_update(heads, tails, codes, cb, blk_count, per, leaves, rows):
    group = min(leaves, 8)
    blocks = blk_count * cb * per
    outs = blk_count * HALVES

    def body(*refs):
        below_kernel(cb, blk_count, per, leaves, len(heads), *refs)

    return pl.pallas_call(
        body,
        name="below",
        compiler_params=limit(16 if len(heads) > 1 else 56),
        out_shape=[pltpu.VMEM((cb * per // HALVES, rows, rows), jnp.float32)] * outs,
        in_specs=spaces(1, pltpu.SMEM) + spaces(2 * len(heads), pltpu.VMEM),
        out_specs=spaces(outs, pltpu.VMEM),
        scratch_shapes=[
            pltpu.VMEM((blocks + 1, rows, rows), jnp.float32),
            pltpu.VMEM((group * SLOTS, tails[0].shape[-2] // SLOTS, rows), jnp.float32),
        ],
        cost_estimate=pl.CostEstimate(flops=2000000000, bytes_accessed=4000000, transcendentals=0),
    )(codes, *(near_core(*tails, *heads) if len(heads) > 1 else [*tails, *heads]))


def factor_block(work, rows):
    lane = lax.broadcasted_iota(jnp.int32, (1, rows), 1)
    sub = lax.broadcasted_iota(jnp.int32, (PANEL, 1), 0)
    segments = 4
    size = rows // segments

    for segment in range(segments):
        top = segment * size

        def panel(index, carry):
            base = pl.multiple_of(top + index * PANEL, PANEL)
            strip = work[pl.ds(base, PANEL), :]
            raw = work[top:, :rows]
            picks = [(lane == base + k) for k in range(PANEL)]
            corner = [
                jnp.sum(jnp.where(picks[k], strip[:, :rows], 0.0), axis=1, keepdims=True)
                for k in range(PANEL)
            ]
            factor = jnp.zeros((PANEL, 2 * rows), jnp.float32)
            for k in range(PANEL):
                scale = lax.rsqrt(corner[k][k:k + 1])
                inverse = scale * scale
                row = strip[k:k + 1]
                factor = jnp.where(sub == k, row * scale, factor)
                scaled = row * inverse
                strip = jnp.where(sub == k, scaled, strip - corner[k] * scaled)
                for m in range(k + 1, PANEL):
                    entry = corner[m][k:k + 1]
                    corner[m] = jnp.where(
                        sub == k, entry * inverse, corner[m] - (corner[k] * entry) * inverse
                    )
            work[pl.ds(base, PANEL), :] = factor
            for start, stop, masked in ((top, top + size, True), (top + size, rows, False)):
                if start == stop:
                    continue
                full = work[start:stop, :]
                row_id = lax.broadcasted_iota(jnp.int32, (stop - start, 1), 0) + start
                for k in range(PANEL):
                    column = jnp.sum(
                        jnp.where(picks[k], raw[start - top:stop - top], 0.0), axis=1, keepdims=True
                    )
                    if masked:
                        column = jnp.where(row_id >= base + PANEL, column, 0.0)
                    full = full - column * strip[k:k + 1]
                work[start:stop, :] = full
            return carry

        lax.fori_loop(0, size // PANEL, panel, 0)


def triangle(rows):
    row = lax.broadcasted_iota(jnp.int32, (rows, rows), 0)
    return row, lax.broadcasted_iota(jnp.int32, (rows, rows), 1)


def fold_sums(first, second, cb, rows):
    def body(first_ref, second_ref, total, folded):
        row, col = triangle(rows)
        line = lax.broadcasted_iota(jnp.int32, (PANEL, rows), 0)
        marks = jnp.zeros((PANEL, rows), jnp.float32)
        total[...] = first_ref[...] + second_ref[...]
        for pair in range(cb // 2):
            lower = total[2 * pair * rows:(2 * pair + 1) * rows]
            upper = total[(2 * pair + 1) * rows:(2 * pair + 2) * rows]
            folded[pair * rows:(pair + 1) * rows] = jnp.where(row >= col, lower, upper)
            edge = jnp.sum(jnp.where(row == col, upper, 0.0), axis=0, keepdims=True)
            marks = jnp.where(line == pair, edge, marks)
        folded[cb // 2 * rows:] = marks

    return pl.pallas_call(
        body,
        name="fold_sums",
        compiler_params=limit(8),
        out_shape=[
            pltpu.VMEM((cb * rows, rows), jnp.float32),
            pltpu.VMEM((cb // 2 * rows + PANEL, rows), jnp.float32),
        ],
        in_specs=spaces(2, pltpu.VMEM),
        out_specs=spaces(2, pltpu.VMEM),
    )(*near_core(first, second))


def unfold_sums(folded, cb, rows):
    row, col = triangle(rows)
    blocks = []
    for pair in range(cb // 2):
        square = folded[pair * rows:(pair + 1) * rows]
        edge = folded[cb // 2 * rows + pair:cb // 2 * rows + pair + 1]
        lower = jnp.where(row > col, square, 0.0)
        upper = jnp.where(row < col, square, 0.0)
        blocks.append(lower + lower.T + jnp.where(row == col, square, 0.0))
        blocks.append(upper + upper.T + jnp.where(row == col, edge, 0.0))
    return blocks


def small_dot(left, right, dims):
    return lax.dot_general(
        left, right, (dims, ((), ())), precision=HIGHEST, preferred_element_type=jnp.float32
    )


def write_inverse(out, first, second, between, rows):
    out[:rows, :rows] = first
    out[:rows, rows:] = jnp.zeros_like(first)
    out[rows:, rows:] = second
    product = small_dot(between, first, ((0,), (0,)))
    out[rows:, :rows] = -small_dot(second, product, ((1,), (0,)))


def eliminate(block, work, rows):
    row, col = triangle(rows)
    work[:, :rows] = block
    work[:, rows:] = (row == col).astype(jnp.float32)
    factor_block(work, rows)
    return jnp.where(row <= col, work[:, :rows], 0.0), work[:, rows:]


def first_factor(own_sum, other_sum, strips, cb, rows):
    blk_count = len(strips)
    half = cb // HALVES

    def body(own_ref, other_ref, *refs):
        strip_refs = refs[:blk_count]
        schur, lead, inverses, work = refs[blk_count:]
        me = lax.axis_index("blk")
        for x in range(blk_count):
            schur[jnp.bitwise_xor(me, x)] = strip_refs[x][...]
        others = unfold_sums(other_ref, cb, rows)
        for c in range(cb):
            part = slice(c * rows, (c + 1) * rows)
            schur[c, :, part] -= own_ref[part] + others[c]
        for block in range(half):
            here = block * rows
            upper, inverse = eliminate(schur[block, :, here:here + rows], work, rows)
            schur[block, :, here:here + rows] = upper
            inverses[block] = inverse
            after = here + rows
            strip = small_dot(inverse, schur[block, :, after:], ((1,), (0,)))
            schur[block, :, after:] = strip
            for other in range(block + 1, cb):
                offset = (other - block - 1) * rows
                schur[other, :, other * rows:] -= small_dot(
                    strip[:, offset:offset + rows], strip[:, offset:], ((0,), (0,))
                )
        write_inverse(lead, inverses[0], inverses[1], schur[0, :, rows:2 * rows], rows)

    return pl.pallas_call(
        body,
        name="factor_first",
        compiler_params=limit(12),
        out_shape=[
            pltpu.VMEM((cb, rows, cb * rows), jnp.float32),
            pltpu.VMEM((half * rows, half * rows), jnp.float32),
        ],
        in_specs=spaces(2 + blk_count, pltpu.VMEM),
        out_specs=spaces(2, pltpu.VMEM),
        scratch_shapes=[
            pltpu.VMEM((half, rows, rows), jnp.float32),
            pltpu.VMEM((rows, 2 * rows), jnp.float32),
        ],
        cost_estimate=pl.CostEstimate(flops=10000000000, bytes_accessed=2000000, transcendentals=0),
    )(*near_core(own_sum, other_sum, *strips))


def middle_factor(schur, cb, rows):
    def body(schur_ref, strip, corner, inverse_ref, work):
        block = cb // HALVES
        here = block * rows
        upper, inverse = eliminate(schur_ref[block, :, here:here + rows], work, rows)
        side = small_dot(inverse, schur_ref[block, :, here + rows:], ((1,), (0,)))
        strip[:, :rows] = upper
        strip[:, rows:] = side
        inverse_ref[...] = inverse
        corner[...] = schur_ref[cb - 1, :, here + rows:] - small_dot(side, side, ((0,), (0,)))

    return pl.pallas_call(
        body,
        name="factor_middle",
        compiler_params=limit(8),
        out_shape=[
            pltpu.VMEM((rows, 2 * rows), jnp.float32),
            pltpu.VMEM((rows, rows), jnp.float32),
            pltpu.VMEM((rows, rows), jnp.float32),
        ],
        in_specs=spaces(1, pltpu.VMEM),
        out_specs=spaces(3, pltpu.VMEM),
        scratch_shapes=[pltpu.VMEM((rows, 2 * rows), jnp.float32)],
        cost_estimate=pl.CostEstimate(flops=5000000000, bytes_accessed=1000000, transcendentals=0),
    )(*near_core(schur))


def last_factor(schur, strip, corner, inverse, cb, rows):
    half = cb // HALVES

    def body(schur_ref, strip_ref, corner_ref, inverse_ref, trail, lower, work):
        me = lax.axis_index("blk")
        upper, last = eliminate(corner_ref[...], work, rows)
        write_inverse(trail, inverse_ref[...], last, strip_ref[:, rows:], rows)
        mine = pl.ds(pl.multiple_of(me * rows, rows), rows)
        late = pl.ds(pl.multiple_of(jnp.maximum(me - half, 0) * rows, rows), rows)
        pieces = [schur_ref[k, :, mine] for k in range(half)] + [strip_ref[:, late], upper]
        for k in range(cb):
            lower[:, k * rows:(k + 1) * rows] = jnp.where(k <= me, pieces[k], 0.0).T

    return pl.pallas_call(
        body,
        name="factor_last",
        compiler_params=limit(8),
        out_shape=[
            pltpu.VMEM((half * rows, half * rows), jnp.float32),
            pltpu.VMEM((rows, cb * rows), jnp.float32),
        ],
        in_specs=spaces(4, pltpu.VMEM),
        out_specs=spaces(2, pltpu.VMEM),
        scratch_shapes=[pltpu.VMEM((rows, 2 * rows), jnp.float32)],
        cost_estimate=pl.CostEstimate(flops=5000000000, bytes_accessed=1000000, transcendentals=0),
    )(*near_core(schur, strip, corner, inverse))


def pack_sums(first, second):
    count, rows, width = first.shape
    pairs = count // 2

    def body(first_ref, second_ref, out):
        row = lax.broadcasted_iota(jnp.int32, (SCALE_ROWS, width), 0)
        scales = jnp.zeros((SCALE_ROWS, width), jnp.int32)
        lows = []
        for j in range(count):
            value = first_ref[j] + second_ref[j]
            peak = jnp.maximum(jnp.max(jnp.abs(value), axis=0, keepdims=True), 1e-30)
            power = jnp.floor(jnp.log(peak) * LOG2E + 1e-3) + 1.0
            scales = jnp.where(row == j, power.astype(jnp.int32), scales)
            whole = jnp.floor(value * jnp.exp2(BITS - power) + 0.5).astype(jnp.int32)
            high = lax.shift_right_arithmetic(whole, 8)
            lows.append(whole - high * 256)
            out[j * rows:(j + 1) * rows] = high.astype(jnp.int16)
        for j in range(pairs):
            low = lows[j] + lows[j + pairs] * 256 - 32768
            out[(count + j) * rows:(count + j + 1) * rows] = low.astype(jnp.int16)
        out[(count + pairs) * rows:] = scales.astype(jnp.int16)

    return pl.pallas_call(
        body,
        name="pack_sums",
        compiler_params=limit(8),
        out_shape=pltpu.VMEM(((count + pairs) * rows + SCALE_ROWS, width), jnp.int16),
        in_specs=spaces(2, pltpu.VMEM),
        out_specs=pl.BlockSpec(memory_space=pltpu.VMEM),
    )(*near_core(first, second))


def unpack_sums(ref, index, count, rows):
    pairs = count // 2
    high = ref[index * rows:(index + 1) * rows].astype(jnp.int32)
    at = (count + index % pairs) * rows
    low = ref[at:at + rows].astype(jnp.int32) + 32768
    upper = lax.shift_right_logical(low, 8)
    low = upper if index >= pairs else low - upper * 256
    scales = ref[(count + pairs) * rows:].astype(jnp.float32)
    scale = jnp.exp2(scales[index:index + 1] - BITS)
    return (high * 256 + low).astype(jnp.float32) * scale


def remaining(panel_ref, update_refs, half, cb, per, rows):
    parts = []
    for c in range(cb // HALVES):
        column = (half * (cb // HALVES) + c) * rows
        block = slice(c * per, (c + 1) * per)
        count = (cb // HALVES) * per
        coded = [unpack_sums(update_refs[2], index, count, rows)[None] for index in range(c * per, (c + 1) * per)]
        update = update_refs[0][block] + update_refs[1][block] + jnp.concatenate(coded, axis=0)
        original = panel_ref[1:, :, column:column + rows]
        parts.append((original - update).reshape(per * rows, rows))
    return jnp.concatenate(parts, axis=1)


def solve_left(panel, updates, lead, schur, lower, cb, per, rows):
    width = cb * rows
    half = width // HALVES

    def body(panel_ref, *refs):
        updates_ref = refs[:len(updates)]
        lead_ref, schur_ref, lower_ref, out, carried = refs[len(updates):]
        left = remaining(panel_ref, updates_ref, 0, cb, per, rows)
        out[0] = lower_ref[...]
        value = small_dot(left, lead_ref[...], ((1,), (1,)))
        out[1:, :, :half] = value.reshape(per, rows, half)
        across = schur_ref[:cb // HALVES, :, half:].reshape(half, half)
        carried[...] = small_dot(value, across, ((1,), (0,)))

    return pl.pallas_call(
        body,
        name="solve_left",
        compiler_params=limit(16),
        out_shape=[
            jax.ShapeDtypeStruct((per + 1, rows, width), jnp.float32),
            pltpu.VMEM((per * rows, half), jnp.float32),
        ],
        in_specs=spaces(4 + len(updates), pltpu.VMEM),
        out_specs=spaces(2, pltpu.VMEM),
        cost_estimate=pl.CostEstimate(flops=2000000000, bytes_accessed=5000000, transcendentals=0),
    )(panel, *near_core(*updates, lead, schur, lower))


def solve_right(panel, updates, trail, carried, out, cb, per, rows):
    width = cb * rows
    half = width // HALVES

    def body(panel_ref, *refs):
        updates_ref = refs[:len(updates)]
        trail_ref, carried_ref, _, result, stage, sem = refs[len(updates):]
        left = remaining(panel_ref, updates_ref, 1, cb, per, rows) - carried_ref[...]
        value = small_dot(left, trail_ref[...], ((1,), (1,)))
        stage[...] = value.reshape(per, rows, half)
        copy = pltpu.make_async_copy(
            stage, result.at[pl.ds(1, per), :, pl.ds(half, half)], sem
        )
        copy.start()
        copy.wait()

    return pl.pallas_call(
        body,
        name="solve_right",
        compiler_params=limit(16),
        out_shape=jax.ShapeDtypeStruct((per + 1, rows, width), jnp.float32),
        in_specs=spaces(3 + len(updates), pltpu.VMEM) + spaces(1, pl.ANY),
        out_specs=pl.BlockSpec(memory_space=pl.ANY),
        scratch_shapes=[pltpu.VMEM((per, rows, half), jnp.float32), pltpu.SemaphoreType.DMA(())],
        input_output_aliases={3 + len(updates): 0},
        cost_estimate=pl.CostEstimate(flops=2000000000, bytes_accessed=5000000, transcendentals=0),
    )(panel, *near_core(*updates, trail, carried), out)


def shards(desc_panel, row_map, anc_order, anc_below, anc_panel):
    leaves = lax.axis_size("leaf")
    blk_count = lax.axis_size("blk")
    rows = anc_panel.shape[3]
    width = anc_panel.shape[4]
    cb = width // rows
    per = anc_below.shape[1] // blk_count
    assert cb == blk_count == 4 and desc_panel.shape[2] == rows
    direct = leaves <= DIRECT and leaves & (leaves - 1) == 0
    near = [(i, i ^ 1) for i in range(blk_count)]
    far = [(i, i ^ 2) for i in range(blk_count)]

    panel = anc_panel.reshape(per + 1, rows, width)
    *packed, strip = pack(desc_panel, row_map, anc_order, anc_below, panel, cb, direct)
    count = len(packed) // 2
    heads, tails = packed[:count], packed[count:]

    def exchange(arrays):
        if not direct:
            return [lax.all_to_all(arrays[0], "leaf", split_axis=0, concat_axis=0, tiled=True)]
        received = [arrays[0]]
        for k in range(1, leaves):
            swap = [(i, i ^ k) for i in range(leaves)]
            received.append(lax.ppermute(arrays[k], "leaf", swap))
        return received

    heads = exchange(heads)
    tails = exchange(tails)
    strip_far = lax.ppermute(strip, "blk", far)
    strip_near = lax.ppermute(strip, "blk", near)
    strip_both = lax.ppermute(strip_far, "blk", near)
    strips = [strip, strip_near, strip_far, strip_both]

    diagonal, codes = diagonal_update(heads, cb, leaves, rows)
    diagonal_near = lax.ppermute(diagonal, "blk", near)
    diagonal, folded = fold_sums(diagonal, diagonal_near, cb, rows)
    folded = lax.ppermute(folded, "blk", far)
    schur, lead = first_factor(diagonal, folded, strips, cb, rows)

    partials = below_update(heads, tails, codes, cb, blk_count, per, leaves, rows)
    kept, for_near, for_far, for_both = (
        partials[HALVES * x:HALVES * (x + 1)] for x in range(blk_count)
    )
    from_near = []
    from_far = []
    for half in range(HALVES):
        passed = lax.ppermute(for_both[half], "blk", near)
        from_far.append(lax.ppermute(pack_sums(for_far[half], passed), "blk", far))
    for half in range(HALVES):
        from_near.append(lax.ppermute(for_near[half], "blk", near))
    strip, corner, inverse = middle_factor(schur, cb, rows)
    trail, lower = last_factor(schur, strip, corner, inverse, cb, rows)
    updates = [[kept[half], from_near[half], from_far[half]] for half in range(HALVES)]
    out, carried = solve_left(panel, updates[0], lead, schur, lower, cb, per, rows)
    out = solve_right(panel, updates[1], trail, carried, out, cb, per, rows)
    return out.reshape(anc_panel.shape)


def solution(mesh):
    in_specs = (
        P(("leaf", "blk"), None, None),
        P(("leaf", "blk"), None),
        P(),
        P(),
        P("leaf", None, "blk", None, None),
    )
    out_specs = P("leaf", None, "blk", None, None)

    return jax.shard_map(shards, mesh=mesh, in_specs=in_specs, out_specs=out_specs, check_vma=False)
```

```python
import jax
import jax.numpy as jnp
from jax import lax
from jax.experimental import pallas as pl
from jax.experimental.pallas import tpu as pltpu
from jax.sharding import PartitionSpec as P


SLOTS = 2
CODES = 4
CODE_ROWS = 8
PANEL = 8
HALVES = 2
SCALE_ROWS = 16
BITS = 23.0
LOG2E = 1.4426950408889634
DIRECT = 8
HIGHEST = lax.Precision.HIGHEST


def repeat(count, body, unroll_to=16):
    if count <= unroll_to:
        for index in range(count):
            body(index)
    else:
        lax.fori_loop(0, count, lambda index, carry: (body(index), carry)[1], 0)


def limit(mib):
    return pltpu.CompilerParams(vmem_limit_bytes=mib * 1024 * 1024)


def near_core(*arrays):
    return [pltpu.with_memory_space_constraint(array, pltpu.VMEM) for array in arrays]


def spaces(count, space):
    return [pl.BlockSpec(memory_space=space)] * count


def pack_kernel(cb, direct, row_map, anc_order, panel_hbm, anc_hbm, *refs):
    leaves = anc_order.shape[0]
    block_count, desc_count = row_map.shape
    rows = panel_hbm.shape[1] // block_count
    tail_rows = (block_count - 1) * rows
    count = leaves if direct else 1
    heads, tails = refs[:count], refs[count:2 * count]
    strip, inverse, used, chosen, codes, panel, panel_sem, strip_sem = refs[2 * count:]
    me = lax.axis_index("leaf")
    panel_copy = pltpu.make_async_copy(panel_hbm, panel, panel_sem)
    panel_copy.start()
    strip_copy = pltpu.make_async_copy(anc_hbm.at[0], strip, strip_sem)
    strip_copy.start()

    def clear(leaf):
        inverse[anc_order[leaf]] = leaf
        used[leaf] = 0
        for slot in range(SLOTS):
            chosen[leaf * SLOTS + slot] = 0
            codes[(leaf * SLOTS + slot) * CODES] = cb
            for r in range(1, CODES):
                codes[(leaf * SLOTS + slot) * CODES + r] = 0

    repeat(leaves, clear)

    def assign(desc):
        head = row_map[0, desc]
        leaf = inverse[lax.div(head, cb)]
        taken = used[leaf]
        used[leaf] = taken + 1
        place = leaf * SLOTS + taken
        chosen[place] = desc
        codes[place * CODES] = head - anc_order[leaf] * cb
        for r in range(1, block_count):
            codes[place * CODES + r] = row_map[r, desc] - leaves * cb

    repeat(desc_count, assign)
    panel_copy.wait()

    def write(index):
        leaf = jnp.bitwise_xor(me, index) if direct else index
        head = heads[index] if direct else heads[0].at[index]
        tail = tails[index] if direct else tails[0].at[index]
        row = lax.broadcasted_iota(jnp.int32, (CODE_ROWS, 128), 0)
        values = jnp.zeros((CODE_ROWS, 128), jnp.int32)
        for entry in range(SLOTS * CODES):
            values = jnp.where(row == entry, codes[leaf * SLOTS * CODES + entry], values)
        head[pl.ds(SLOTS * rows, CODE_ROWS)] = values.astype(jnp.float32).astype(panel.dtype)
        for slot in range(SLOTS):
            desc = chosen[leaf * SLOTS + slot]
            head[pl.ds(slot * rows, rows)] = panel[desc, pl.ds(0, rows)]
            tail[pl.ds(slot * tail_rows, tail_rows)] = panel[desc, pl.ds(rows, tail_rows)]

    repeat(leaves, write)
    strip_copy.wait()


def pack(desc_panel, row_map, anc_order, anc, cb, direct):
    leaves = anc_order.shape[0]
    block_count = row_map.shape[1]
    rows = desc_panel.shape[1] // block_count
    width = desc_panel.shape[2]
    head = (SLOTS * rows + CODE_ROWS, width)
    tail = (SLOTS * (block_count - 1) * rows, width)
    dtype = desc_panel.dtype
    if direct:
        outs = [pltpu.VMEM(head, dtype)] * leaves + [pltpu.VMEM(tail, dtype)] * leaves
    else:
        outs = [jax.ShapeDtypeStruct((leaves,) + shape, dtype) for shape in (head, tail)]
    outs.append(pltpu.VMEM(anc.shape[1:], anc.dtype))

    def body(*refs):
        pack_kernel(cb, direct, *refs)

    return pl.pallas_call(
        body,
        name="pack",
        compiler_params=limit(12 if direct else 40),
        out_shape=outs,
        in_specs=spaces(2, pltpu.SMEM) + spaces(2, pl.ANY),
        out_specs=spaces(len(outs), pltpu.VMEM),
        scratch_shapes=[
            pltpu.SMEM((leaves,), jnp.int32),
            pltpu.SMEM((leaves,), jnp.int32),
            pltpu.SMEM((leaves * SLOTS,), jnp.int32),
            pltpu.SMEM((leaves * SLOTS * CODES,), jnp.int32),
            pltpu.VMEM(desc_panel.shape, dtype),
            pltpu.SemaphoreType.DMA(()),
            pltpu.SemaphoreType.DMA(()),
        ],
    )(
        *(
            pltpu.with_memory_space_constraint(array, pltpu.HBM)
            for array in (row_map.T, anc_order, desc_panel, anc)
        )
    )


def diagonal_kernel(cb, leaves, anc_below, *refs):
    heads = refs[:-4]
    out, codes, left, right = refs[-4:]
    direct = len(heads) > 1
    rows = out.shape[1]
    group = min(leaves, 8)

    def load(index, start, size):
        if direct:
            return heads[index][pl.ds(start, size)]
        return heads[0][index, pl.ds(start, size)]

    lane = lax.broadcasted_iota(jnp.int32, (1, rows), 1)

    def step(base):
        for offset in range(group):
            marks = load(base + offset, SLOTS * rows, CODE_ROWS).astype(jnp.float32)
            packed = jnp.zeros((1, rows), jnp.float32)
            for entry in range(SLOTS * CODES):
                packed = jnp.where(lane == entry, marks[entry:entry + 1], packed)
            codes[pl.ds(base + offset, 1)] = packed.astype(jnp.int32)
            for slot in range(SLOTS):
                block = load(base + offset, slot * rows, rows)
                lanes = pl.ds((offset * SLOTS + slot) * rows, rows)
                code = jnp.broadcast_to(marks[slot * CODES:slot * CODES + 1], (rows, rows))
                code = code.astype(block.dtype)
                zero = jnp.zeros_like(block)
                right[:, lanes] = jnp.where(code < cb, block, zero)
                for c in range(cb):
                    left[c * rows:(c + 1) * rows, lanes] = jnp.where(code == c, block, zero)
        return lax.dot_general(
            left[...], right[...], (((1,), (1,)), ((), ())), preferred_element_type=jnp.float32
        )

    def locate(first, size):
        ids = codes[pl.ds(first, size)] + leaves * cb
        found = jnp.zeros_like(ids)
        me = lax.axis_index("leaf")
        for q in range(anc_below.shape[1]):
            found = jnp.where(ids == anc_below[me, q], q, found)
        codes[pl.ds(first, size)] = jnp.where(
            lax.rem(lane, CODES) == 0, codes[pl.ds(first, size)], found
        )

    if leaves == group:
        out[...] = step(0).reshape(out.shape)
        locate(0, group)
    else:
        out[...] = jnp.zeros_like(out)

        def accumulate(index, carry):
            first = pl.multiple_of(index * group, group)
            out[...] += step(first).reshape(out.shape)
            locate(first, group)
            return carry

        lax.fori_loop(0, leaves // group, accumulate, 0)


def diagonal_update(heads, anc_below, cb, leaves, rows):
    group = min(leaves, 8)

    def body(*refs):
        diagonal_kernel(cb, leaves, *refs)

    return pl.pallas_call(
        body,
        name="diagonal",
        compiler_params=limit(12 if len(heads) > 1 else 40),
        out_shape=[
            pltpu.VMEM((cb * rows, rows), jnp.float32),
            jax.ShapeDtypeStruct((leaves, rows), jnp.int32),
        ],
        in_specs=spaces(1, pltpu.SMEM) + spaces(len(heads), pltpu.VMEM),
        out_specs=spaces(2, pltpu.VMEM),
        scratch_shapes=[
            pltpu.VMEM((cb * rows, group * SLOTS * rows), heads[0].dtype),
            pltpu.VMEM((rows, group * SLOTS * rows), heads[0].dtype),
        ],
        cost_estimate=pl.CostEstimate(flops=2000000000, bytes_accessed=1000000, transcendentals=0),
    )(anc_below, *(near_core(*heads) if len(heads) > 1 else heads))


def below_kernel(cb, blk_count, per, leaves, count, parts, codes, *refs):
    tails, refs = refs[:count], refs[count:]
    heads = refs[:count]
    outs = refs[count:count + len(parts)]
    acc, products = refs[count + len(parts):]
    direct = count > 1
    me_blk = lax.axis_index("blk")
    rows = acc.shape[1]
    group = min(leaves, 8)
    tail_rows = tails[0].shape[-2] // SLOTS
    extra = tail_rows // rows
    size = cb * per // HALVES
    trash = len(parts) * size
    for first in range(0, trash, size):
        acc[pl.ds(first, size)] = jnp.zeros((size, rows, rows), jnp.float32)

    def step(base):
        for offset in range(group):
            index = base + offset
            for slot in range(SLOTS):
                if direct:
                    head = heads[index][pl.ds(slot * rows, rows)]
                    tail = tails[index][pl.ds(slot * tail_rows, tail_rows)]
                else:
                    head = heads[0][index, pl.ds(slot * rows, rows)]
                    tail = tails[0][index, pl.ds(slot * tail_rows, tail_rows)]
                products[offset * SLOTS + slot] = lax.dot_general(
                    tail, head, (((1,), (1,)), ((), ())), preferred_element_type=jnp.float32
                )
        for offset in range(group):
            for slot in range(SLOTS):
                column = codes[base + offset, slot * CODES]
                for r in range(extra):
                    position = codes[base + offset, slot * CODES + 1 + r]
                    relative = jnp.bitwise_xor(lax.rem(position, blk_count), me_blk)
                    part = relative * HALVES + lax.div(column * HALVES, cb)
                    start = jnp.int32(-1)
                    for at, (x, half) in enumerate(parts):
                        start = jnp.where(part == x * HALVES + half, at * size, start)
                    inside = lax.rem(column, cb // HALVES) * per + lax.div(position, blk_count)
                    place = jnp.where((column < cb) & (start >= 0), start + inside, trash)
                    acc[place] += products[offset * SLOTS + slot, pl.ds(r * rows, rows)]

    if leaves == group:
        step(0)
    else:
        lax.fori_loop(0, leaves // group, lambda index, carry: (step(index * group), carry)[1], 0)
    for at, out in enumerate(outs):
        out[...] = acc[pl.ds(at * size, size)]


def below_update(heads, tails, codes, parts, cb, blk_count, per, leaves, rows):
    group = min(leaves, 8)
    size = cb * per // HALVES

    def body(*refs):
        below_kernel(cb, blk_count, per, leaves, len(heads), parts, *refs)

    results = pl.pallas_call(
        body,
        compiler_params=limit(16 if len(heads) > 1 else 56),
        out_shape=[pltpu.VMEM((size, rows, rows), jnp.float32)] * len(parts),
        in_specs=spaces(1, pltpu.SMEM) + spaces(2 * len(heads), pltpu.VMEM),
        out_specs=spaces(len(parts), pltpu.VMEM),
        scratch_shapes=[
            pltpu.VMEM((len(parts) * size + 1, rows, rows), jnp.float32),
            pltpu.VMEM((group * SLOTS, tails[0].shape[-2] // SLOTS, rows), jnp.float32),
        ],
        cost_estimate=pl.CostEstimate(flops=2000000000, bytes_accessed=4000000, transcendentals=0),
    )(codes, *(near_core(*tails, *heads) if len(heads) > 1 else [*tails, *heads]))
    return dict(zip(parts, results))


def factor_block(work, rows):
    lane = lax.broadcasted_iota(jnp.int32, (1, rows), 1)
    sub = lax.broadcasted_iota(jnp.int32, (PANEL, 1), 0)
    segments = 4
    size = rows // segments

    for segment in range(segments):
        top = segment * size

        def panel(index, carry):
            base = pl.multiple_of(top + index * PANEL, PANEL)
            strip = work[pl.ds(base, PANEL), :]
            raw = work[top:, :rows]
            picks = [(lane == base + k) for k in range(PANEL)]
            corner = [
                jnp.sum(jnp.where(picks[k], strip[:, :rows], 0.0), axis=1, keepdims=True)
                for k in range(PANEL)
            ]
            factor = jnp.zeros((PANEL, 2 * rows), jnp.float32)
            for k in range(PANEL):
                scale = lax.rsqrt(corner[k][k:k + 1])
                inverse = scale * scale
                row = strip[k:k + 1]
                factor = jnp.where(sub == k, row * scale, factor)
                scaled = row * inverse
                strip = jnp.where(sub == k, scaled, strip - corner[k] * scaled)
                for m in range(k + 1, PANEL):
                    entry = corner[m][k:k + 1]
                    corner[m] = jnp.where(
                        sub == k, entry * inverse, corner[m] - (corner[k] * entry) * inverse
                    )
            work[pl.ds(base, PANEL), :] = factor
            for start, stop, masked in ((top, top + size, True), (top + size, rows, False)):
                if start == stop:
                    continue
                full = work[start:stop, :]
                row_id = lax.broadcasted_iota(jnp.int32, (stop - start, 1), 0) + start
                for k in range(PANEL):
                    column = jnp.sum(
                        jnp.where(picks[k], raw[start - top:stop - top], 0.0), axis=1, keepdims=True
                    )
                    if masked:
                        column = jnp.where(row_id >= base + PANEL, column, 0.0)
                    full = full - column * strip[k:k + 1]
                work[start:stop, :] = full
            return carry

        lax.fori_loop(0, size // PANEL, panel, 0)


def triangle(rows):
    row = lax.broadcasted_iota(jnp.int32, (rows, rows), 0)
    return row, lax.broadcasted_iota(jnp.int32, (rows, rows), 1)


def fold_sums(first, second, cb, rows):
    def body(first_ref, second_ref, total, folded):
        row, col = triangle(rows)
        line = lax.broadcasted_iota(jnp.int32, (PANEL, rows), 0)
        marks = jnp.zeros((PANEL, rows), jnp.float32)
        total[...] = first_ref[...] + second_ref[...]
        for pair in range(cb // 2):
            lower = total[2 * pair * rows:(2 * pair + 1) * rows]
            upper = total[(2 * pair + 1) * rows:(2 * pair + 2) * rows]
            folded[pair * rows:(pair + 1) * rows] = jnp.where(row >= col, lower, upper)
            edge = jnp.sum(jnp.where(row == col, upper, 0.0), axis=0, keepdims=True)
            marks = jnp.where(line == pair, edge, marks)
        folded[cb // 2 * rows:] = marks

    return pl.pallas_call(
        body,
        name="fold_sums",
        compiler_params=limit(8),
        out_shape=[
            pltpu.VMEM((cb * rows, rows), jnp.float32),
            pltpu.VMEM((cb // 2 * rows + PANEL, rows), jnp.float32),
        ],
        in_specs=spaces(2, pltpu.VMEM),
        out_specs=spaces(2, pltpu.VMEM),
    )(*near_core(first, second))


def unfold_sums(folded, cb, rows):
    row, col = triangle(rows)
    blocks = []
    for pair in range(cb // 2):
        square = folded[pair * rows:(pair + 1) * rows]
        edge = folded[cb // 2 * rows + pair:cb // 2 * rows + pair + 1]
        lower = jnp.where(row > col, square, 0.0)
        upper = jnp.where(row < col, square, 0.0)
        blocks.append(lower + lower.T + jnp.where(row == col, square, 0.0))
        blocks.append(upper + upper.T + jnp.where(row == col, edge, 0.0))
    return blocks


def small_dot(left, right, dims):
    return lax.dot_general(
        left, right, (dims, ((), ())), precision=HIGHEST, preferred_element_type=jnp.float32
    )


def write_inverse(out, first, second, between, rows):
    out[:rows, :rows] = first
    out[:rows, rows:] = jnp.zeros_like(first)
    out[rows:, rows:] = second
    product = small_dot(between, first, ((0,), (0,)))
    out[rows:, :rows] = -small_dot(second, product, ((1,), (0,)))


def eliminate(block, work, rows):
    row, col = triangle(rows)
    work[:, :rows] = block
    work[:, rows:] = (row == col).astype(jnp.float32)
    factor_block(work, rows)
    return jnp.where(row <= col, work[:, :rows], 0.0), work[:, rows:]


def first_factor(own_sum, other_sum, strips, cb, rows):
    blk_count = len(strips)
    half = cb // HALVES

    def body(own_ref, other_ref, *refs):
        strip_refs = refs[:blk_count]
        schur, lead, inverses, work = refs[blk_count:]
        me = lax.axis_index("blk")
        for x in range(blk_count):
            schur[jnp.bitwise_xor(me, x)] = strip_refs[x][...]
        others = unfold_sums(other_ref, cb, rows)
        for c in range(cb):
            part = slice(c * rows, (c + 1) * rows)
            schur[c, :, part] -= own_ref[part] + others[c]
        for block in range(half):
            here = block * rows
            upper, inverse = eliminate(schur[block, :, here:here + rows], work, rows)
            schur[block, :, here:here + rows] = upper
            inverses[block] = inverse
            after = here + rows
            strip = small_dot(inverse, schur[block, :, after:], ((1,), (0,)))
            schur[block, :, after:] = strip
            for other in range(block + 1, cb):
                offset = (other - block - 1) * rows
                schur[other, :, other * rows:] -= small_dot(
                    strip[:, offset:offset + rows], strip[:, offset:], ((0,), (0,))
                )
        write_inverse(lead, inverses[0], inverses[1], schur[0, :, rows:2 * rows], rows)

    return pl.pallas_call(
        body,
        name="factor_first",
        compiler_params=limit(12),
        out_shape=[
            pltpu.VMEM((cb, rows, cb * rows), jnp.float32),
            pltpu.VMEM((half * rows, half * rows), jnp.float32),
        ],
        in_specs=spaces(2 + blk_count, pltpu.VMEM),
        out_specs=spaces(2, pltpu.VMEM),
        scratch_shapes=[
            pltpu.VMEM((half, rows, rows), jnp.float32),
            pltpu.VMEM((rows, 2 * rows), jnp.float32),
        ],
        cost_estimate=pl.CostEstimate(flops=10000000000, bytes_accessed=2000000, transcendentals=0),
    )(*near_core(own_sum, other_sum, *strips))


def middle_factor(schur, cb, rows):
    def body(schur_ref, strip, corner, inverse_ref, work):
        block = cb // HALVES
        here = block * rows
        upper, inverse = eliminate(schur_ref[block, :, here:here + rows], work, rows)
        side = small_dot(inverse, schur_ref[block, :, here + rows:], ((1,), (0,)))
        strip[:, :rows] = upper
        strip[:, rows:] = side
        inverse_ref[...] = inverse
        corner[...] = schur_ref[cb - 1, :, here + rows:] - small_dot(side, side, ((0,), (0,)))

    return pl.pallas_call(
        body,
        name="factor_middle",
        compiler_params=limit(8),
        out_shape=[
            pltpu.VMEM((rows, 2 * rows), jnp.float32),
            pltpu.VMEM((rows, rows), jnp.float32),
            pltpu.VMEM((rows, rows), jnp.float32),
        ],
        in_specs=spaces(1, pltpu.VMEM),
        out_specs=spaces(3, pltpu.VMEM),
        scratch_shapes=[pltpu.VMEM((rows, 2 * rows), jnp.float32)],
        cost_estimate=pl.CostEstimate(flops=5000000000, bytes_accessed=1000000, transcendentals=0),
    )(*near_core(schur))


def last_factor(schur, strip, corner, inverse, cb, rows):
    half = cb // HALVES

    def body(schur_ref, strip_ref, corner_ref, inverse_ref, trail, lower, work):
        me = lax.axis_index("blk")
        upper, last = eliminate(corner_ref[...], work, rows)
        write_inverse(trail, inverse_ref[...], last, strip_ref[:, rows:], rows)
        mine = pl.ds(pl.multiple_of(me * rows, rows), rows)
        late = pl.ds(pl.multiple_of(jnp.maximum(me - half, 0) * rows, rows), rows)
        pieces = [schur_ref[k, :, mine] for k in range(half)] + [strip_ref[:, late], upper]
        for k in range(cb):
            lower[:, k * rows:(k + 1) * rows] = jnp.where(k <= me, pieces[k], 0.0).T

    return pl.pallas_call(
        body,
        name="factor_last",
        compiler_params=limit(8),
        out_shape=[
            pltpu.VMEM((half * rows, half * rows), jnp.float32),
            pltpu.VMEM((rows, cb * rows), jnp.float32),
        ],
        in_specs=spaces(4, pltpu.VMEM),
        out_specs=spaces(2, pltpu.VMEM),
        scratch_shapes=[pltpu.VMEM((rows, 2 * rows), jnp.float32)],
        cost_estimate=pl.CostEstimate(flops=5000000000, bytes_accessed=1000000, transcendentals=0),
    )(*near_core(schur, strip, corner, inverse))


def pack_sums(first, second):
    count, rows, width = first.shape
    pairs = count // 2

    def body(first_ref, second_ref, out):
        row = lax.broadcasted_iota(jnp.int32, (SCALE_ROWS, width), 0)
        scales = jnp.zeros((SCALE_ROWS, width), jnp.int32)
        lows = []
        for j in range(count):
            value = first_ref[j] + second_ref[j]
            peak = jnp.maximum(jnp.max(jnp.abs(value), axis=0, keepdims=True), 1e-30)
            power = jnp.floor(jnp.log(peak) * LOG2E + 1e-3) + 1.0
            scales = jnp.where(row == j, power.astype(jnp.int32), scales)
            whole = jnp.floor(value * jnp.exp2(BITS - power) + 0.5).astype(jnp.int32)
            high = lax.shift_right_arithmetic(whole, 8)
            lows.append(whole - high * 256)
            out[j * rows:(j + 1) * rows] = high.astype(jnp.int16)
        for j in range(pairs):
            low = lows[j] + lows[j + pairs] * 256 - 32768
            out[(count + j) * rows:(count + j + 1) * rows] = low.astype(jnp.int16)
        out[(count + pairs) * rows:] = scales.astype(jnp.int16)

    return pl.pallas_call(
        body,
        name="pack_sums",
        compiler_params=limit(8),
        out_shape=pltpu.VMEM(((count + pairs) * rows + SCALE_ROWS, width), jnp.int16),
        in_specs=spaces(2, pltpu.VMEM),
        out_specs=pl.BlockSpec(memory_space=pltpu.VMEM),
    )(*near_core(first, second))


def unpack_sums(ref, index, count, rows):
    pairs = count // 2
    high = ref[index * rows:(index + 1) * rows].astype(jnp.int32)
    at = (count + index % pairs) * rows
    low = ref[at:at + rows].astype(jnp.int32) + 32768
    upper = lax.shift_right_logical(low, 8)
    low = upper if index >= pairs else low - upper * 256
    scales = ref[(count + pairs) * rows:].astype(jnp.float32)
    scale = jnp.exp2(scales[index:index + 1] - BITS)
    return (high * 256 + low).astype(jnp.float32) * scale


def remaining(panel_ref, update_refs, half, cb, per, rows):
    parts = []
    for c in range(cb // HALVES):
        column = (half * (cb // HALVES) + c) * rows
        block = slice(c * per, (c + 1) * per)
        count = (cb // HALVES) * per
        coded = [unpack_sums(update_refs[2], index, count, rows)[None] for index in range(c * per, (c + 1) * per)]
        update = update_refs[0][block] + update_refs[1][block] + jnp.concatenate(coded, axis=0)
        original = panel_ref[1:, :, column:column + rows]
        parts.append((original - update).reshape(per * rows, rows))
    return jnp.concatenate(parts, axis=1)


def solve_left(panel, updates, lead, schur, lower, cb, per, rows):
    width = cb * rows
    half = width // HALVES

    def body(panel_ref, *refs):
        updates_ref = refs[:len(updates)]
        lead_ref, schur_ref, lower_ref, out, carried = refs[len(updates):]
        left = remaining(panel_ref, updates_ref, 0, cb, per, rows)
        out[0] = lower_ref[...]
        value = small_dot(left, lead_ref[...], ((1,), (1,)))
        out[1:, :, :half] = value.reshape(per, rows, half)
        across = schur_ref[:cb // HALVES, :, half:].reshape(half, half)
        carried[...] = small_dot(value, across, ((1,), (0,)))

    return pl.pallas_call(
        body,
        name="solve_left",
        compiler_params=limit(16),
        out_shape=[
            jax.ShapeDtypeStruct((per + 1, rows, width), jnp.float32),
            pltpu.VMEM((per * rows, half), jnp.float32),
        ],
        in_specs=spaces(4 + len(updates), pltpu.VMEM),
        out_specs=spaces(2, pltpu.VMEM),
        cost_estimate=pl.CostEstimate(flops=2000000000, bytes_accessed=5000000, transcendentals=0),
    )(panel, *near_core(*updates, lead, schur, lower))


def solve_right(panel, updates, trail, carried, out, cb, per, rows):
    width = cb * rows
    half = width // HALVES

    def body(panel_ref, *refs):
        updates_ref = refs[:len(updates)]
        trail_ref, carried_ref, _, result, stage, sem = refs[len(updates):]
        left = remaining(panel_ref, updates_ref, 1, cb, per, rows) - carried_ref[...]
        value = small_dot(left, trail_ref[...], ((1,), (1,)))
        stage[...] = value.reshape(per, rows, half)
        copy = pltpu.make_async_copy(
            stage, result.at[pl.ds(1, per), :, pl.ds(half, half)], sem
        )
        copy.start()
        copy.wait()

    return pl.pallas_call(
        body,
        name="solve_right",
        compiler_params=limit(16),
        out_shape=jax.ShapeDtypeStruct((per + 1, rows, width), jnp.float32),
        in_specs=spaces(3 + len(updates), pltpu.VMEM) + spaces(1, pl.ANY),
        out_specs=pl.BlockSpec(memory_space=pl.ANY),
        scratch_shapes=[pltpu.VMEM((per, rows, half), jnp.float32), pltpu.SemaphoreType.DMA(())],
        input_output_aliases={3 + len(updates): 0},
        cost_estimate=pl.CostEstimate(flops=2000000000, bytes_accessed=5000000, transcendentals=0),
    )(panel, *near_core(*updates, trail, carried), out)


def shards(desc_panel, row_map, anc_order, anc_below, anc_panel):
    leaves = lax.axis_size("leaf")
    blk_count = lax.axis_size("blk")
    rows = anc_panel.shape[3]
    width = anc_panel.shape[4]
    cb = width // rows
    per = anc_below.shape[1] // blk_count
    assert cb == blk_count == 4 and desc_panel.shape[2] == rows
    direct = leaves <= DIRECT and leaves & (leaves - 1) == 0
    near = [(i, i ^ 1) for i in range(blk_count)]
    far = [(i, i ^ 2) for i in range(blk_count)]

    panel = anc_panel.reshape(per + 1, rows, width)
    *packed, strip = pack(desc_panel, row_map, anc_order, panel, cb, direct)
    count = len(packed) // 2
    heads, tails = packed[:count], packed[count:]

    def exchange(arrays):
        if not direct:
            return [lax.all_to_all(arrays[0], "leaf", split_axis=0, concat_axis=0, tiled=True)]
        received = [arrays[0]]
        for k in range(1, leaves):
            swap = [(i, i ^ k) for i in range(leaves)]
            received.append(lax.ppermute(arrays[k], "leaf", swap))
        return received

    heads = exchange(heads)
    tails = exchange(tails)
    strip_far = lax.ppermute(strip, "blk", far)
    strip_near = lax.ppermute(strip, "blk", near)
    strip_both = lax.ppermute(strip_far, "blk", near)
    strips = [strip, strip_near, strip_far, strip_both]

    diagonal, codes = diagonal_update(heads, anc_below, cb, leaves, rows)
    diagonal_near = lax.ppermute(diagonal, "blk", near)
    diagonal, folded = fold_sums(diagonal, diagonal_near, cb, rows)
    folded = lax.ppermute(folded, "blk", far)
    schur, lead = first_factor(diagonal, folded, strips, cb, rows)

    every = [(x, half) for x in range(blk_count) for half in range(HALVES)]
    urgent = [(2, 0), (3, 0)]
    later = [part for part in every if part not in urgent]
    sizes = (cb, blk_count, per, leaves, rows)
    partials = below_update(heads, tails, codes, urgent, *sizes)
    partials.update(below_update(heads, tails, codes, later, *sizes))
    kept, for_near, for_far, for_both = (
        [partials[x, half] for half in range(HALVES)] for x in range(blk_count)
    )
    from_near = []
    from_far = []
    for half in range(HALVES):
        passed = lax.ppermute(for_both[half], "blk", near)
        from_far.append(lax.ppermute(pack_sums(for_far[half], passed), "blk", far))
    for half in range(HALVES):
        from_near.append(lax.ppermute(for_near[half], "blk", near))
    strip, corner, inverse = middle_factor(schur, cb, rows)
    trail, lower = last_factor(schur, strip, corner, inverse, cb, rows)
    updates = [[kept[half], from_near[half], from_far[half]] for half in range(HALVES)]
    out, carried = solve_left(panel, updates[0], lead, schur, lower, cb, per, rows)
    out = solve_right(panel, updates[1], trail, carried, out, cb, per, rows)
    return out.reshape(anc_panel.shape)


def solution(mesh):
    in_specs = (
        P(("leaf", "blk"), None, None),
        P(("leaf", "blk"), None),
        P(),
        P(),
        P("leaf", None, "blk", None, None),
    )
    out_specs = P("leaf", None, "blk", None, None)

    return jax.shard_map(shards, mesh=mesh, in_specs=in_specs, out_specs=out_specs, check_vma=False)
```

```python
import jax
import jax.numpy as jnp
from jax import lax
from jax.experimental import pallas as pl
from jax.experimental.pallas import tpu as pltpu
from jax.sharding import PartitionSpec as P


SLOTS = 2
CODES = 4
CODE_ROWS = 8
PANEL = 8
HALVES = 2
SCALE_ROWS = 16
BITS = 23.0
LOG2E = 1.4426950408889634
DIRECT = 8
HIGHEST = lax.Precision.HIGHEST


def repeat(count, body, unroll_to=16):
    if count <= unroll_to:
        for index in range(count):
            body(index)
    else:
        lax.fori_loop(0, count, lambda index, carry: (body(index), carry)[1], 0)


def limit(mib):
    return pltpu.CompilerParams(vmem_limit_bytes=mib * 1024 * 1024)


def near_core(*arrays):
    return [pltpu.with_memory_space_constraint(array, pltpu.VMEM) for array in arrays]


def spaces(count, space):
    return [pl.BlockSpec(memory_space=space)] * count


def pack_kernel(cb, direct, map_hbm, order_hbm, panel_hbm, anc_hbm, *refs):
    leaves = order_hbm.shape[0]
    block_count, desc_count = map_hbm.shape
    rows = panel_hbm.shape[1] // block_count
    tail_rows = (block_count - 1) * rows
    count = leaves if direct else 1
    heads, tails = refs[:count], refs[count:2 * count]
    strip, inverse, used, chosen, codes, row_map, anc_order, panel, sems = refs[2 * count:]
    me = lax.axis_index("leaf")
    copies = [
        pltpu.make_async_copy(source, target, sems.at[at])
        for at, (source, target) in enumerate((
            (map_hbm, row_map), (order_hbm, anc_order),
            (panel_hbm, panel), (anc_hbm.at[0], strip),
        ))
    ]
    for copy in copies:
        copy.start()
    copies[0].wait()
    copies[1].wait()

    def clear(leaf):
        inverse[anc_order[leaf]] = leaf
        used[leaf] = 0
        for slot in range(SLOTS):
            chosen[leaf * SLOTS + slot] = 0
            codes[(leaf * SLOTS + slot) * CODES] = cb
            for r in range(1, CODES):
                codes[(leaf * SLOTS + slot) * CODES + r] = 0

    repeat(leaves, clear)

    def assign(desc):
        head = row_map[0, desc]
        leaf = inverse[lax.div(head, cb)]
        taken = used[leaf]
        used[leaf] = taken + 1
        place = leaf * SLOTS + taken
        chosen[place] = desc
        codes[place * CODES] = head - anc_order[leaf] * cb
        for r in range(1, block_count):
            codes[place * CODES + r] = row_map[r, desc] - leaves * cb

    repeat(desc_count, assign)
    copies[2].wait()

    def write(index):
        leaf = jnp.bitwise_xor(me, index) if direct else index
        head = heads[index] if direct else heads[0].at[index]
        tail = tails[index] if direct else tails[0].at[index]
        row = lax.broadcasted_iota(jnp.int32, (CODE_ROWS, 128), 0)
        values = jnp.zeros((CODE_ROWS, 128), jnp.int32)
        for entry in range(SLOTS * CODES):
            values = jnp.where(row == entry, codes[leaf * SLOTS * CODES + entry], values)
        head[pl.ds(SLOTS * rows, CODE_ROWS)] = values.astype(jnp.float32).astype(panel.dtype)
        for slot in range(SLOTS):
            desc = chosen[leaf * SLOTS + slot]
            head[pl.ds(slot * rows, rows)] = panel[desc, pl.ds(0, rows)]
            tail[pl.ds(slot * tail_rows, tail_rows)] = panel[desc, pl.ds(rows, tail_rows)]

    repeat(leaves, write)
    copies[3].wait()


def pack(desc_panel, row_map, anc_order, anc, cb, direct):
    leaves = anc_order.shape[0]
    block_count = row_map.shape[1]
    rows = desc_panel.shape[1] // block_count
    width = desc_panel.shape[2]
    head = (SLOTS * rows + CODE_ROWS, width)
    tail = (SLOTS * (block_count - 1) * rows, width)
    dtype = desc_panel.dtype
    if direct:
        outs = [pltpu.VMEM(head, dtype)] * leaves + [pltpu.VMEM(tail, dtype)] * leaves
    else:
        outs = [jax.ShapeDtypeStruct((leaves,) + shape, dtype) for shape in (head, tail)]
    outs.append(pltpu.VMEM(anc.shape[1:], anc.dtype))

    def body(*refs):
        pack_kernel(cb, direct, *refs)

    return pl.pallas_call(
        body,
        name="pack",
        compiler_params=limit(12 if direct else 40),
        out_shape=outs,
        in_specs=spaces(4, pl.ANY),
        out_specs=spaces(len(outs), pltpu.VMEM),
        scratch_shapes=[
            pltpu.SMEM((leaves,), jnp.int32),
            pltpu.SMEM((leaves,), jnp.int32),
            pltpu.SMEM((leaves * SLOTS,), jnp.int32),
            pltpu.SMEM((leaves * SLOTS * CODES,), jnp.int32),
            pltpu.SMEM(row_map.T.shape, jnp.int32),
            pltpu.SMEM(anc_order.shape, jnp.int32),
            pltpu.VMEM(desc_panel.shape, dtype),
            pltpu.SemaphoreType.DMA((4,)),
        ],
    )(
        *(
            pltpu.with_memory_space_constraint(array, pltpu.HBM)
            for array in (row_map.T, anc_order, desc_panel, anc)
        )
    )


def diagonal_kernel(cb, leaves, anc_below, *refs):
    heads = refs[:-6]
    out, codes_out, left, right, codes, code_sem = refs[-6:]
    direct = len(heads) > 1
    rows = out.shape[1]
    group = min(leaves, 8)

    def load(index, start, size):
        if direct:
            return heads[index][pl.ds(start, size)]
        return heads[0][index, pl.ds(start, size)]

    lane = lax.broadcasted_iota(jnp.int32, (1, rows), 1)

    def step(base):
        for offset in range(group):
            marks = load(base + offset, SLOTS * rows, CODE_ROWS).astype(jnp.float32)
            packed = jnp.zeros((1, rows), jnp.float32)
            for entry in range(SLOTS * CODES):
                packed = jnp.where(lane == entry, marks[entry:entry + 1], packed)
            codes[pl.ds(base + offset, 1)] = packed.astype(jnp.int32)
            for slot in range(SLOTS):
                block = load(base + offset, slot * rows, rows)
                lanes = pl.ds((offset * SLOTS + slot) * rows, rows)
                code = jnp.broadcast_to(marks[slot * CODES:slot * CODES + 1], (rows, rows))
                code = code.astype(block.dtype)
                zero = jnp.zeros_like(block)
                right[:, lanes] = jnp.where(code < cb, block, zero)
                for c in range(cb):
                    left[c * rows:(c + 1) * rows, lanes] = jnp.where(code == c, block, zero)
        return lax.dot_general(
            left[...], right[...], (((1,), (1,)), ((), ())), preferred_element_type=jnp.float32
        )

    def locate(first, size):
        ids = codes[pl.ds(first, size)] + leaves * cb
        found = jnp.zeros_like(ids)
        me = lax.axis_index("leaf")
        for q in range(anc_below.shape[1]):
            found = jnp.where(ids == anc_below[me, q], q, found)
        codes[pl.ds(first, size)] = jnp.where(
            lax.rem(lane, CODES) == 0, codes[pl.ds(first, size)], found
        )

    code_copy = pltpu.make_async_copy(codes, codes_out, code_sem)
    if leaves == group:
        product = step(0)
        locate(0, group)
        code_copy.start()
        out[...] = product.reshape(out.shape)
        code_copy.wait()
    else:
        out[...] = jnp.zeros_like(out)

        def accumulate(index, carry):
            first = pl.multiple_of(index * group, group)
            out[...] += step(first).reshape(out.shape)
            locate(first, group)
            return carry

        lax.fori_loop(0, leaves // group, accumulate, 0)
        code_copy.start()
        code_copy.wait()


def diagonal_update(heads, anc_below, cb, leaves, rows):
    group = min(leaves, 8)

    def body(*refs):
        diagonal_kernel(cb, leaves, *refs)

    return pl.pallas_call(
        body,
        name="diagonal",
        compiler_params=limit(12 if len(heads) > 1 else 40),
        out_shape=[
            pltpu.VMEM((cb * rows, rows), jnp.float32),
            pltpu.SMEM((leaves, rows), jnp.int32),
        ],
        in_specs=spaces(1, pltpu.SMEM) + spaces(len(heads), pltpu.VMEM),
        out_specs=spaces(1, pltpu.VMEM) + spaces(1, pltpu.SMEM),
        scratch_shapes=[
            pltpu.VMEM((cb * rows, group * SLOTS * rows), heads[0].dtype),
            pltpu.VMEM((rows, group * SLOTS * rows), heads[0].dtype),
            pltpu.VMEM((leaves, rows), jnp.int32),
            pltpu.SemaphoreType.DMA(()),
        ],
        cost_estimate=pl.CostEstimate(flops=2000000000, bytes_accessed=1000000, transcendentals=0),
    )(anc_below, *(near_core(*heads) if len(heads) > 1 else heads))


def below_kernel(cb, blk_count, per, leaves, count, parts, codes, *refs):
    tails, refs = refs[:count], refs[count:]
    heads = refs[:count]
    outs = refs[count:count + len(parts)]
    acc, products = refs[count + len(parts):]
    direct = count > 1
    me_blk = lax.axis_index("blk")
    rows = acc.shape[1]
    group = min(leaves, 8)
    tail_rows = tails[0].shape[-2] // SLOTS
    extra = tail_rows // rows
    size = cb * per // HALVES
    trash = len(parts) * size
    for first in range(0, trash, size):
        acc[pl.ds(first, size)] = jnp.zeros((size, rows, rows), jnp.float32)

    def step(base):
        for offset in range(group):
            index = base + offset
            for slot in range(SLOTS):
                if direct:
                    head = heads[index][pl.ds(slot * rows, rows)]
                    tail = tails[index][pl.ds(slot * tail_rows, tail_rows)]
                else:
                    head = heads[0][index, pl.ds(slot * rows, rows)]
                    tail = tails[0][index, pl.ds(slot * tail_rows, tail_rows)]
                products[offset * SLOTS + slot] = lax.dot_general(
                    tail, head, (((1,), (1,)), ((), ())), preferred_element_type=jnp.float32
                )
        for offset in range(group):
            for slot in range(SLOTS):
                column = codes[base + offset, slot * CODES]
                for r in range(extra):
                    position = codes[base + offset, slot * CODES + 1 + r]
                    relative = jnp.bitwise_xor(lax.rem(position, blk_count), me_blk)
                    part = relative * HALVES + lax.div(column * HALVES, cb)
                    start = jnp.int32(-1)
                    for at, (x, half) in enumerate(parts):
                        start = jnp.where(part == x * HALVES + half, at * size, start)
                    inside = lax.rem(column, cb // HALVES) * per + lax.div(position, blk_count)
                    place = jnp.where((column < cb) & (start >= 0), start + inside, trash)
                    acc[place] += products[offset * SLOTS + slot, pl.ds(r * rows, rows)]

    if leaves == group:
        step(0)
    else:
        lax.fori_loop(0, leaves // group, lambda index, carry: (step(index * group), carry)[1], 0)
    for at, out in enumerate(outs):
        out[...] = acc[pl.ds(at * size, size)]


def below_update(heads, tails, codes, parts, cb, blk_count, per, leaves, rows):
    group = min(leaves, 8)
    size = cb * per // HALVES

    def body(*refs):
        below_kernel(cb, blk_count, per, leaves, len(heads), parts, *refs)

    results = pl.pallas_call(
        body,
        compiler_params=limit(16 if len(heads) > 1 else 56),
        out_shape=[pltpu.VMEM((size, rows, rows), jnp.float32)] * len(parts),
        in_specs=spaces(1, pltpu.SMEM) + spaces(2 * len(heads), pltpu.VMEM),
        out_specs=spaces(len(parts), pltpu.VMEM),
        scratch_shapes=[
            pltpu.VMEM((len(parts) * size + 1, rows, rows), jnp.float32),
            pltpu.VMEM((group * SLOTS, tails[0].shape[-2] // SLOTS, rows), jnp.float32),
        ],
        cost_estimate=pl.CostEstimate(flops=2000000000, bytes_accessed=4000000, transcendentals=0),
    )(pltpu.with_memory_space_constraint(codes, pltpu.SMEM), *(near_core(*tails, *heads) if len(heads) > 1 else [*tails, *heads]))
    return dict(zip(parts, results))


def factor_block(work, rows):
    lane = lax.broadcasted_iota(jnp.int32, (1, rows), 1)
    sub = lax.broadcasted_iota(jnp.int32, (PANEL, 1), 0)
    segments = 4
    size = rows // segments

    for segment in range(segments):
        top = segment * size

        def panel(index, carry):
            base = pl.multiple_of(top + index * PANEL, PANEL)
            strip = work[pl.ds(base, PANEL), :]
            raw = work[top:, :rows]
            picks = [(lane == base + k) for k in range(PANEL)]
            corner = [
                jnp.sum(jnp.where(picks[k], strip[:, :rows], 0.0), axis=1, keepdims=True)
                for k in range(PANEL)
            ]
            factor = jnp.zeros((PANEL, 2 * rows), jnp.float32)
            for k in range(PANEL):
                scale = lax.rsqrt(corner[k][k:k + 1])
                inverse = scale * scale
                row = strip[k:k + 1]
                factor = jnp.where(sub == k, row * scale, factor)
                scaled = row * inverse
                strip = jnp.where(sub == k, scaled, strip - corner[k] * scaled)
                for m in range(k + 1, PANEL):
                    entry = corner[m][k:k + 1]
                    corner[m] = jnp.where(
                        sub == k, entry * inverse, corner[m] - (corner[k] * entry) * inverse
                    )
            work[pl.ds(base, PANEL), :] = factor
            for start, stop, masked in ((top, top + size, True), (top + size, rows, False)):
                if start == stop:
                    continue
                full = work[start:stop, :]
                row_id = lax.broadcasted_iota(jnp.int32, (stop - start, 1), 0) + start
                for k in range(PANEL):
                    column = jnp.sum(
                        jnp.where(picks[k], raw[start - top:stop - top], 0.0), axis=1, keepdims=True
                    )
                    if masked:
                        column = jnp.where(row_id >= base + PANEL, column, 0.0)
                    full = full - column * strip[k:k + 1]
                work[start:stop, :] = full
            return carry

        lax.fori_loop(0, size // PANEL, panel, 0)


def triangle(rows):
    row = lax.broadcasted_iota(jnp.int32, (rows, rows), 0)
    return row, lax.broadcasted_iota(jnp.int32, (rows, rows), 1)


def fold_sums(first, second, cb, rows):
    def body(first_ref, second_ref, total, folded):
        row, col = triangle(rows)
        line = lax.broadcasted_iota(jnp.int32, (PANEL, rows), 0)
        marks = jnp.zeros((PANEL, rows), jnp.float32)
        total[...] = first_ref[...] + second_ref[...]
        for pair in range(cb // 2):
            lower = total[2 * pair * rows:(2 * pair + 1) * rows]
            upper = total[(2 * pair + 1) * rows:(2 * pair + 2) * rows]
            folded[pair * rows:(pair + 1) * rows] = jnp.where(row >= col, lower, upper)
            edge = jnp.sum(jnp.where(row == col, upper, 0.0), axis=0, keepdims=True)
            marks = jnp.where(line == pair, edge, marks)
        folded[cb // 2 * rows:] = marks

    return pl.pallas_call(
        body,
        name="fold_sums",
        compiler_params=limit(8),
        out_shape=[
            pltpu.VMEM((cb * rows, rows), jnp.float32),
            pltpu.VMEM((cb // 2 * rows + PANEL, rows), jnp.float32),
        ],
        in_specs=spaces(2, pltpu.VMEM),
        out_specs=spaces(2, pltpu.VMEM),
    )(*near_core(first, second))


def unfold_sums(folded, cb, rows):
    row, col = triangle(rows)
    blocks = []
    for pair in range(cb // 2):
        square = folded[pair * rows:(pair + 1) * rows]
        edge = folded[cb // 2 * rows + pair:cb // 2 * rows + pair + 1]
        lower = jnp.where(row > col, square, 0.0)
        upper = jnp.where(row < col, square, 0.0)
        blocks.append(lower + lower.T + jnp.where(row == col, square, 0.0))
        blocks.append(upper + upper.T + jnp.where(row == col, edge, 0.0))
    return blocks


def small_dot(left, right, dims):
    return lax.dot_general(
        left, right, (dims, ((), ())), precision=HIGHEST, preferred_element_type=jnp.float32
    )


def write_inverse(out, first, second, between, rows):
    out[:rows, :rows] = first
    out[:rows, rows:] = jnp.zeros_like(first)
    out[rows:, rows:] = second
    product = small_dot(between, first, ((0,), (0,)))
    out[rows:, :rows] = -small_dot(second, product, ((1,), (0,)))


def eliminate(block, work, rows):
    row, col = triangle(rows)
    work[:, :rows] = block
    work[:, rows:] = (row == col).astype(jnp.float32)
    factor_block(work, rows)
    return jnp.where(row <= col, work[:, :rows], 0.0), work[:, rows:]


def first_factor(own_sum, other_sum, strips, cb, rows):
    blk_count = len(strips)
    half = cb // HALVES

    def body(own_ref, other_ref, *refs):
        strip_refs = refs[:blk_count]
        schur, lead, inverses, work = refs[blk_count:]
        me = lax.axis_index("blk")
        for x in range(blk_count):
            schur[jnp.bitwise_xor(me, x)] = strip_refs[x][...]
        others = unfold_sums(other_ref, cb, rows)
        for c in range(cb):
            part = slice(c * rows, (c + 1) * rows)
            schur[c, :, part] -= own_ref[part] + others[c]
        for block in range(half):
            here = block * rows
            upper, inverse = eliminate(schur[block, :, here:here + rows], work, rows)
            schur[block, :, here:here + rows] = upper
            inverses[block] = inverse
            after = here + rows
            strip = small_dot(inverse, schur[block, :, after:], ((1,), (0,)))
            schur[block, :, after:] = strip
            for other in range(block + 1, cb):
                offset = (other - block - 1) * rows
                schur[other, :, other * rows:] -= small_dot(
                    strip[:, offset:offset + rows], strip[:, offset:], ((0,), (0,))
                )
        write_inverse(lead, inverses[0], inverses[1], schur[0, :, rows:2 * rows], rows)

    return pl.pallas_call(
        body,
        name="factor_first",
        compiler_params=limit(12),
        out_shape=[
            pltpu.VMEM((cb, rows, cb * rows), jnp.float32),
            pltpu.VMEM((half * rows, half * rows), jnp.float32),
        ],
        in_specs=spaces(2 + blk_count, pltpu.VMEM),
        out_specs=spaces(2, pltpu.VMEM),
        scratch_shapes=[
            pltpu.VMEM((half, rows, rows), jnp.float32),
            pltpu.VMEM((rows, 2 * rows), jnp.float32),
        ],
        cost_estimate=pl.CostEstimate(flops=10000000000, bytes_accessed=2000000, transcendentals=0),
    )(*near_core(own_sum, other_sum, *strips))


def middle_factor(schur, cb, rows):
    def body(schur_ref, strip, corner, inverse_ref, work):
        block = cb // HALVES
        here = block * rows
        upper, inverse = eliminate(schur_ref[block, :, here:here + rows], work, rows)
        side = small_dot(inverse, schur_ref[block, :, here + rows:], ((1,), (0,)))
        strip[:, :rows] = upper
        strip[:, rows:] = side
        inverse_ref[...] = inverse
        corner[...] = schur_ref[cb - 1, :, here + rows:] - small_dot(side, side, ((0,), (0,)))

    return pl.pallas_call(
        body,
        name="factor_middle",
        compiler_params=limit(8),
        out_shape=[
            pltpu.VMEM((rows, 2 * rows), jnp.float32),
            pltpu.VMEM((rows, rows), jnp.float32),
            pltpu.VMEM((rows, rows), jnp.float32),
        ],
        in_specs=spaces(1, pltpu.VMEM),
        out_specs=spaces(3, pltpu.VMEM),
        scratch_shapes=[pltpu.VMEM((rows, 2 * rows), jnp.float32)],
        cost_estimate=pl.CostEstimate(flops=5000000000, bytes_accessed=1000000, transcendentals=0),
    )(*near_core(schur))


def last_factor(schur, strip, corner, inverse, cb, rows):
    half = cb // HALVES

    def body(schur_ref, strip_ref, corner_ref, inverse_ref, trail, lower, work):
        me = lax.axis_index("blk")
        upper, last = eliminate(corner_ref[...], work, rows)
        write_inverse(trail, inverse_ref[...], last, strip_ref[:, rows:], rows)
        mine = pl.ds(pl.multiple_of(me * rows, rows), rows)
        late = pl.ds(pl.multiple_of(jnp.maximum(me - half, 0) * rows, rows), rows)
        pieces = [schur_ref[k, :, mine] for k in range(half)] + [strip_ref[:, late], upper]
        for k in range(cb):
            lower[:, k * rows:(k + 1) * rows] = jnp.where(k <= me, pieces[k], 0.0).T

    return pl.pallas_call(
        body,
        name="factor_last",
        compiler_params=limit(8),
        out_shape=[
            pltpu.VMEM((half * rows, half * rows), jnp.float32),
            pltpu.VMEM((rows, cb * rows), jnp.float32),
        ],
        in_specs=spaces(4, pltpu.VMEM),
        out_specs=spaces(2, pltpu.VMEM),
        scratch_shapes=[pltpu.VMEM((rows, 2 * rows), jnp.float32)],
        cost_estimate=pl.CostEstimate(flops=5000000000, bytes_accessed=1000000, transcendentals=0),
    )(*near_core(schur, strip, corner, inverse))


def pack_sums(first, second):
    count, rows, width = first.shape
    pairs = count // 2

    def body(first_ref, second_ref, out):
        row = lax.broadcasted_iota(jnp.int32, (SCALE_ROWS, width), 0)
        scales = jnp.zeros((SCALE_ROWS, width), jnp.int32)
        lows = []
        for j in range(count):
            value = first_ref[j] + second_ref[j]
            peak = jnp.maximum(jnp.max(jnp.abs(value), axis=0, keepdims=True), 1e-30)
            power = jnp.floor(jnp.log(peak) * LOG2E + 1e-3) + 1.0
            scales = jnp.where(row == j, power.astype(jnp.int32), scales)
            whole = jnp.floor(value * jnp.exp2(BITS - power) + 0.5).astype(jnp.int32)
            high = lax.shift_right_arithmetic(whole, 8)
            lows.append(whole - high * 256)
            out[j * rows:(j + 1) * rows] = high.astype(jnp.int16)
        for j in range(pairs):
            low = lows[j] + lows[j + pairs] * 256 - 32768
            out[(count + j) * rows:(count + j + 1) * rows] = low.astype(jnp.int16)
        out[(count + pairs) * rows:] = scales.astype(jnp.int16)

    return pl.pallas_call(
        body,
        name="pack_sums",
        compiler_params=limit(8),
        out_shape=pltpu.VMEM(((count + pairs) * rows + SCALE_ROWS, width), jnp.int16),
        in_specs=spaces(2, pltpu.VMEM),
        out_specs=pl.BlockSpec(memory_space=pltpu.VMEM),
    )(*near_core(first, second))


def unpack_sums(ref, index, count, rows):
    pairs = count // 2
    high = ref[index * rows:(index + 1) * rows].astype(jnp.int32)
    at = (count + index % pairs) * rows
    low = ref[at:at + rows].astype(jnp.int32) + 32768
    upper = lax.shift_right_logical(low, 8)
    low = upper if index >= pairs else low - upper * 256
    scales = ref[(count + pairs) * rows:].astype(jnp.float32)
    scale = jnp.exp2(scales[index:index + 1] - BITS)
    return (high * 256 + low).astype(jnp.float32) * scale


def remaining(panel_ref, update_refs, half, cb, per, rows):
    parts = []
    for c in range(cb // HALVES):
        column = (half * (cb // HALVES) + c) * rows
        block = slice(c * per, (c + 1) * per)
        count = (cb // HALVES) * per
        coded = [unpack_sums(update_refs[2], index, count, rows)[None] for index in range(c * per, (c + 1) * per)]
        update = update_refs[0][block] + update_refs[1][block] + jnp.concatenate(coded, axis=0)
        original = panel_ref[1:, :, column:column + rows]
        parts.append((original - update).reshape(per * rows, rows))
    return jnp.concatenate(parts, axis=1)


def solve_left(panel, updates, lead, schur, lower, cb, per, rows):
    width = cb * rows
    half = width // HALVES

    def body(panel_ref, *refs):
        updates_ref = refs[:len(updates)]
        lead_ref, schur_ref, lower_ref, out, carried = refs[len(updates):]
        left = remaining(panel_ref, updates_ref, 0, cb, per, rows)
        out[0] = lower_ref[...]
        value = small_dot(left, lead_ref[...], ((1,), (1,)))
        out[1:, :, :half] = value.reshape(per, rows, half)
        across = schur_ref[:cb // HALVES, :, half:].reshape(half, half)
        carried[...] = small_dot(value, across, ((1,), (0,)))

    return pl.pallas_call(
        body,
        name="solve_left",
        compiler_params=limit(16),
        out_shape=[
            jax.ShapeDtypeStruct((per + 1, rows, width), jnp.float32),
            pltpu.VMEM((per * rows, half), jnp.float32),
        ],
        in_specs=spaces(4 + len(updates), pltpu.VMEM),
        out_specs=spaces(2, pltpu.VMEM),
        cost_estimate=pl.CostEstimate(flops=2000000000, bytes_accessed=5000000, transcendentals=0),
    )(panel, *near_core(*updates, lead, schur, lower))


def solve_right(panel, updates, trail, carried, out, cb, per, rows):
    width = cb * rows
    half = width // HALVES

    def body(panel_ref, *refs):
        updates_ref = refs[:len(updates)]
        trail_ref, carried_ref, _, result, stage, sem = refs[len(updates):]
        left = remaining(panel_ref, updates_ref, 1, cb, per, rows) - carried_ref[...]
        value = small_dot(left, trail_ref[...], ((1,), (1,)))
        stage[...] = value.reshape(per, rows, half)
        copy = pltpu.make_async_copy(
            stage, result.at[pl.ds(1, per), :, pl.ds(half, half)], sem
        )
        copy.start()
        copy.wait()

    return pl.pallas_call(
        body,
        name="solve_right",
        compiler_params=limit(16),
        out_shape=jax.ShapeDtypeStruct((per + 1, rows, width), jnp.float32),
        in_specs=spaces(3 + len(updates), pltpu.VMEM) + spaces(1, pl.ANY),
        out_specs=pl.BlockSpec(memory_space=pl.ANY),
        scratch_shapes=[pltpu.VMEM((per, rows, half), jnp.float32), pltpu.SemaphoreType.DMA(())],
        input_output_aliases={3 + len(updates): 0},
        cost_estimate=pl.CostEstimate(flops=2000000000, bytes_accessed=5000000, transcendentals=0),
    )(panel, *near_core(*updates, trail, carried), out)


def shards(desc_panel, row_map, anc_order, anc_below, anc_panel):
    leaves = lax.axis_size("leaf")
    blk_count = lax.axis_size("blk")
    rows = anc_panel.shape[3]
    width = anc_panel.shape[4]
    cb = width // rows
    per = anc_below.shape[1] // blk_count
    assert cb == blk_count == 4 and desc_panel.shape[2] == rows
    direct = leaves <= DIRECT and leaves & (leaves - 1) == 0
    near = [(i, i ^ 1) for i in range(blk_count)]
    far = [(i, i ^ 2) for i in range(blk_count)]

    panel = anc_panel.reshape(per + 1, rows, width)
    *packed, strip = pack(desc_panel, row_map, anc_order, panel, cb, direct)
    count = len(packed) // 2
    heads, tails = packed[:count], packed[count:]

    def exchange(arrays):
        if not direct:
            return [lax.all_to_all(arrays[0], "leaf", split_axis=0, concat_axis=0, tiled=True)]
        received = [arrays[0]]
        for k in range(1, leaves):
            swap = [(i, i ^ k) for i in range(leaves)]
            received.append(lax.ppermute(arrays[k], "leaf", swap))
        return received

    heads = exchange(heads)
    tails = exchange(tails)
    strip_far = lax.ppermute(strip, "blk", far)
    strip_near = lax.ppermute(strip, "blk", near)
    strip_both = lax.ppermute(strip_far, "blk", near)
    strips = [strip, strip_near, strip_far, strip_both]

    diagonal, codes = diagonal_update(heads, anc_below, cb, leaves, rows)
    diagonal_near = lax.ppermute(diagonal, "blk", near)
    diagonal, folded = fold_sums(diagonal, diagonal_near, cb, rows)
    folded = lax.ppermute(folded, "blk", far)
    schur, lead = first_factor(diagonal, folded, strips, cb, rows)

    every = [(x, half) for x in range(blk_count) for half in range(HALVES)]
    urgent = [(2, 0), (3, 0)]
    later = [part for part in every if part not in urgent]
    sizes = (cb, blk_count, per, leaves, rows)
    partials = below_update(heads, tails, codes, urgent, *sizes)
    partials.update(below_update(heads, tails, codes, later, *sizes))
    kept, for_near, for_far, for_both = (
        [partials[x, half] for half in range(HALVES)] for x in range(blk_count)
    )
    from_near = []
    from_far = []
    for half in range(HALVES):
        passed = lax.ppermute(for_both[half], "blk", near)
        from_far.append(lax.ppermute(pack_sums(for_far[half], passed), "blk", far))
    for half in range(HALVES):
        from_near.append(lax.ppermute(for_near[half], "blk", near))
    strip, corner, inverse = middle_factor(schur, cb, rows)
    trail, lower = last_factor(schur, strip, corner, inverse, cb, rows)
    updates = [[kept[half], from_near[half], from_far[half]] for half in range(HALVES)]
    out, carried = solve_left(panel, updates[0], lead, schur, lower, cb, per, rows)
    out = solve_right(panel, updates[1], trail, carried, out, cb, per, rows)
    return out.reshape(anc_panel.shape)


def solution(mesh):
    in_specs = (
        P(("leaf", "blk"), None, None),
        P(("leaf", "blk"), None),
        P(),
        P(),
        P("leaf", None, "blk", None, None),
    )
    out_specs = P("leaf", None, "blk", None, None)

    return jax.shard_map(shards, mesh=mesh, in_specs=in_specs, out_specs=out_specs, check_vma=False)
```

```python
import jax
import jax.numpy as jnp
from jax import lax
from jax.experimental import pallas as pl
from jax.experimental.pallas import tpu as pltpu
from jax.sharding import PartitionSpec as P


SLOTS = 2
CODES = 4
CODE_ROWS = 8
PANEL = 8
HALVES = 2
SCALE_ROWS = 16
BITS = 20.0
LOW_BITS = 5
LOWS = 3
LOG2E = 1.4426950408889634
DIRECT = 8
HIGHEST = lax.Precision.HIGHEST


def repeat(count, body, unroll_to=16):
    if count <= unroll_to:
        for index in range(count):
            body(index)
    else:
        lax.fori_loop(0, count, lambda index, carry: (body(index), carry)[1], 0)


def limit(mib):
    return pltpu.CompilerParams(vmem_limit_bytes=mib * 1024 * 1024)


def near_core(*arrays):
    return [pltpu.with_memory_space_constraint(array, pltpu.VMEM) for array in arrays]


def spaces(count, space):
    return [pl.BlockSpec(memory_space=space)] * count


def pack_kernel(cb, direct, map_hbm, order_hbm, panel_hbm, anc_hbm, *refs):
    leaves = order_hbm.shape[0]
    block_count, desc_count = map_hbm.shape
    rows = panel_hbm.shape[1] // block_count
    tail_rows = (block_count - 1) * rows
    count = leaves if direct else 1
    heads, tails = refs[:count], refs[count:2 * count]
    strip, inverse, used, chosen, codes, row_map, anc_order, panel, sems = refs[2 * count:]
    me = lax.axis_index("leaf")
    copies = [
        pltpu.make_async_copy(source, target, sems.at[at])
        for at, (source, target) in enumerate((
            (map_hbm, row_map), (order_hbm, anc_order),
            (panel_hbm, panel), (anc_hbm.at[0], strip),
        ))
    ]
    for copy in copies:
        copy.start()
    copies[0].wait()
    copies[1].wait()

    def clear(leaf):
        inverse[anc_order[leaf]] = leaf
        used[leaf] = 0
        for slot in range(SLOTS):
            chosen[leaf * SLOTS + slot] = 0
            codes[(leaf * SLOTS + slot) * CODES] = cb
            for r in range(1, CODES):
                codes[(leaf * SLOTS + slot) * CODES + r] = 0

    repeat(leaves, clear)

    def assign(desc):
        head = row_map[0, desc]
        leaf = inverse[lax.div(head, cb)]
        taken = used[leaf]
        used[leaf] = taken + 1
        place = leaf * SLOTS + taken
        chosen[place] = desc
        codes[place * CODES] = head - anc_order[leaf] * cb
        for r in range(1, block_count):
            codes[place * CODES + r] = row_map[r, desc] - leaves * cb

    repeat(desc_count, assign)
    copies[2].wait()

    def write(index):
        leaf = jnp.bitwise_xor(me, index) if direct else index
        head = heads[index] if direct else heads[0].at[index]
        tail = tails[index] if direct else tails[0].at[index]
        row = lax.broadcasted_iota(jnp.int32, (CODE_ROWS, 128), 0)
        values = jnp.zeros((CODE_ROWS, 128), jnp.int32)
        for entry in range(SLOTS * CODES):
            values = jnp.where(row == entry, codes[leaf * SLOTS * CODES + entry], values)
        head[pl.ds(SLOTS * rows, CODE_ROWS)] = values.astype(jnp.float32).astype(panel.dtype)
        for slot in range(SLOTS):
            desc = chosen[leaf * SLOTS + slot]
            head[pl.ds(slot * rows, rows)] = panel[desc, pl.ds(0, rows)]
            tail[pl.ds(slot * tail_rows, tail_rows)] = panel[desc, pl.ds(rows, tail_rows)]

    repeat(leaves, write)
    copies[3].wait()


def pack(desc_panel, row_map, anc_order, anc, cb, direct):
    leaves = anc_order.shape[0]
    block_count = row_map.shape[1]
    rows = desc_panel.shape[1] // block_count
    width = desc_panel.shape[2]
    head = (SLOTS * rows + CODE_ROWS, width)
    tail = (SLOTS * (block_count - 1) * rows, width)
    dtype = desc_panel.dtype
    if direct:
        outs = [pltpu.VMEM(head, dtype)] * leaves + [pltpu.VMEM(tail, dtype)] * leaves
    else:
        outs = [jax.ShapeDtypeStruct((leaves,) + shape, dtype) for shape in (head, tail)]
    outs.append(pltpu.VMEM(anc.shape[1:], anc.dtype))

    def body(*refs):
        pack_kernel(cb, direct, *refs)

    return pl.pallas_call(
        body,
        name="pack",
        compiler_params=limit(12 if direct else 40),
        out_shape=outs,
        in_specs=spaces(4, pl.ANY),
        out_specs=spaces(len(outs), pltpu.VMEM),
        scratch_shapes=[
            pltpu.SMEM((leaves,), jnp.int32),
            pltpu.SMEM((leaves,), jnp.int32),
            pltpu.SMEM((leaves * SLOTS,), jnp.int32),
            pltpu.SMEM((leaves * SLOTS * CODES,), jnp.int32),
            pltpu.SMEM(row_map.T.shape, jnp.int32),
            pltpu.SMEM(anc_order.shape, jnp.int32),
            pltpu.VMEM(desc_panel.shape, dtype),
            pltpu.SemaphoreType.DMA((4,)),
        ],
    )(
        *(
            pltpu.with_memory_space_constraint(array, pltpu.HBM)
            for array in (row_map.T, anc_order, desc_panel, anc)
        )
    )


def diagonal_kernel(cb, leaves, anc_below, *refs):
    heads = refs[:-6]
    out, codes_out, left, right, codes, code_sem = refs[-6:]
    direct = len(heads) > 1
    rows = out.shape[1]
    group = min(leaves, 8)

    def load(index, start, size):
        if direct:
            return heads[index][pl.ds(start, size)]
        return heads[0][index, pl.ds(start, size)]

    lane = lax.broadcasted_iota(jnp.int32, (1, rows), 1)

    def step(base):
        for offset in range(group):
            marks = load(base + offset, SLOTS * rows, CODE_ROWS).astype(jnp.float32)
            packed = jnp.zeros((1, rows), jnp.float32)
            for entry in range(SLOTS * CODES):
                packed = jnp.where(lane == entry, marks[entry:entry + 1], packed)
            codes[pl.ds(base + offset, 1)] = packed.astype(jnp.int32)
            for slot in range(SLOTS):
                block = load(base + offset, slot * rows, rows)
                lanes = pl.ds((offset * SLOTS + slot) * rows, rows)
                code = jnp.broadcast_to(marks[slot * CODES:slot * CODES + 1], (rows, rows))
                code = code.astype(block.dtype)
                zero = jnp.zeros_like(block)
                right[:, lanes] = jnp.where(code < cb, block, zero)
                for c in range(cb):
                    left[c * rows:(c + 1) * rows, lanes] = jnp.where(code == c, block, zero)
        return lax.dot_general(
            left[...], right[...], (((1,), (1,)), ((), ())), preferred_element_type=jnp.float32
        )

    def locate(first, size):
        ids = codes[pl.ds(first, size)] + leaves * cb
        found = jnp.zeros_like(ids)
        me = lax.axis_index("leaf")
        for q in range(anc_below.shape[1]):
            found = jnp.where(ids == anc_below[me, q], q, found)
        codes[pl.ds(first, size)] = jnp.where(
            lax.rem(lane, CODES) == 0, codes[pl.ds(first, size)], found
        )

    code_copy = pltpu.make_async_copy(codes, codes_out, code_sem)
    if leaves == group:
        product = step(0)
        locate(0, group)
        code_copy.start()
        out[...] = product.reshape(out.shape)
        code_copy.wait()
    else:
        out[...] = jnp.zeros_like(out)

        def accumulate(index, carry):
            first = pl.multiple_of(index * group, group)
            out[...] += step(first).reshape(out.shape)
            locate(first, group)
            return carry

        lax.fori_loop(0, leaves // group, accumulate, 0)
        code_copy.start()
        code_copy.wait()


def diagonal_update(heads, anc_below, cb, leaves, rows):
    group = min(leaves, 8)

    def body(*refs):
        diagonal_kernel(cb, leaves, *refs)

    return pl.pallas_call(
        body,
        name="diagonal",
        compiler_params=limit(12 if len(heads) > 1 else 40),
        out_shape=[
            pltpu.VMEM((cb * rows, rows), jnp.float32),
            pltpu.SMEM((leaves, rows), jnp.int32),
        ],
        in_specs=spaces(1, pltpu.SMEM) + spaces(len(heads), pltpu.VMEM),
        out_specs=spaces(1, pltpu.VMEM) + spaces(1, pltpu.SMEM),
        scratch_shapes=[
            pltpu.VMEM((cb * rows, group * SLOTS * rows), heads[0].dtype),
            pltpu.VMEM((rows, group * SLOTS * rows), heads[0].dtype),
            pltpu.VMEM((leaves, rows), jnp.int32),
            pltpu.SemaphoreType.DMA(()),
        ],
        cost_estimate=pl.CostEstimate(flops=2000000000, bytes_accessed=1000000, transcendentals=0),
    )(anc_below, *(near_core(*heads) if len(heads) > 1 else heads))


def below_kernel(cb, blk_count, per, leaves, count, parts, codes, *refs):
    tails, refs = refs[:count], refs[count:]
    heads = refs[:count]
    outs = refs[count:count + len(parts)]
    acc, products = refs[count + len(parts):]
    direct = count > 1
    me_blk = lax.axis_index("blk")
    rows = acc.shape[1]
    group = min(leaves, 8)
    tail_rows = tails[0].shape[-2] // SLOTS
    extra = tail_rows // rows
    size = cb * per // HALVES
    trash = len(parts) * size
    for first in range(0, trash, size):
        acc[pl.ds(first, size)] = jnp.zeros((size, rows, rows), jnp.float32)

    def step(base):
        for offset in range(group):
            index = base + offset
            for slot in range(SLOTS):
                if direct:
                    head = heads[index][pl.ds(slot * rows, rows)]
                    tail = tails[index][pl.ds(slot * tail_rows, tail_rows)]
                else:
                    head = heads[0][index, pl.ds(slot * rows, rows)]
                    tail = tails[0][index, pl.ds(slot * tail_rows, tail_rows)]
                products[offset * SLOTS + slot] = lax.dot_general(
                    tail, head, (((1,), (1,)), ((), ())), preferred_element_type=jnp.float32
                )
        for offset in range(group):
            for slot in range(SLOTS):
                column = codes[base + offset, slot * CODES]
                for r in range(extra):
                    position = codes[base + offset, slot * CODES + 1 + r]
                    relative = jnp.bitwise_xor(lax.rem(position, blk_count), me_blk)
                    part = relative * HALVES + lax.div(column * HALVES, cb)
                    start = jnp.int32(-1)
                    for at, (x, half) in enumerate(parts):
                        start = jnp.where(part == x * HALVES + half, at * size, start)
                    inside = lax.rem(column, cb // HALVES) * per + lax.div(position, blk_count)
                    place = jnp.where((column < cb) & (start >= 0), start + inside, trash)
                    acc[place] += products[offset * SLOTS + slot, pl.ds(r * rows, rows)]

    if leaves == group:
        step(0)
    else:
        lax.fori_loop(0, leaves // group, lambda index, carry: (step(index * group), carry)[1], 0)
    for at, out in enumerate(outs):
        out[...] = acc[pl.ds(at * size, size)]


def below_update(heads, tails, codes, parts, cb, blk_count, per, leaves, rows):
    group = min(leaves, 8)
    size = cb * per // HALVES

    def body(*refs):
        below_kernel(cb, blk_count, per, leaves, len(heads), parts, *refs)

    results = pl.pallas_call(
        body,
        compiler_params=limit(16 if len(heads) > 1 else 56),
        out_shape=[pltpu.VMEM((size, rows, rows), jnp.float32)] * len(parts),
        in_specs=spaces(1, pltpu.SMEM) + spaces(2 * len(heads), pltpu.VMEM),
        out_specs=spaces(len(parts), pltpu.VMEM),
        scratch_shapes=[
            pltpu.VMEM((len(parts) * size + 1, rows, rows), jnp.float32),
            pltpu.VMEM((group * SLOTS, tails[0].shape[-2] // SLOTS, rows), jnp.float32),
        ],
        cost_estimate=pl.CostEstimate(flops=2000000000, bytes_accessed=4000000, transcendentals=0),
    )(pltpu.with_memory_space_constraint(codes, pltpu.SMEM), *(near_core(*tails, *heads) if len(heads) > 1 else [*tails, *heads]))
    return dict(zip(parts, results))


def factor_block(work, rows):
    lane = lax.broadcasted_iota(jnp.int32, (1, rows), 1)
    sub = lax.broadcasted_iota(jnp.int32, (PANEL, 1), 0)
    segments = 4
    size = rows // segments

    for segment in range(segments):
        top = segment * size

        def panel(index, carry):
            base = pl.multiple_of(top + index * PANEL, PANEL)
            strip = work[pl.ds(base, PANEL), :]
            raw = work[top:, :rows]
            picks = [(lane == base + k) for k in range(PANEL)]
            corner = [
                jnp.sum(jnp.where(picks[k], strip[:, :rows], 0.0), axis=1, keepdims=True)
                for k in range(PANEL)
            ]
            factor = jnp.zeros((PANEL, 2 * rows), jnp.float32)
            for k in range(PANEL):
                scale = lax.rsqrt(corner[k][k:k + 1])
                inverse = scale * scale
                row = strip[k:k + 1]
                factor = jnp.where(sub == k, row * scale, factor)
                scaled = row * inverse
                strip = jnp.where(sub == k, scaled, strip - corner[k] * scaled)
                for m in range(k + 1, PANEL):
                    entry = corner[m][k:k + 1]
                    corner[m] = jnp.where(
                        sub == k, entry * inverse, corner[m] - (corner[k] * entry) * inverse
                    )
            work[pl.ds(base, PANEL), :] = factor
            for start, stop, masked in ((top, top + size, True), (top + size, rows, False)):
                if start == stop:
                    continue
                full = work[start:stop, :]
                row_id = lax.broadcasted_iota(jnp.int32, (stop - start, 1), 0) + start
                for k in range(PANEL):
                    column = jnp.sum(
                        jnp.where(picks[k], raw[start - top:stop - top], 0.0), axis=1, keepdims=True
                    )
                    if masked:
                        column = jnp.where(row_id >= base + PANEL, column, 0.0)
                    full = full - column * strip[k:k + 1]
                work[start:stop, :] = full
            return carry

        lax.fori_loop(0, size // PANEL, panel, 0)


def triangle(rows):
    row = lax.broadcasted_iota(jnp.int32, (rows, rows), 0)
    return row, lax.broadcasted_iota(jnp.int32, (rows, rows), 1)


def fold_sums(first, second, cb, rows):
    def body(first_ref, second_ref, total, folded):
        row, col = triangle(rows)
        line = lax.broadcasted_iota(jnp.int32, (PANEL, rows), 0)
        marks = jnp.zeros((PANEL, rows), jnp.float32)
        total[...] = first_ref[...] + second_ref[...]
        for pair in range(cb // 2):
            lower = total[2 * pair * rows:(2 * pair + 1) * rows]
            upper = total[(2 * pair + 1) * rows:(2 * pair + 2) * rows]
            folded[pair * rows:(pair + 1) * rows] = jnp.where(row >= col, lower, upper)
            edge = jnp.sum(jnp.where(row == col, upper, 0.0), axis=0, keepdims=True)
            marks = jnp.where(line == pair, edge, marks)
        folded[cb // 2 * rows:] = marks

    return pl.pallas_call(
        body,
        name="fold_sums",
        compiler_params=limit(8),
        out_shape=[
            pltpu.VMEM((cb * rows, rows), jnp.float32),
            pltpu.VMEM((cb // 2 * rows + PANEL, rows), jnp.float32),
        ],
        in_specs=spaces(2, pltpu.VMEM),
        out_specs=spaces(2, pltpu.VMEM),
    )(*near_core(first, second))


def unfold_sums(folded, cb, rows):
    row, col = triangle(rows)
    blocks = []
    for pair in range(cb // 2):
        square = folded[pair * rows:(pair + 1) * rows]
        edge = folded[cb // 2 * rows + pair:cb // 2 * rows + pair + 1]
        lower = jnp.where(row > col, square, 0.0)
        upper = jnp.where(row < col, square, 0.0)
        blocks.append(lower + lower.T + jnp.where(row == col, square, 0.0))
        blocks.append(upper + upper.T + jnp.where(row == col, edge, 0.0))
    return blocks


def small_dot(left, right, dims):
    return lax.dot_general(
        left, right, (dims, ((), ())), precision=HIGHEST, preferred_element_type=jnp.float32
    )


def write_inverse(out, first, second, between, rows):
    out[:rows, :rows] = first
    out[:rows, rows:] = jnp.zeros_like(first)
    out[rows:, rows:] = second
    product = small_dot(between, first, ((0,), (0,)))
    out[rows:, :rows] = -small_dot(second, product, ((1,), (0,)))


def eliminate(block, work, rows):
    row, col = triangle(rows)
    work[:, :rows] = block
    work[:, rows:] = (row == col).astype(jnp.float32)
    factor_block(work, rows)
    return jnp.where(row <= col, work[:, :rows], 0.0), work[:, rows:]


def first_factor(own_sum, other_sum, strips, cb, rows):
    blk_count = len(strips)
    half = cb // HALVES

    def body(own_ref, other_ref, *refs):
        strip_refs = refs[:blk_count]
        schur, lead, inverses, work = refs[blk_count:]
        me = lax.axis_index("blk")
        for x in range(blk_count):
            schur[jnp.bitwise_xor(me, x)] = strip_refs[x][...]
        others = unfold_sums(other_ref, cb, rows)
        for c in range(cb):
            part = slice(c * rows, (c + 1) * rows)
            schur[c, :, part] -= own_ref[part] + others[c]
        for block in range(half):
            here = block * rows
            upper, inverse = eliminate(schur[block, :, here:here + rows], work, rows)
            schur[block, :, here:here + rows] = upper
            inverses[block] = inverse
            after = here + rows
            strip = small_dot(inverse, schur[block, :, after:], ((1,), (0,)))
            schur[block, :, after:] = strip
            for other in range(block + 1, cb):
                offset = (other - block - 1) * rows
                schur[other, :, other * rows:] -= small_dot(
                    strip[:, offset:offset + rows], strip[:, offset:], ((0,), (0,))
                )
        write_inverse(lead, inverses[0], inverses[1], schur[0, :, rows:2 * rows], rows)

    return pl.pallas_call(
        body,
        name="factor_first",
        compiler_params=limit(12),
        out_shape=[
            pltpu.VMEM((cb, rows, cb * rows), jnp.float32),
            pltpu.VMEM((half * rows, half * rows), jnp.float32),
        ],
        in_specs=spaces(2 + blk_count, pltpu.VMEM),
        out_specs=spaces(2, pltpu.VMEM),
        scratch_shapes=[
            pltpu.VMEM((half, rows, rows), jnp.float32),
            pltpu.VMEM((rows, 2 * rows), jnp.float32),
        ],
        cost_estimate=pl.CostEstimate(flops=10000000000, bytes_accessed=2000000, transcendentals=0),
    )(*near_core(own_sum, other_sum, *strips))


def middle_factor(schur, cb, rows):
    def body(schur_ref, strip, corner, inverse_ref, work):
        block = cb // HALVES
        here = block * rows
        upper, inverse = eliminate(schur_ref[block, :, here:here + rows], work, rows)
        side = small_dot(inverse, schur_ref[block, :, here + rows:], ((1,), (0,)))
        strip[:, :rows] = upper
        strip[:, rows:] = side
        inverse_ref[...] = inverse
        corner[...] = schur_ref[cb - 1, :, here + rows:] - small_dot(side, side, ((0,), (0,)))

    return pl.pallas_call(
        body,
        name="factor_middle",
        compiler_params=limit(8),
        out_shape=[
            pltpu.VMEM((rows, 2 * rows), jnp.float32),
            pltpu.VMEM((rows, rows), jnp.float32),
            pltpu.VMEM((rows, rows), jnp.float32),
        ],
        in_specs=spaces(1, pltpu.VMEM),
        out_specs=spaces(3, pltpu.VMEM),
        scratch_shapes=[pltpu.VMEM((rows, 2 * rows), jnp.float32)],
        cost_estimate=pl.CostEstimate(flops=5000000000, bytes_accessed=1000000, transcendentals=0),
    )(*near_core(schur))


def last_factor(schur, strip, corner, inverse, cb, rows):
    half = cb // HALVES

    def body(schur_ref, strip_ref, corner_ref, inverse_ref, trail, lower, work):
        me = lax.axis_index("blk")
        upper, last = eliminate(corner_ref[...], work, rows)
        write_inverse(trail, inverse_ref[...], last, strip_ref[:, rows:], rows)
        mine = pl.ds(pl.multiple_of(me * rows, rows), rows)
        late = pl.ds(pl.multiple_of(jnp.maximum(me - half, 0) * rows, rows), rows)
        pieces = [schur_ref[k, :, mine] for k in range(half)] + [strip_ref[:, late], upper]
        for k in range(cb):
            lower[:, k * rows:(k + 1) * rows] = jnp.where(k <= me, pieces[k], 0.0).T

    return pl.pallas_call(
        body,
        name="factor_last",
        compiler_params=limit(8),
        out_shape=[
            pltpu.VMEM((half * rows, half * rows), jnp.float32),
            pltpu.VMEM((rows, cb * rows), jnp.float32),
        ],
        in_specs=spaces(4, pltpu.VMEM),
        out_specs=spaces(2, pltpu.VMEM),
        scratch_shapes=[pltpu.VMEM((rows, 2 * rows), jnp.float32)],
        cost_estimate=pl.CostEstimate(flops=5000000000, bytes_accessed=1000000, transcendentals=0),
    )(*near_core(schur, strip, corner, inverse))


def pack_sums(first, second):
    count, rows, width = first.shape
    groups = -(-count // LOWS)
    base = 2**LOW_BITS

    def body(first_ref, second_ref, out):
        row = lax.broadcasted_iota(jnp.int32, (SCALE_ROWS, width), 0)
        scales = jnp.zeros((SCALE_ROWS, width), jnp.int32)
        lows = []
        for j in range(count):
            value = first_ref[j] + second_ref[j]
            peak = jnp.maximum(jnp.max(jnp.abs(value), axis=0, keepdims=True), 1e-30)
            power = jnp.floor(jnp.log(peak) * LOG2E + 1e-3) + 1.0
            scales = jnp.where(row == j, power.astype(jnp.int32), scales)
            whole = jnp.floor(value * jnp.exp2(BITS - power) + 0.5).astype(jnp.int32)
            high = lax.shift_right_arithmetic(whole, LOW_BITS)
            lows.append(whole - high * base)
            out[j * rows:(j + 1) * rows] = high.astype(jnp.int16)
        for group in range(groups):
            low = jnp.zeros((rows, width), jnp.int32)
            for j in reversed(range(group, count, groups)):
                low = low * base + lows[j]
            out[(count + group) * rows:(count + group + 1) * rows] = low.astype(jnp.int16)
        out[(count + groups) * rows:] = scales.astype(jnp.int16)

    return pl.pallas_call(
        body,
        name="pack_sums",
        compiler_params=limit(8),
        out_shape=pltpu.VMEM(((count + groups) * rows + SCALE_ROWS, width), jnp.int16),
        in_specs=spaces(2, pltpu.VMEM),
        out_specs=pl.BlockSpec(memory_space=pltpu.VMEM),
    )(*near_core(first, second))


def unpack_sums(ref, index, count, rows):
    groups = -(-count // LOWS)
    base = 2**LOW_BITS
    high = ref[index * rows:(index + 1) * rows].astype(jnp.int32)
    at = (count + index % groups) * rows
    low = ref[at:at + rows].astype(jnp.int32)
    low = lax.shift_right_logical(low, LOW_BITS * (index // groups)) & (base - 1)
    scales = ref[(count + groups) * rows:].astype(jnp.float32)
    scale = jnp.exp2(scales[index:index + 1] - BITS)
    return (high * base + low).astype(jnp.float32) * scale


def remaining(panel_ref, update_refs, half, cb, per, rows):
    parts = []
    for c in range(cb // HALVES):
        column = (half * (cb // HALVES) + c) * rows
        block = slice(c * per, (c + 1) * per)
        count = (cb // HALVES) * per
        coded = [unpack_sums(update_refs[2], index, count, rows)[None] for index in range(c * per, (c + 1) * per)]
        update = update_refs[0][block] + update_refs[1][block] + jnp.concatenate(coded, axis=0)
        original = panel_ref[1:, :, column:column + rows]
        parts.append((original - update).reshape(per * rows, rows))
    return jnp.concatenate(parts, axis=1)


def solve_left(panel, updates, lead, schur, lower, cb, per, rows):
    width = cb * rows
    half = width // HALVES

    def body(panel_ref, *refs):
        updates_ref = refs[:len(updates)]
        lead_ref, schur_ref, lower_ref, out, carried = refs[len(updates):]
        left = remaining(panel_ref, updates_ref, 0, cb, per, rows)
        out[0] = lower_ref[...]
        value = small_dot(left, lead_ref[...], ((1,), (1,)))
        out[1:, :, :half] = value.reshape(per, rows, half)
        across = schur_ref[:cb // HALVES, :, half:].reshape(half, half)
        carried[...] = small_dot(value, across, ((1,), (0,)))

    return pl.pallas_call(
        body,
        name="solve_left",
        compiler_params=limit(16),
        out_shape=[
            jax.ShapeDtypeStruct((per + 1, rows, width), jnp.float32),
            pltpu.VMEM((per * rows, half), jnp.float32),
        ],
        in_specs=spaces(4 + len(updates), pltpu.VMEM),
        out_specs=spaces(2, pltpu.VMEM),
        cost_estimate=pl.CostEstimate(flops=2000000000, bytes_accessed=5000000, transcendentals=0),
    )(panel, *near_core(*updates, lead, schur, lower))


def solve_right(panel, updates, trail, carried, out, cb, per, rows):
    width = cb * rows
    half = width // HALVES

    def body(panel_ref, *refs):
        updates_ref = refs[:len(updates)]
        trail_ref, carried_ref, _, result, stage, sem = refs[len(updates):]
        left = remaining(panel_ref, updates_ref, 1, cb, per, rows) - carried_ref[...]
        value = small_dot(left, trail_ref[...], ((1,), (1,)))
        stage[...] = value.reshape(per, rows, half)
        copy = pltpu.make_async_copy(
            stage, result.at[pl.ds(1, per), :, pl.ds(half, half)], sem
        )
        copy.start()
        copy.wait()

    return pl.pallas_call(
        body,
        name="solve_right",
        compiler_params=limit(16),
        out_shape=jax.ShapeDtypeStruct((per + 1, rows, width), jnp.float32),
        in_specs=spaces(3 + len(updates), pltpu.VMEM) + spaces(1, pl.ANY),
        out_specs=pl.BlockSpec(memory_space=pl.ANY),
        scratch_shapes=[pltpu.VMEM((per, rows, half), jnp.float32), pltpu.SemaphoreType.DMA(())],
        input_output_aliases={3 + len(updates): 0},
        cost_estimate=pl.CostEstimate(flops=2000000000, bytes_accessed=5000000, transcendentals=0),
    )(panel, *near_core(*updates, trail, carried), out)


def shards(desc_panel, row_map, anc_order, anc_below, anc_panel):
    leaves = lax.axis_size("leaf")
    blk_count = lax.axis_size("blk")
    rows = anc_panel.shape[3]
    width = anc_panel.shape[4]
    cb = width // rows
    per = anc_below.shape[1] // blk_count
    assert cb == blk_count == 4 and desc_panel.shape[2] == rows
    direct = leaves <= DIRECT and leaves & (leaves - 1) == 0
    near = [(i, i ^ 1) for i in range(blk_count)]
    far = [(i, i ^ 2) for i in range(blk_count)]

    panel = anc_panel.reshape(per + 1, rows, width)
    *packed, strip = pack(desc_panel, row_map, anc_order, panel, cb, direct)
    count = len(packed) // 2
    heads, tails = packed[:count], packed[count:]

    def exchange(arrays):
        if not direct:
            return [lax.all_to_all(arrays[0], "leaf", split_axis=0, concat_axis=0, tiled=True)]
        received = [arrays[0]]
        for k in range(1, leaves):
            swap = [(i, i ^ k) for i in range(leaves)]
            received.append(lax.ppermute(arrays[k], "leaf", swap))
        return received

    heads = exchange(heads)
    tails = exchange(tails)
    strip_far = lax.ppermute(strip, "blk", far)
    strip_near = lax.ppermute(strip, "blk", near)
    strip_both = lax.ppermute(strip_far, "blk", near)
    strips = [strip, strip_near, strip_far, strip_both]

    diagonal, codes = diagonal_update(heads, anc_below, cb, leaves, rows)
    diagonal_near = lax.ppermute(diagonal, "blk", near)
    diagonal, folded = fold_sums(diagonal, diagonal_near, cb, rows)
    folded = lax.ppermute(folded, "blk", far)
    schur, lead = first_factor(diagonal, folded, strips, cb, rows)

    every = [(x, half) for x in range(blk_count) for half in range(HALVES)]
    urgent = [(2, 0), (3, 0)]
    later = [part for part in every if part not in urgent]
    sizes = (cb, blk_count, per, leaves, rows)
    partials = below_update(heads, tails, codes, urgent, *sizes)
    partials.update(below_update(heads, tails, codes, later, *sizes))
    kept, for_near, for_far, for_both = (
        [partials[x, half] for half in range(HALVES)] for x in range(blk_count)
    )
    from_near = []
    from_far = []
    for half in range(HALVES):
        passed = lax.ppermute(for_both[half], "blk", near)
        from_far.append(lax.ppermute(pack_sums(for_far[half], passed), "blk", far))
    for half in range(HALVES):
        from_near.append(lax.ppermute(for_near[half], "blk", near))
    strip, corner, inverse = middle_factor(schur, cb, rows)
    trail, lower = last_factor(schur, strip, corner, inverse, cb, rows)
    updates = [[kept[half], from_near[half], from_far[half]] for half in range(HALVES)]
    out, carried = solve_left(panel, updates[0], lead, schur, lower, cb, per, rows)
    out = solve_right(panel, updates[1], trail, carried, out, cb, per, rows)
    return out.reshape(anc_panel.shape)


def solution(mesh):
    in_specs = (
        P(("leaf", "blk"), None, None),
        P(("leaf", "blk"), None),
        P(),
        P(),
        P("leaf", None, "blk", None, None),
    )
    out_specs = P("leaf", None, "blk", None, None)

    return jax.shard_map(shards, mesh=mesh, in_specs=in_specs, out_specs=out_specs, check_vma=False)
```

```python
import jax
import jax.numpy as jnp
from jax import lax
from jax.experimental import pallas as pl
from jax.experimental.pallas import tpu as pltpu
from jax.sharding import PartitionSpec as P


SLOTS = 2
CODES = 4
CODE_ROWS = 8
PANEL = 8
HALVES = 2
SCALE_ROWS = 16
BITS = 19.0
LOW_BITS = 4
LOWS = 4
LOG2E = 1.4426950408889634
DIRECT = 8
HIGHEST = lax.Precision.HIGHEST


def repeat(count, body, unroll_to=16):
    if count <= unroll_to:
        for index in range(count):
            body(index)
    else:
        lax.fori_loop(0, count, lambda index, carry: (body(index), carry)[1], 0)


def limit(mib):
    return pltpu.CompilerParams(vmem_limit_bytes=mib * 1024 * 1024)


def near_core(*arrays):
    return [pltpu.with_memory_space_constraint(array, pltpu.VMEM) for array in arrays]


def spaces(count, space):
    return [pl.BlockSpec(memory_space=space)] * count


def pack_kernel(cb, direct, map_hbm, order_hbm, panel_hbm, anc_hbm, *refs):
    leaves = order_hbm.shape[0]
    block_count, desc_count = map_hbm.shape
    rows = panel_hbm.shape[1] // block_count
    tail_rows = (block_count - 1) * rows
    count = leaves if direct else 1
    heads, tails = refs[:count], refs[count:2 * count]
    strip, inverse, used, chosen, codes, row_map, anc_order, panel, sems = refs[2 * count:]
    me = lax.axis_index("leaf")
    copies = [
        pltpu.make_async_copy(source, target, sems.at[at])
        for at, (source, target) in enumerate((
            (map_hbm, row_map), (order_hbm, anc_order),
            (panel_hbm, panel), (anc_hbm.at[0], strip),
        ))
    ]
    for copy in copies:
        copy.start()
    copies[0].wait()
    copies[1].wait()

    def clear(leaf):
        inverse[anc_order[leaf]] = leaf
        used[leaf] = 0
        for slot in range(SLOTS):
            chosen[leaf * SLOTS + slot] = 0
            codes[(leaf * SLOTS + slot) * CODES] = cb
            for r in range(1, CODES):
                codes[(leaf * SLOTS + slot) * CODES + r] = 0

    repeat(leaves, clear)

    def assign(desc):
        head = row_map[0, desc]
        leaf = inverse[lax.div(head, cb)]
        taken = used[leaf]
        used[leaf] = taken + 1
        place = leaf * SLOTS + taken
        chosen[place] = desc
        codes[place * CODES] = head - anc_order[leaf] * cb
        for r in range(1, block_count):
            codes[place * CODES + r] = row_map[r, desc] - leaves * cb

    repeat(desc_count, assign)
    copies[2].wait()

    def write(index):
        leaf = jnp.bitwise_xor(me, index) if direct else index
        head = heads[index] if direct else heads[0].at[index]
        tail = tails[index] if direct else tails[0].at[index]
        row = lax.broadcasted_iota(jnp.int32, (CODE_ROWS, 128), 0)
        values = jnp.zeros((CODE_ROWS, 128), jnp.int32)
        for entry in range(SLOTS * CODES):
            values = jnp.where(row == entry, codes[leaf * SLOTS * CODES + entry], values)
        head[pl.ds(SLOTS * rows, CODE_ROWS)] = values.astype(jnp.float32).astype(panel.dtype)
        for slot in range(SLOTS):
            desc = chosen[leaf * SLOTS + slot]
            head[pl.ds(slot * rows, rows)] = panel[desc, pl.ds(0, rows)]
            tail[pl.ds(slot * tail_rows, tail_rows)] = panel[desc, pl.ds(rows, tail_rows)]

    repeat(leaves, write)
    copies[3].wait()


def pack(desc_panel, row_map, anc_order, anc, cb, direct):
    leaves = anc_order.shape[0]
    block_count = row_map.shape[1]
    rows = desc_panel.shape[1] // block_count
    width = desc_panel.shape[2]
    head = (SLOTS * rows + CODE_ROWS, width)
    tail = (SLOTS * (block_count - 1) * rows, width)
    dtype = desc_panel.dtype
    if direct:
        outs = [pltpu.VMEM(head, dtype)] * leaves + [pltpu.VMEM(tail, dtype)] * leaves
    else:
        outs = [jax.ShapeDtypeStruct((leaves,) + shape, dtype) for shape in (head, tail)]
    outs.append(pltpu.VMEM(anc.shape[1:], anc.dtype))

    def body(*refs):
        pack_kernel(cb, direct, *refs)

    return pl.pallas_call(
        body,
        name="pack",
        compiler_params=limit(12 if direct else 40),
        out_shape=outs,
        in_specs=spaces(4, pl.ANY),
        out_specs=spaces(len(outs), pltpu.VMEM),
        scratch_shapes=[
            pltpu.SMEM((leaves,), jnp.int32),
            pltpu.SMEM((leaves,), jnp.int32),
            pltpu.SMEM((leaves * SLOTS,), jnp.int32),
            pltpu.SMEM((leaves * SLOTS * CODES,), jnp.int32),
            pltpu.SMEM(row_map.T.shape, jnp.int32),
            pltpu.SMEM(anc_order.shape, jnp.int32),
            pltpu.VMEM(desc_panel.shape, dtype),
            pltpu.SemaphoreType.DMA((4,)),
        ],
    )(
        *(
            pltpu.with_memory_space_constraint(array, pltpu.HBM)
            for array in (row_map.T, anc_order, desc_panel, anc)
        )
    )


def diagonal_kernel(cb, leaves, anc_below, *refs):
    heads = refs[:-6]
    out, codes_out, left, right, codes, code_sem = refs[-6:]
    direct = len(heads) > 1
    rows = out.shape[1]
    group = min(leaves, 8)

    def load(index, start, size):
        if direct:
            return heads[index][pl.ds(start, size)]
        return heads[0][index, pl.ds(start, size)]

    lane = lax.broadcasted_iota(jnp.int32, (1, rows), 1)

    def step(base):
        for offset in range(group):
            marks = load(base + offset, SLOTS * rows, CODE_ROWS).astype(jnp.float32)
            packed = jnp.zeros((1, rows), jnp.float32)
            for entry in range(SLOTS * CODES):
                packed = jnp.where(lane == entry, marks[entry:entry + 1], packed)
            codes[pl.ds(base + offset, 1)] = packed.astype(jnp.int32)
            for slot in range(SLOTS):
                block = load(base + offset, slot * rows, rows)
                lanes = pl.ds((offset * SLOTS + slot) * rows, rows)
                code = jnp.broadcast_to(marks[slot * CODES:slot * CODES + 1], (rows, rows))
                code = code.astype(block.dtype)
                zero = jnp.zeros_like(block)
                right[:, lanes] = jnp.where(code < cb, block, zero)
                for c in range(cb):
                    left[c * rows:(c + 1) * rows, lanes] = jnp.where(code == c, block, zero)
        return lax.dot_general(
            left[...], right[...], (((1,), (1,)), ((), ())), preferred_element_type=jnp.float32
        )

    def locate(first, size):
        ids = codes[pl.ds(first, size)] + leaves * cb
        found = jnp.zeros_like(ids)
        me = lax.axis_index("leaf")
        for q in range(anc_below.shape[1]):
            found = jnp.where(ids == anc_below[me, q], q, found)
        codes[pl.ds(first, size)] = jnp.where(
            lax.rem(lane, CODES) == 0, codes[pl.ds(first, size)], found
        )

    code_copy = pltpu.make_async_copy(codes, codes_out, code_sem)
    if leaves == group:
        product = step(0)
        locate(0, group)
        code_copy.start()
        out[...] = product.reshape(out.shape)
        code_copy.wait()
    else:
        out[...] = jnp.zeros_like(out)

        def accumulate(index, carry):
            first = pl.multiple_of(index * group, group)
            out[...] += step(first).reshape(out.shape)
            locate(first, group)
            return carry

        lax.fori_loop(0, leaves // group, accumulate, 0)
        code_copy.start()
        code_copy.wait()


def diagonal_update(heads, anc_below, cb, leaves, rows):
    group = min(leaves, 8)

    def body(*refs):
        diagonal_kernel(cb, leaves, *refs)

    return pl.pallas_call(
        body,
        name="diagonal",
        compiler_params=limit(12 if len(heads) > 1 else 40),
        out_shape=[
            pltpu.VMEM((cb * rows, rows), jnp.float32),
            pltpu.SMEM((leaves, rows), jnp.int32),
        ],
        in_specs=spaces(1, pltpu.SMEM) + spaces(len(heads), pltpu.VMEM),
        out_specs=spaces(1, pltpu.VMEM) + spaces(1, pltpu.SMEM),
        scratch_shapes=[
            pltpu.VMEM((cb * rows, group * SLOTS * rows), heads[0].dtype),
            pltpu.VMEM((rows, group * SLOTS * rows), heads[0].dtype),
            pltpu.VMEM((leaves, rows), jnp.int32),
            pltpu.SemaphoreType.DMA(()),
        ],
        cost_estimate=pl.CostEstimate(flops=2000000000, bytes_accessed=1000000, transcendentals=0),
    )(anc_below, *(near_core(*heads) if len(heads) > 1 else heads))


def below_kernel(cb, blk_count, per, leaves, count, parts, codes, *refs):
    tails, refs = refs[:count], refs[count:]
    heads = refs[:count]
    outs = refs[count:count + len(parts)]
    acc, products = refs[count + len(parts):]
    direct = count > 1
    me_blk = lax.axis_index("blk")
    rows = acc.shape[1]
    group = min(leaves, 8)
    tail_rows = tails[0].shape[-2] // SLOTS
    extra = tail_rows // rows
    size = cb * per // HALVES
    trash = len(parts) * size
    for first in range(0, trash, size):
        acc[pl.ds(first, size)] = jnp.zeros((size, rows, rows), jnp.float32)

    def step(base):
        for offset in range(group):
            index = base + offset
            for slot in range(SLOTS):
                if direct:
                    head = heads[index][pl.ds(slot * rows, rows)]
                    tail = tails[index][pl.ds(slot * tail_rows, tail_rows)]
                else:
                    head = heads[0][index, pl.ds(slot * rows, rows)]
                    tail = tails[0][index, pl.ds(slot * tail_rows, tail_rows)]
                products[offset * SLOTS + slot] = lax.dot_general(
                    tail, head, (((1,), (1,)), ((), ())), preferred_element_type=jnp.float32
                )
        for offset in range(group):
            for slot in range(SLOTS):
                column = codes[base + offset, slot * CODES]
                for r in range(extra):
                    position = codes[base + offset, slot * CODES + 1 + r]
                    relative = jnp.bitwise_xor(lax.rem(position, blk_count), me_blk)
                    part = relative * HALVES + lax.div(column * HALVES, cb)
                    start = jnp.int32(-1)
                    for at, (x, half) in enumerate(parts):
                        start = jnp.where(part == x * HALVES + half, at * size, start)
                    inside = lax.rem(column, cb // HALVES) * per + lax.div(position, blk_count)
                    place = jnp.where((column < cb) & (start >= 0), start + inside, trash)
                    acc[place] += products[offset * SLOTS + slot, pl.ds(r * rows, rows)]

    if leaves == group:
        step(0)
    else:
        lax.fori_loop(0, leaves // group, lambda index, carry: (step(index * group), carry)[1], 0)
    for at, out in enumerate(outs):
        out[...] = acc[pl.ds(at * size, size)]


def below_update(heads, tails, codes, parts, cb, blk_count, per, leaves, rows):
    group = min(leaves, 8)
    size = cb * per // HALVES

    def body(*refs):
        below_kernel(cb, blk_count, per, leaves, len(heads), parts, *refs)

    results = pl.pallas_call(
        body,
        compiler_params=limit(16 if len(heads) > 1 else 56),
        out_shape=[pltpu.VMEM((size, rows, rows), jnp.float32)] * len(parts),
        in_specs=spaces(1, pltpu.SMEM) + spaces(2 * len(heads), pltpu.VMEM),
        out_specs=spaces(len(parts), pltpu.VMEM),
        scratch_shapes=[
            pltpu.VMEM((len(parts) * size + 1, rows, rows), jnp.float32),
            pltpu.VMEM((group * SLOTS, tails[0].shape[-2] // SLOTS, rows), jnp.float32),
        ],
        cost_estimate=pl.CostEstimate(flops=2000000000, bytes_accessed=4000000, transcendentals=0),
    )(pltpu.with_memory_space_constraint(codes, pltpu.SMEM), *(near_core(*tails, *heads) if len(heads) > 1 else [*tails, *heads]))
    return dict(zip(parts, results))


def factor_block(work, rows):
    lane = lax.broadcasted_iota(jnp.int32, (1, rows), 1)
    sub = lax.broadcasted_iota(jnp.int32, (PANEL, 1), 0)
    segments = 4
    size = rows // segments

    for segment in range(segments):
        top = segment * size

        def panel(index, carry):
            base = pl.multiple_of(top + index * PANEL, PANEL)
            strip = work[pl.ds(base, PANEL), :]
            raw = work[top:, :rows]
            picks = [(lane == base + k) for k in range(PANEL)]
            corner = [
                jnp.sum(jnp.where(picks[k], strip[:, :rows], 0.0), axis=1, keepdims=True)
                for k in range(PANEL)
            ]
            factor = jnp.zeros((PANEL, 2 * rows), jnp.float32)
            for k in range(PANEL):
                scale = lax.rsqrt(corner[k][k:k + 1])
                inverse = scale * scale
                row = strip[k:k + 1]
                factor = jnp.where(sub == k, row * scale, factor)
                scaled = row * inverse
                strip = jnp.where(sub == k, scaled, strip - corner[k] * scaled)
                for m in range(k + 1, PANEL):
                    entry = corner[m][k:k + 1]
                    corner[m] = jnp.where(
                        sub == k, entry * inverse, corner[m] - (corner[k] * entry) * inverse
                    )
            work[pl.ds(base, PANEL), :] = factor
            for start, stop, masked in ((top, top + size, True), (top + size, rows, False)):
                if start == stop:
                    continue
                full = work[start:stop, :]
                row_id = lax.broadcasted_iota(jnp.int32, (stop - start, 1), 0) + start
                for k in range(PANEL):
                    column = jnp.sum(
                        jnp.where(picks[k], raw[start - top:stop - top], 0.0), axis=1, keepdims=True
                    )
                    if masked:
                        column = jnp.where(row_id >= base + PANEL, column, 0.0)
                    full = full - column * strip[k:k + 1]
                work[start:stop, :] = full
            return carry

        lax.fori_loop(0, size // PANEL, panel, 0)


def triangle(rows):
    row = lax.broadcasted_iota(jnp.int32, (rows, rows), 0)
    return row, lax.broadcasted_iota(jnp.int32, (rows, rows), 1)


def fold_sums(first, second, cb, rows):
    def body(first_ref, second_ref, total, folded):
        row, col = triangle(rows)
        line = lax.broadcasted_iota(jnp.int32, (PANEL, rows), 0)
        marks = jnp.zeros((PANEL, rows), jnp.float32)
        total[...] = first_ref[...] + second_ref[...]
        for pair in range(cb // 2):
            lower = total[2 * pair * rows:(2 * pair + 1) * rows]
            upper = total[(2 * pair + 1) * rows:(2 * pair + 2) * rows]
            folded[pair * rows:(pair + 1) * rows] = jnp.where(row >= col, lower, upper)
            edge = jnp.sum(jnp.where(row == col, upper, 0.0), axis=0, keepdims=True)
            marks = jnp.where(line == pair, edge, marks)
        folded[cb // 2 * rows:] = marks

    return pl.pallas_call(
        body,
        name="fold_sums",
        compiler_params=limit(8),
        out_shape=[
            pltpu.VMEM((cb * rows, rows), jnp.float32),
            pltpu.VMEM((cb // 2 * rows + PANEL, rows), jnp.float32),
        ],
        in_specs=spaces(2, pltpu.VMEM),
        out_specs=spaces(2, pltpu.VMEM),
    )(*near_core(first, second))


def unfold_sums(folded, cb, rows):
    row, col = triangle(rows)
    blocks = []
    for pair in range(cb // 2):
        square = folded[pair * rows:(pair + 1) * rows]
        edge = folded[cb // 2 * rows + pair:cb // 2 * rows + pair + 1]
        lower = jnp.where(row > col, square, 0.0)
        upper = jnp.where(row < col, square, 0.0)
        blocks.append(lower + lower.T + jnp.where(row == col, square, 0.0))
        blocks.append(upper + upper.T + jnp.where(row == col, edge, 0.0))
    return blocks


def small_dot(left, right, dims):
    return lax.dot_general(
        left, right, (dims, ((), ())), precision=HIGHEST, preferred_element_type=jnp.float32
    )


def write_inverse(out, first, second, between, rows):
    out[:rows, :rows] = first
    out[:rows, rows:] = jnp.zeros_like(first)
    out[rows:, rows:] = second
    product = small_dot(between, first, ((0,), (0,)))
    out[rows:, :rows] = -small_dot(second, product, ((1,), (0,)))


def eliminate(block, work, rows):
    row, col = triangle(rows)
    work[:, :rows] = block
    work[:, rows:] = (row == col).astype(jnp.float32)
    factor_block(work, rows)
    return jnp.where(row <= col, work[:, :rows], 0.0), work[:, rows:]


def first_factor(own_sum, other_sum, strips, cb, rows):
    blk_count = len(strips)
    half = cb // HALVES

    def body(own_ref, other_ref, *refs):
        strip_refs = refs[:blk_count]
        schur, lead, inverses, work = refs[blk_count:]
        me = lax.axis_index("blk")
        for x in range(blk_count):
            schur[jnp.bitwise_xor(me, x)] = strip_refs[x][...]
        others = unfold_sums(other_ref, cb, rows)
        for c in range(cb):
            part = slice(c * rows, (c + 1) * rows)
            schur[c, :, part] -= own_ref[part] + others[c]
        for block in range(half):
            here = block * rows
            upper, inverse = eliminate(schur[block, :, here:here + rows], work, rows)
            schur[block, :, here:here + rows] = upper
            inverses[block] = inverse
            after = here + rows
            strip = small_dot(inverse, schur[block, :, after:], ((1,), (0,)))
            schur[block, :, after:] = strip
            for other in range(block + 1, cb):
                offset = (other - block - 1) * rows
                schur[other, :, other * rows:] -= small_dot(
                    strip[:, offset:offset + rows], strip[:, offset:], ((0,), (0,))
                )
        write_inverse(lead, inverses[0], inverses[1], schur[0, :, rows:2 * rows], rows)

    return pl.pallas_call(
        body,
        name="factor_first",
        compiler_params=limit(12),
        out_shape=[
            pltpu.VMEM((cb, rows, cb * rows), jnp.float32),
            pltpu.VMEM((half * rows, half * rows), jnp.float32),
        ],
        in_specs=spaces(2 + blk_count, pltpu.VMEM),
        out_specs=spaces(2, pltpu.VMEM),
        scratch_shapes=[
            pltpu.VMEM((half, rows, rows), jnp.float32),
            pltpu.VMEM((rows, 2 * rows), jnp.float32),
        ],
        cost_estimate=pl.CostEstimate(flops=10000000000, bytes_accessed=2000000, transcendentals=0),
    )(*near_core(own_sum, other_sum, *strips))


def middle_factor(schur, cb, rows):
    def body(schur_ref, strip, corner, inverse_ref, work):
        block = cb // HALVES
        here = block * rows
        upper, inverse = eliminate(schur_ref[block, :, here:here + rows], work, rows)
        side = small_dot(inverse, schur_ref[block, :, here + rows:], ((1,), (0,)))
        strip[:, :rows] = upper
        strip[:, rows:] = side
        inverse_ref[...] = inverse
        corner[...] = schur_ref[cb - 1, :, here + rows:] - small_dot(side, side, ((0,), (0,)))

    return pl.pallas_call(
        body,
        name="factor_middle",
        compiler_params=limit(8),
        out_shape=[
            pltpu.VMEM((rows, 2 * rows), jnp.float32),
            pltpu.VMEM((rows, rows), jnp.float32),
            pltpu.VMEM((rows, rows), jnp.float32),
        ],
        in_specs=spaces(1, pltpu.VMEM),
        out_specs=spaces(3, pltpu.VMEM),
        scratch_shapes=[pltpu.VMEM((rows, 2 * rows), jnp.float32)],
        cost_estimate=pl.CostEstimate(flops=5000000000, bytes_accessed=1000000, transcendentals=0),
    )(*near_core(schur))


def last_factor(schur, strip, corner, inverse, cb, rows):
    half = cb // HALVES

    def body(schur_ref, strip_ref, corner_ref, inverse_ref, trail, lower, work):
        me = lax.axis_index("blk")
        upper, last = eliminate(corner_ref[...], work, rows)
        write_inverse(trail, inverse_ref[...], last, strip_ref[:, rows:], rows)
        mine = pl.ds(pl.multiple_of(me * rows, rows), rows)
        late = pl.ds(pl.multiple_of(jnp.maximum(me - half, 0) * rows, rows), rows)
        pieces = [schur_ref[k, :, mine] for k in range(half)] + [strip_ref[:, late], upper]
        for k in range(cb):
            lower[:, k * rows:(k + 1) * rows] = jnp.where(k <= me, pieces[k], 0.0).T

    return pl.pallas_call(
        body,
        name="factor_last",
        compiler_params=limit(8),
        out_shape=[
            pltpu.VMEM((half * rows, half * rows), jnp.float32),
            pltpu.VMEM((rows, cb * rows), jnp.float32),
        ],
        in_specs=spaces(4, pltpu.VMEM),
        out_specs=spaces(2, pltpu.VMEM),
        scratch_shapes=[pltpu.VMEM((rows, 2 * rows), jnp.float32)],
        cost_estimate=pl.CostEstimate(flops=5000000000, bytes_accessed=1000000, transcendentals=0),
    )(*near_core(schur, strip, corner, inverse))


def pack_sums(first, second):
    count, rows, width = first.shape
    groups = -(-2 * count // LOWS)
    part = rows // 2
    base = 2**LOW_BITS

    def body(first_ref, second_ref, out):
        row = lax.broadcasted_iota(jnp.int32, (SCALE_ROWS, width), 0)
        scales = jnp.zeros((SCALE_ROWS, width), jnp.int32)
        lows = []
        for j in range(count):
            value = first_ref[j] + second_ref[j]
            peak = jnp.maximum(jnp.max(jnp.abs(value), axis=0, keepdims=True), 1e-30)
            power = jnp.floor(jnp.log(peak) * LOG2E + 1e-3) + 1.0
            scales = jnp.where(row == j, power.astype(jnp.int32), scales)
            whole = jnp.floor(value * jnp.exp2(BITS - power) + 0.5).astype(jnp.int32)
            high = lax.shift_right_arithmetic(whole, LOW_BITS)
            low = whole - high * base
            lows.extend((low[:part], low[part:]))
            out[j * rows:(j + 1) * rows] = high.astype(jnp.int16)
        for group in range(groups):
            low = jnp.zeros((part, width), jnp.int32)
            for j in reversed(range(group, 2 * count, groups)):
                low = low * base + lows[j]
            at = count * rows + group * part
            out[at:at + part] = (low - 32768).astype(jnp.int16)
        out[count * rows + groups * part:] = scales.astype(jnp.int16)

    return pl.pallas_call(
        body,
        name="pack_sums",
        compiler_params=limit(8),
        out_shape=pltpu.VMEM((count * rows + groups * part + SCALE_ROWS, width), jnp.int16),
        in_specs=spaces(2, pltpu.VMEM),
        out_specs=pl.BlockSpec(memory_space=pltpu.VMEM),
    )(*near_core(first, second))


def unpack_sums(ref, index, count, rows):
    groups = -(-2 * count // LOWS)
    part = rows // 2
    base = 2**LOW_BITS
    high = ref[index * rows:(index + 1) * rows].astype(jnp.int32)
    lows = []
    for j in (2 * index, 2 * index + 1):
        at = count * rows + j % groups * part
        low = ref[at:at + part].astype(jnp.int32) + 32768
        lows.append(lax.shift_right_logical(low, LOW_BITS * (j // groups)) & (base - 1))
    scales = ref[count * rows + groups * part:].astype(jnp.float32)
    scale = jnp.exp2(scales[index:index + 1] - BITS)
    return (high * base + jnp.concatenate(lows, axis=0)).astype(jnp.float32) * scale


def original(panel_ref, half, column_blocks, per, rows):
    first = half * column_blocks
    parts = [
        panel_ref[1:, :, (first + c) * rows:(first + c + 1) * rows].reshape(per * rows, rows)
        for c in range(column_blocks)
    ]
    return jnp.concatenate(parts, axis=1)


def side_by_side(blocks, per):
    columns = [
        jnp.concatenate(blocks[first:first + per], axis=0)
        for first in range(0, len(blocks), per)
    ]
    return jnp.concatenate(columns, axis=1)


def local_sums(first_ref, second_ref, per):
    return side_by_side([first_ref[j] + second_ref[j] for j in range(first_ref.shape[0])], per)


def far_sums(ref, count, per, rows):
    return side_by_side([unpack_sums(ref, j, count, rows) for j in range(count)], per)


def solve_left(panel, local, coded, later, lead, schur, cb, per, rows):
    width = cb * rows
    half = width // HALVES
    columns = cb // HALVES

    def body(panel_ref, kept, near, far, kept_later, near_later, lead_ref, schur_ref, solved,
             carried):
        left = original(panel_ref, 0, columns, per, rows) - local_sums(kept, near, per)
        left = left - far_sums(far, columns * per, per, rows)
        value = small_dot(left, lead_ref[...], ((1,), (1,)))
        solved[...] = value.reshape(per, rows, half)
        across = schur_ref[:columns, :, half:].reshape(half, half)
        right = original(panel_ref, 1, columns, per, rows)
        right = right - local_sums(kept_later, near_later, per)
        carried[...] = right - small_dot(value, across, ((1,), (0,)))

    return pl.pallas_call(
        body,
        name="solve_left",
        compiler_params=limit(16),
        out_shape=[
            pltpu.VMEM((per, rows, half), jnp.float32),
            pltpu.VMEM((per * rows, half), jnp.float32),
        ],
        in_specs=spaces(8, pltpu.VMEM),
        out_specs=spaces(2, pltpu.VMEM),
        cost_estimate=pl.CostEstimate(flops=2000000000, bytes_accessed=5000000, transcendentals=0),
    )(panel, *near_core(*local, coded, *later, lead, schur))


def solve_right(coded, trail, carried, solved, lower, cb, per, rows):
    width = cb * rows
    half = width // HALVES

    def body(far, trail_ref, carried_ref, solved_ref, lower_ref, result, stage, sems):
        below = result.at[pl.ds(1, per)]
        copies = [
            pltpu.make_async_copy(lower_ref, result.at[0], sems.at[0]),
            pltpu.make_async_copy(solved_ref, below.at[:, :, pl.ds(0, half)], sems.at[1]),
            pltpu.make_async_copy(stage, below.at[:, :, pl.ds(half, half)], sems.at[2]),
        ]
        copies[0].start()
        copies[1].start()
        left = carried_ref[...] - far_sums(far, cb // HALVES * per, per, rows)
        value = small_dot(left, trail_ref[...], ((1,), (1,)))
        stage[...] = value.reshape(per, rows, half)
        copies[2].start()
        for copy in copies:
            copy.wait()

    return pl.pallas_call(
        body,
        name="solve_right",
        compiler_params=limit(16),
        out_shape=jax.ShapeDtypeStruct((per + 1, rows, width), jnp.float32),
        in_specs=spaces(5, pltpu.VMEM),
        out_specs=pl.BlockSpec(memory_space=pl.ANY),
        scratch_shapes=[pltpu.VMEM((per, rows, half), jnp.float32), pltpu.SemaphoreType.DMA((3,))],
        cost_estimate=pl.CostEstimate(flops=2000000000, bytes_accessed=5000000, transcendentals=0),
    )(*near_core(coded, trail, carried, solved, lower))


def shards(desc_panel, row_map, anc_order, anc_below, anc_panel):
    leaves = lax.axis_size("leaf")
    blk_count = lax.axis_size("blk")
    rows = anc_panel.shape[3]
    width = anc_panel.shape[4]
    cb = width // rows
    per = anc_below.shape[1] // blk_count
    assert cb == blk_count == 4 and desc_panel.shape[2] == rows
    direct = leaves <= DIRECT and leaves & (leaves - 1) == 0
    near = [(i, i ^ 1) for i in range(blk_count)]
    far = [(i, i ^ 2) for i in range(blk_count)]

    panel = anc_panel.reshape(per + 1, rows, width)
    *packed, strip = pack(desc_panel, row_map, anc_order, panel, cb, direct)
    count = len(packed) // 2
    heads, tails = packed[:count], packed[count:]

    def exchange(arrays):
        if not direct:
            return [lax.all_to_all(arrays[0], "leaf", split_axis=0, concat_axis=0, tiled=True)]
        received = [arrays[0]]
        for k in range(1, leaves):
            swap = [(i, i ^ k) for i in range(leaves)]
            received.append(lax.ppermute(arrays[k], "leaf", swap))
        return received

    heads = exchange(heads)
    tails = exchange(tails)
    strip_far = lax.ppermute(strip, "blk", far)
    strip_near = lax.ppermute(strip, "blk", near)
    strip_both = lax.ppermute(strip_far, "blk", near)
    strips = [strip, strip_near, strip_far, strip_both]

    diagonal, codes = diagonal_update(heads, anc_below, cb, leaves, rows)
    diagonal_near = lax.ppermute(diagonal, "blk", near)
    diagonal, folded = fold_sums(diagonal, diagonal_near, cb, rows)
    folded = lax.ppermute(folded, "blk", far)
    schur, lead = first_factor(diagonal, folded, strips, cb, rows)

    every = [(x, half) for x in range(blk_count) for half in range(HALVES)]
    urgent = [(2, 0), (3, 0)]
    later = [part for part in every if part not in urgent]
    sizes = (cb, blk_count, per, leaves, rows)
    partials = below_update(heads, tails, codes, urgent, *sizes)
    partials.update(below_update(heads, tails, codes, later, *sizes))
    kept, for_near, for_far, for_both = (
        [partials[x, half] for half in range(HALVES)] for x in range(blk_count)
    )
    from_near = []
    from_far = []
    for half in range(HALVES):
        passed = lax.ppermute(for_both[half], "blk", near)
        from_far.append(lax.ppermute(pack_sums(for_far[half], passed), "blk", far))
    for half in range(HALVES):
        from_near.append(lax.ppermute(for_near[half], "blk", near))
    strip, corner, inverse = middle_factor(schur, cb, rows)
    trail, lower = last_factor(schur, strip, corner, inverse, cb, rows)
    local = [[kept[half], from_near[half]] for half in range(HALVES)]
    solved, carried = solve_left(
        panel, local[0], from_far[0], local[1], lead, schur, cb, per, rows
    )
    out = solve_right(from_far[1], trail, carried, solved, lower, cb, per, rows)
    return out.reshape(anc_panel.shape)


def solution(mesh):
    in_specs = (
        P(("leaf", "blk"), None, None),
        P(("leaf", "blk"), None),
        P(),
        P(),
        P("leaf", None, "blk", None, None),
    )
    out_specs = P("leaf", None, "blk", None, None)

    return jax.shard_map(shards, mesh=mesh, in_specs=in_specs, out_specs=out_specs, check_vma=False)
```
